32 devices in a mesh: shard: 4 (over x, core), replica: 8 (over z, y).
Axes of the slice: x: 2, y: 2, z: 4, core: 2. Of those that a mesh axis runs over, the one named last changes fastest.
Arguments:
- tokens: bfloat16 [16384, 768], P(('shard', 'replica')), may hold values from -6 to 6
- cotangent: bfloat16 [16384, 768], P(('shard', 'replica')), may hold values from -6 to 6
- lengths: int32 [32], replicated, may hold values from 16 to 512, as said below
- assignment: int32 [32], replicated, may hold values from 0 to 31, as said below
- positions: int32 [16384], P(('shard', 'replica')), may hold values from 0 to 2047, as said below
- attention_gain: bfloat16 [768], P('shard'), may hold values from 0.25 to 2.5
- query_weight: bfloat16 [768, 768], P('shard'), may hold values from -0.21875 to 0.21875
- key_weight: bfloat16 [768, 768], P('shard'), may hold values from -0.21875 to 0.21875
- value_weight: bfloat16 [768, 768], P('shard'), may hold values from -0.21875 to 0.21875
- out_weight: bfloat16 [768, 768], P('shard'), may hold values from -1.25 to 1.25
- feedforward_gain: bfloat16 [768], P('shard'), may hold values from 0.25 to 2.5
- gate_weight: bfloat16 [768, 3072], P('shard'), may hold values from -0.21875 to 0.21875
- up_weight: bfloat16 [768, 3072], P('shard'), may hold values from -0.21875 to 0.21875
- down_weight: bfloat16 [3072, 768], P('shard'), may hold values from -0.21875 to 0.21875
Outputs:
- output: bfloat16 [16384, 768], P(('shard', 'replica'))
- input_grad: float32 [16384, 768], P(('shard', 'replica'))
- attention_gain_grad: float32 [768], P('shard')
- query_grad: float32 [768, 768], P('shard')
- key_grad: float32 [768, 768], P('shard')
- value_grad: float32 [768, 768], P('shard')
- out_grad: float32 [768, 768], P('shard')
- feedforward_gain_grad: float32 [768], P('shard')
- gate_grad: float32 [768, 3072], P('shard')
- up_grad: float32 [768, 3072], P('shard')
- down_grad: float32 [3072, 768], P('shard')
The draws below stay inside these ranges and needn't reach their ends.
Inputs may be any that keep to these rules, and one draw needn't show every extreme that they name: `lengths`: each block holds exactly 1 sequence, 16 to 512 rows long; in some block it is exactly 512 rows long. `assignment`: every block index is named by exactly 1 sequence. Within a sequence, positions rise by one from row to row from a start between 0 and 2048 minus the sequence's length; empty rows hold 0.
All inputs are finite; a program needn't handle non-finite values.
Results may differ from the reference program's by a relative error of at most 0.023.
Values may be sent and summed in bfloat16 or wider, within the bound.
A program may use at most 192 MiB of HBM per device.

```python
import math
import jax
import jax.numpy as jnp
from jax import lax

D = 768
HEADS = 12
HDIM = 64
FF = 3072
MAXLEN = 512
MINLEN = 16
POSMAX = 2048
SEQ_DEV = 1
CAP = 512
NSEQ = 32
TOKENS = 16384
N_SHARD = 4
N_REPLICA = 8


def layout(key):
    base_key = jax.random.fold_in(key, 7001)
    split_keys = jax.random.split(base_key, 4)
    devices = NSEQ // SEQ_DEV
    drawn_lengths = jax.random.randint(split_keys[0], (devices, SEQ_DEV), MINLEN, MAXLEN + 1)
    fullest = jax.random.randint(split_keys[1], (), 0, devices)
    device_ids = jnp.arange(devices)[:, None]
    slot_ids = jnp.arange(SEQ_DEV)[None, :]
    drawn_lengths = jnp.where(device_ids == fullest, MAXLEN, drawn_lengths)
    drawn_lengths = jnp.where((device_ids == (fullest + 1) % devices) & (slot_ids == 0), MINLEN, drawn_lengths)
    filled = jnp.zeros((devices,), jnp.int32)
    columns = []
    for slot_index in range(SEQ_DEV):
        space_left = CAP - filled - (SEQ_DEV - 1 - slot_index) * MINLEN
        length_now = jnp.minimum(drawn_lengths[:, slot_index], space_left)
        filled = filled + length_now
        columns.append(length_now)
    length_table = jnp.stack(columns, axis=1)
    shuffled = jax.random.permutation(split_keys[2], NSEQ)
    assignment = (shuffled // SEQ_DEV).astype(jnp.int32)
    lengths = length_table[assignment, shuffled % SEQ_DEV].astype(jnp.int32)
    offsets = jax.random.randint(split_keys[3], (NSEQ,), 0, POSMAX - lengths + 1).astype(jnp.int32)
    offsets = offsets.at[0].set(0)
    offsets = offsets.at[1].set(POSMAX - lengths[1])
    return (lengths, assignment, offsets.astype(jnp.int32))


def draw_lengths(key, part):
    return layout(key)[0]


def draw_assignment(key, part):
    return layout(key)[1]


def draw_positions(key, part):
    lengths, assignment, offsets = layout(key)
    devices = NSEQ // SEQ_DEV

    def device_positions(device):
        owned_lengths = jnp.where(assignment == device, lengths, 0)
        seq_ends = jnp.cumsum(owned_lengths).astype(jnp.int32)
        starts = seq_ends - owned_lengths
        slot_ids = jnp.arange(CAP, dtype=jnp.int32)
        labels = jnp.sum((seq_ends[None, :] <= slot_ids[:, None]).astype(jnp.int32), axis=1)
        matches = labels[:, None] == jnp.arange(NSEQ, dtype=jnp.int32)[None, :]
        base_offset = jnp.sum(jnp.where(matches, (offsets - starts)[None, :], 0), axis=1)
        return jnp.where(slot_ids < seq_ends[-1], base_offset + slot_ids, 0).astype(jnp.int32)
    return lax.map(device_positions, jnp.arange(devices, dtype=jnp.int32)).reshape(-1)


def levels(key, dims, cuts, smallest, largest):
    def one(dim, parts):
        steps = jax.random.uniform(jax.random.fold_in(jax.random.fold_in(key, 6), dim), (parts,), jnp.float32, smallest / len(cuts), largest / len(cuts))
        return jnp.repeat(jnp.exp(steps), dims[dim] // parts).reshape((-1,) + (1,) * (len(dims) - dim - 1))

    loudness = one(*cuts[0])
    for cut in cuts[1:]:
        loudness = loudness * one(*cut)
    return loudness


def gaussian(key, extent, deviation, bound, cuts=(), kind=jnp.bfloat16):
    entries = jax.random.normal(key, extent, jnp.float32) * deviation
    if len(cuts) > 0:
        entries = levels(key, extent, cuts, -0.22, 0.18) * entries
    return jnp.clip(entries, min=-bound, max=bound).astype(kind)


def setup_inputs(seed: int = 0) -> dict:
    splits = jax.random.split(jax.random.key(seed), 15)
    tokens = gaussian(splits[0], (TOKENS, D), 1.0, 6.0, ((0, 32),))
    cotangent = gaussian(splits[1], (TOKENS, D), 1.0, 6.0, ((0, 32),))
    lengths = draw_lengths(jax.random.fold_in(splits[14], 71), 0)
    assignment = draw_assignment(jax.random.fold_in(splits[14], 71), 0)
    positions = draw_positions(jax.random.fold_in(splits[14], 71), 0)
    attention_gain = jnp.clip(jnp.exp(math.log(2.5) - 2.3025851 * jax.random.uniform(splits[5], (D,), jnp.float32) ** levels(splits[5], (D,), ((0, 4),), -0.2, 0.2)), 0.25, 2.5).astype(jnp.bfloat16)
    query_weight = gaussian(splits[6], (D, D), D ** -0.5, 0.21875, ((0, 4),))
    key_weight = gaussian(splits[7], (D, D), D ** -0.5, 0.21875, ((0, 4),))
    value_weight = gaussian(splits[8], (D, D), D ** -0.5, 0.21875, ((0, 4),))
    out_weight = gaussian(splits[9], (D, D), (D // 32) ** -0.5, 1.25, ((0, 4),))
    feedforward_gain = jnp.clip(jnp.exp(math.log(2.5) - 2.3025851 * jax.random.uniform(splits[10], (D,), jnp.float32) ** levels(splits[10], (D,), ((0, 4),), -0.2, 0.2)), 0.25, 2.5).astype(jnp.bfloat16)
    gate_weight = gaussian(splits[11], (D, FF), D ** -0.5, 0.21875, ((0, 4),))
    up_weight = gaussian(splits[12], (D, FF), D ** -0.5, 0.21875, ((0, 4),))
    down_weight = gaussian(splits[13], (FF, D), (FF // 4) ** -0.5, 0.21875, ((0, 4),))
    return dict(tokens=tokens, cotangent=cotangent, lengths=lengths, assignment=assignment, positions=positions, attention_gain=attention_gain, query_weight=query_weight, key_weight=key_weight, value_weight=value_weight, out_weight=out_weight, feedforward_gain=feedforward_gain, gate_weight=gate_weight, up_weight=up_weight, down_weight=down_weight)


EPSILON = 1e-05
ROPE_BASE = 10000.0

@jax.custom_vjp
def low(v):
    return lax.optimization_barrier(v.astype(jnp.bfloat16)).astype(jnp.float32)

@jax.custom_vjp
def low_back(v):
    return v

def low_keep(v):
    return (low(v), None)

def low_pass(kept, grad):
    return (grad,)

def back_keep(v):
    return (v, None)

def back_low(kept, grad):
    return (low(grad),)
low.defvjp(low_keep, low_pass)
low_back.defvjp(back_keep, back_low)

def rms_scale(values):
    return lax.rsqrt(lax.optimization_barrier(jnp.mean(values * values, axis=-1, keepdims=True)) + EPSILON)

def rotation(positions, head_size):
    half_size = head_size // 2
    steps_range = jnp.arange(half_size, dtype=jnp.float32)
    frequency = jnp.exp(steps_range * (-2.0 * math.log(ROPE_BASE) / head_size))
    angles = positions.astype(jnp.float32)[:, None] * frequency[None, :]
    return (jnp.cos(angles), jnp.sin(angles))

def rotate(values, cosine_table, sine_table):
    half_size = cosine_table.shape[1]
    shaped = values.reshape(values.shape[0], -1, 2 * half_size)
    first_half = shaped[..., :half_size]
    second_half = shaped[..., half_size:]
    cos_rows = cosine_table[:, None, :]
    sin_rows = sine_table[:, None, :]
    turned = jnp.concatenate([first_half * cos_rows - second_half * sin_rows, second_half * cos_rows + first_half * sin_rows], axis=-1)
    return turned.reshape(values.shape)

def sequence_mask(lengths, assignment, device, slot_count):
    owned_lengths = jnp.where(assignment == device, lengths, 0)
    seq_ends = jnp.cumsum(owned_lengths).astype(jnp.int32)
    slot_ids = jnp.arange(slot_count, dtype=jnp.int32)
    labels = lax.optimization_barrier(jnp.sum((seq_ends[None, :] <= slot_ids[:, None]).astype(jnp.int32), axis=1))
    allowed = (labels[:, None] == labels[None, :]) & (slot_ids[None, :] <= slot_ids[:, None])
    valid_rows = (slot_ids < seq_ends[-1]).astype(jnp.float32)[:, None]
    return (allowed, valid_rows)

def layer_forward(params, values, valid_rows, allowed, cosine_table, sine_table):
    gain_one, w_query, w_key, w_value, w_out, gain_two, w_gate, w_up, w_down = params
    highest = lax.Precision.HIGHEST
    rows_count = values.shape[0]
    normed = low(values * rms_scale(values) * gain_one)
    query_lin = low_back(jnp.dot(normed, w_query, precision=highest))
    key_lin = low_back(jnp.dot(normed, w_key, precision=highest))
    value_low = low(low_back(jnp.dot(normed, w_value, precision=highest)))
    query_rot = low(rotate(query_lin, cosine_table, sine_table)).reshape(rows_count, HEADS, HDIM)
    key_rot = low(rotate(key_lin, cosine_table, sine_table)).reshape(rows_count, HEADS, HDIM)
    value_heads = value_low.reshape(rows_count, HEADS, HDIM)
    scores = low_back(jnp.einsum('qhd,khd->hqk', query_rot, key_rot, precision=highest) * (1.0 / math.sqrt(HDIM)))
    scores = jnp.where(allowed[None], scores, -jnp.inf)
    row_peak = lax.optimization_barrier(jnp.max(scores, axis=-1, keepdims=True))
    exponent = jnp.exp(scores - row_peak)
    probability = low(exponent / lax.optimization_barrier(jnp.sum(exponent, axis=-1, keepdims=True)))
    attended = jnp.einsum('hqk,khd->qhd', probability, value_heads, precision=highest).reshape(rows_count, HEADS * HDIM)
    attended = low(low_back(attended))
    branch_one = low_back(jnp.dot(attended, w_out, precision=highest))
    hidden_one = values + branch_one
    normed_two = low(hidden_one * rms_scale(hidden_one) * gain_two)
    gate = low_back(jnp.dot(normed_two, w_gate, precision=highest))
    upward = low_back(jnp.dot(normed_two, w_up, precision=highest))
    hidden = low(jax.nn.silu(gate) * upward)
    branch_two = low_back(jnp.dot(hidden, w_down, precision=highest))
    return (hidden_one + branch_two) * valid_rows

def reference(tokens, cotangent, lengths, assignment, positions, attention_gain, query_weight, key_weight, value_weight, out_weight, feedforward_gain, gate_weight, up_weight, down_weight):
    devices = N_SHARD * N_REPLICA
    params = tuple((weight.astype(jnp.float32) for weight in (attention_gain, query_weight, key_weight, value_weight, out_weight, feedforward_gain, gate_weight, up_weight, down_weight)))
    inputs = tokens.astype(jnp.float32).reshape(devices, CAP, D)
    cotangents = cotangent.astype(jnp.float32).reshape(devices, CAP, D)
    places = positions.reshape(devices, CAP)

    def one_block(carry, item):
        values, grad_rows, place_rows, device = item
        allowed, valid_rows = sequence_mask(lengths, assignment, device, CAP)
        cosine_table, sine_table = rotation(place_rows, HDIM)

        def slab_forward(weights, rows_in):
            return layer_forward(weights, rows_in, valid_rows, allowed, cosine_table, sine_table)
        result, pullback = jax.vjp(jax.checkpoint(slab_forward), params, values)
        grad_params, grad_rows_in = pullback(grad_rows)
        carry = tuple((total + piece for total, piece in zip(carry, grad_params)))
        return (carry, (result.astype(jnp.bfloat16), grad_rows_in))
    initial = tuple((jnp.zeros_like(weight) for weight in params))
    grads, (outputs, input_grads) = lax.scan(one_block, initial, (inputs, cotangents, places, jnp.arange(devices, dtype=jnp.int32)))
    return (outputs.reshape(TOKENS, D), input_grads.reshape(TOKENS, D), grads[0], grads[1], grads[2], grads[3], grads[4], grads[5], grads[6], grads[7], grads[8])
```

```python
import functools
import math

import jax
import jax.numpy as jnp
from jax import lax
from jax.experimental import pallas as pl
from jax.experimental.pallas import tpu as pltpu
from jax.sharding import PartitionSpec as P

HEADS = 12
HDIM = 64
EPSILON = 1e-05
ROPE_BASE = 10000.0
MESH = pl.DeviceIdType.MESH
F32 = jnp.float32
BF16 = jnp.bfloat16


def whereabouts():
    return lax.axis_index("shard"), lax.axis_index("replica")


def toggle(index, stride):
    return index + (1 - 2 * ((index // stride) % 2)) * stride


def flip(index, stride, count):
    place = (index // stride) % count
    base = index - place * stride
    return place, [base + ((place + step) % count) * stride for step in range(1, count)]


def at(shard, replica):
    return {"shard": shard, "replica": replica}


def greet(peers):
    barrier = pltpu.get_barrier_semaphore()
    for peer in peers:
        pl.semaphore_signal(barrier, inc=1, device_id=peer, device_id_type=MESH)
    pl.semaphore_wait(barrier, len(peers))


def remote(source, target, send, receive, peer):
    return pltpu.make_async_remote_copy(
        src_ref=source,
        dst_ref=target,
        send_sem=send,
        recv_sem=receive,
        device_id=peer,
        device_id_type=MESH,
    )


def rows_at(start, size, step=16):
    return pl.ds(pl.multiple_of(start, step), size)


def unit_list(arrays):
    units = []
    for number, (rows, columns) in enumerate(arrays):
        for row in range(0, rows, UNIT_ROWS):
            for column in range(0, columns, UNIT_COLS):
                units.append((number, row, column))
    return units


UNIT_ROWS = 192
UNIT_COLS = 768


def gather_kernel(units, shard_rows, targets, *refs):
    count = len(shard_rows)
    own = refs[:count]
    own_gain = refs[count]
    outs = refs[count + 1 : count + 1 + 5]
    sems = refs[count + 6 :]
    (local, x_out, x_in, y_out, y_in, p_out, p_in, f_out, f_in, g_out, g_in) = sems
    shard, replica = whereabouts()
    core, _ = flip(shard, 1, 2)
    partner = flip(shard, 1, 2)[1][0]
    across = flip(shard, 2, 2)[1][0]
    opposite = flip(across, 1, 2)[1][0]
    side, (beside,) = flip(replica, 1, 2)
    half = UNIT_ROWS // 2

    to_partner = at(partner, replica)
    to_across = at(across, replica)
    to_opposite = at(opposite, replica)
    to_beside = at(shard, beside)
    greet([to_partner, to_across, to_opposite, to_beside])

    def place(unit, owner, part):
        number, row, column = unit
        target, offset = targets[number]
        start, size = row, UNIT_ROWS
        if part is not None:
            start, size = row + part * half, half
        return outs[target].at[
            rows_at(owner * shard_rows[number] + start, size),
            pl.ds(offset + column, UNIT_COLS),
        ]

    def mine(unit, part):
        number, row, column = unit
        start, size = row, UNIT_ROWS
        if part is not None:
            start, size = row + part * half, half
        return own[number].at[rows_at(start, size), pl.ds(column, UNIT_COLS)]

    gains = outs[4]
    gain_copies = []
    for number, peer in enumerate((to_partner, to_across, to_opposite)):
        copy = remote(
            own_gain, gains.at[shard], g_out.at[number], g_in.at[number], peer
        )
        copy.start()
        gain_copies.append(copy)
    total = len(units)
    keep_gain = pltpu.make_async_copy(own_gain, gains.at[shard], local.at[total])
    keep_gain.start()

    keeps, crosses, shares = [], [], []
    for number, unit in enumerate(units):
        cross = remote(
            mine(unit, side), place(unit, shard, side), x_out.at[number], x_in.at[number], to_across
        )
        cross.start()
        share = remote(
            mine(unit, None), place(unit, shard, None), p_out.at[number], p_in.at[number], to_partner
        )
        share.start()
        keep = pltpu.make_async_copy(mine(unit, None), place(unit, shard, None), local.at[number])
        keep.start()
        crosses.append(cross)
        shares.append(share)
        keeps.append(keep)

    passes, forwards = [], []

    def finish(number):
        unit = units[number]
        passes[number].wait_recv()
        second = remote(
            place(unit, across, 1 - side),
            place(unit, across, 1 - side),
            f_out.at[1, number],
            f_in.at[1, number],
            to_partner,
        )
        second.start()
        forwards.append(second)

    for number, unit in enumerate(units):
        crosses[number].wait_recv()
        beside_copy = remote(
            place(unit, across, side),
            place(unit, across, side),
            y_out.at[number],
            y_in.at[number],
            to_beside,
        )
        beside_copy.start()
        passes.append(beside_copy)
        first = remote(
            place(unit, across, side),
            place(unit, across, side),
            f_out.at[0, number],
            f_in.at[0, number],
            to_partner,
        )
        first.start()
        forwards.append(first)
        if number > 0:
            finish(number - 1)
    finish(total - 1)
    for copy in crosses + passes:
        copy.wait_send()
    for copy in shares + forwards + gain_copies:
        copy.wait()
    for copy in keeps + [keep_gain]:
        copy.wait()


def gather_weights(arrays, gain_rows):
    width = arrays[0].shape[1]
    inner = arrays[4].shape[1]
    shards = lax.axis_size("shard")
    shard_rows = [a.shape[0] for a in arrays]
    targets = [(0, 0), (0, width), (0, 2 * width), (1, 0), (2, 0), (2, inner), (3, 0)]
    units = unit_list([a.shape for a in arrays])
    total = len(units)
    dma = pltpu.SemaphoreType.DMA
    return pl.pallas_call(
        functools.partial(gather_kernel, units, shard_rows, targets),
        out_shape=(
            jax.ShapeDtypeStruct((shards * shard_rows[0], 3 * width), BF16),
            jax.ShapeDtypeStruct((shards * shard_rows[3], width), BF16),
            jax.ShapeDtypeStruct((shards * shard_rows[4], 2 * inner), BF16),
            jax.ShapeDtypeStruct((shards * shard_rows[6], width), BF16),
            jax.ShapeDtypeStruct((shards,) + gain_rows.shape, gain_rows.dtype),
        ),
        in_specs=[pl.BlockSpec(memory_space=pltpu.VMEM)] * 8,
        out_specs=[pl.BlockSpec(memory_space=pl.ANY)] * 5,
        scratch_shapes=[
            dma((total + 1,)),
            dma((total,)),
            dma((total,)),
            dma((total,)),
            dma((total,)),
            dma((total,)),
            dma((total,)),
            dma((2, total)),
            dma((2, total)),
            dma((3,)),
            dma((3,)),
        ],
        compiler_params=pltpu.CompilerParams(
            collective_id=0, has_side_effects=True, vmem_limit_bytes=16 * 1024 * 1024
        ),
        name="gather_weights",
    )(*arrays, gain_rows)


def replica_factors(count):
    if count == 8:
        return [(2, 1), (4, 2)], 1
    assert count == 32
    return [(2, 16), (4, 4), (4, 1)], 4


def reduce_kernel(factors, pack, units, shard_rows, *refs):
    levels = len(factors)
    count = len(shard_rows)
    grads = refs[:count]
    gain_in, out, gain_out = refs[count : count + 3]
    own, near, far, fin, gain_sum, gain_got = refs[count + 3 : count + 9]
    parts = refs[count + 9 : count + 9 + levels]
    sems = list(refs[count + 9 + levels :])
    load_sem, near_out, near_in, far_out, far_in, store_sem, gain_send, gain_recv = sems[:8]
    down_out, down_in, up_out, up_in = (
        sems[8 + kind * levels : 8 + (kind + 1) * levels] for kind in range(4)
    )
    shard, replica = whereabouts()
    partner, across = toggle(shard, 1), toggle(shard, 2)
    opposite = toggle(across, 1)
    groups = []
    for members, stride in factors:
        place, others = flip(replica, stride, members)
        groups.append((members, place, others))
    greet(
        [at(partner, replica), at(across, replica)]
        + [at(shard, other) for group in groups for other in group[2]]
    )
    chunk_rows = UNIT_ROWS * pack
    chunks = len(units) // pack

    def region(places):
        row, rows, column, columns = 0, chunk_rows, 0, UNIT_COLS
        for level, place in enumerate(places):
            members = factors[level][0]
            if level == levels - 1:
                rows, columns = rows // 2, columns // 2
                row = row + (place // 2) * rows
                column = column + (place % 2) * columns
            else:
                rows = rows // members
                row = row + place * rows
        return rows_at(row, rows), rows_at(column, columns, 128)

    my_places = [group[1] for group in groups]

    def block(unit, owner):
        number, row, column = units[unit]
        return grads[number].at[
            rows_at(owner * shard_rows[number] + row, UNIT_ROWS), pl.ds(column, UNIT_COLS)
        ]

    for chunk in range(chunks):
        for which, (keep, give) in enumerate(((across, opposite), (shard, partner))):
            for piece in range(pack):
                unit = chunk * pack + piece
                inside = pl.ds(piece * UNIT_ROWS, UNIT_ROWS)
                remote(
                    block(unit, give),
                    near.at[chunk, which, inside],
                    near_out.at[chunk, which, piece],
                    near_in.at[chunk, which, piece],
                    at(partner, replica),
                ).start()
                pltpu.make_async_copy(
                    block(unit, keep), own.at[chunk, which, inside], load_sem.at[chunk, which, piece]
                ).start()

    flips = [at(partner, replica), at(across, replica)]
    stride = 1
    total_replicas = math.prod(members for members, _ in factors)
    while stride < total_replicas:
        flips.append(at(shard, toggle(replica, stride)))
        stride *= 2

    def gain_copy(step):
        source = gain_in if step == 0 else gain_sum.at[step - 1]
        return remote(source, gain_got.at[step], gain_send.at[step], gain_recv.at[step], flips[step])

    gain_copy(0).start()

    def near_copy(chunk, which, piece):
        inside = pl.ds(piece * UNIT_ROWS, UNIT_ROWS)
        return remote(
            own.at[chunk, which, inside],
            near.at[chunk, which, inside],
            near_out.at[chunk, which, piece],
            near_in.at[chunk, which, piece],
            at(partner, replica),
        )

    def far_copy(chunk):
        return remote(
            own.at[chunk, 0], far.at[chunk], far_out.at[chunk], far_in.at[chunk], at(across, replica)
        )

    def down_copy(level, chunk, step):
        members, place, others = groups[level]
        theirs = (place + step + 1) % members
        where = region(my_places[:level] + [theirs])
        return remote(
            own.at[(chunk, 1) + where],
            parts[level].at[chunk, step],
            down_out[level].at[chunk, step],
            down_in[level].at[chunk, step],
            at(shard, others[step]),
        )

    def up_copy(level, chunk, step):
        where = region(my_places[: level + 1])
        return remote(
            fin.at[(chunk,) + where],
            fin.at[(chunk,) + where],
            up_out[level].at[chunk, step],
            up_in[level].at[chunk, step],
            at(shard, groups[level][2][step]),
        )

    def store_copy(chunk):
        return pltpu.make_async_copy(fin.at[chunk], out.at[chunk], store_sem.at[chunk])

    def over_steps(level, act):
        for step in range(groups[level][0] - 1):
            act(step)

    def add_into(target, *sources):
        total = target[...].astype(F32)
        for source in sources:
            total = total + source[...].astype(F32)
        return total.astype(BF16)

    def stage_near(chunk):
        for which in range(2):
            for piece in range(pack):
                inside = pl.ds(piece * UNIT_ROWS, UNIT_ROWS)
                pltpu.make_async_copy(
                    own.at[chunk, which, inside],
                    own.at[chunk, which, inside],
                    load_sem.at[chunk, which, piece],
                ).wait()
                near_copy(chunk, which, piece).wait_recv()
            mine = own.at[chunk, which]
            mine[...] = add_into(mine, near.at[chunk, which])
            if which == 0:
                far_copy(chunk).start()

    def stage_far(chunk):
        far_copy(chunk).wait_recv()
        mine = own.at[chunk, 1]
        mine[...] = add_into(mine, far.at[chunk])
        over_steps(0, lambda step: down_copy(0, chunk, step).start())

    def stage_down(level, chunk):
        over_steps(level, lambda step: down_copy(level, chunk, step).wait_recv())
        where = region(my_places[: level + 1])
        total = add_into(
            own.at[(chunk, 1) + where],
            *[parts[level].at[chunk, step] for step in range(groups[level][0] - 1)],
        )
        if level + 1 < levels:
            own.at[(chunk, 1) + where][...] = total
            over_steps(level + 1, lambda step: down_copy(level + 1, chunk, step).start())
        else:
            fin.at[(chunk,) + where][...] = total
            over_steps(level, lambda step: up_copy(level, chunk, step).start())

    def stage_up(level, chunk):
        over_steps(level, lambda step: up_copy(level, chunk, step).wait_recv())
        if level > 0:
            over_steps(level - 1, lambda step: up_copy(level - 1, chunk, step).start())
        else:
            store_copy(chunk).start()

    stages = [stage_near, None, stage_far]
    stages += [functools.partial(stage_down, level) for level in range(levels)]
    stages += [functools.partial(stage_up, level) for level in reversed(range(levels))]
    steps = chunks + len(stages) - 1

    def tick(time, carry):
        for lag, stage in enumerate(stages):
            if stage is not None:
                pl.when((time >= lag) & (time < chunks + lag))(functools.partial(stage, time - lag))
        for step in range(len(flips)):

            @pl.when(time == step)
            def _():
                gain_copy(step).wait_recv()
                if step == 0:
                    total = gain_in[...] + gain_got[step]
                else:
                    total = gain_sum[step - 1] + gain_got[step]
                if step + 1 < len(flips):
                    gain_sum[step] = total
                    gain_copy(step + 1).start()
                else:
                    gain_out[...] = total

        return carry

    assert len(flips) <= steps
    lax.fori_loop(0, steps, tick, 0)

    def settle(chunk, carry):
        for which in range(2):
            for piece in range(pack):
                near_copy(chunk, which, piece).wait_send()
        far_copy(chunk).wait_send()
        for level in range(levels):
            over_steps(level, lambda step: down_copy(level, chunk, step).wait_send())
            over_steps(level, lambda step: up_copy(level, chunk, step).wait_send())
        store_copy(chunk).wait()
        return carry

    lax.fori_loop(0, chunks, settle, 0)
    for step in range(len(flips)):
        gain_copy(step).wait_send()


def reduce_grads(grads, gain_sums):
    shards = lax.axis_size("shard")
    replicas = lax.axis_size("replica")
    factors, pack = replica_factors(replicas)
    levels = len(factors)
    shapes = [(g.shape[0] // shards, g.shape[1]) for g in grads]
    units = unit_list(shapes)
    chunks, chunk_rows = len(units) // pack, UNIT_ROWS * pack
    dma = pltpu.SemaphoreType.DMA
    flips = 2 + replicas.bit_length() - 1
    part_shapes = []
    rows, columns = chunk_rows, UNIT_COLS
    for level, (members, _) in enumerate(factors):
        if level == levels - 1:
            rows, columns = rows // 2, columns // 2
        else:
            rows = rows // members
        part_shapes.append((chunks, members - 1, rows, columns))
    counts = [(chunks, members - 1) for members, _ in factors]
    out, gain_out = pl.pallas_call(
        functools.partial(reduce_kernel, factors, pack, units, [s[0] for s in shapes]),
        out_shape=(
            jax.ShapeDtypeStruct((chunks, chunk_rows, UNIT_COLS), BF16),
            jax.ShapeDtypeStruct(gain_sums.shape, F32),
        ),
        in_specs=[pl.BlockSpec(memory_space=pl.ANY)] * len(grads)
        + [pl.BlockSpec(memory_space=pltpu.VMEM)],
        out_specs=[
            pl.BlockSpec(memory_space=pl.ANY),
            pl.BlockSpec(memory_space=pltpu.VMEM),
        ],
        scratch_shapes=[
            pltpu.VMEM((chunks, 2, chunk_rows, UNIT_COLS), BF16),
            pltpu.VMEM((chunks, 2, chunk_rows, UNIT_COLS), BF16),
            pltpu.VMEM((chunks, chunk_rows, UNIT_COLS), BF16),
            pltpu.VMEM((chunks, chunk_rows, UNIT_COLS), BF16),
            pltpu.VMEM((flips - 1,) + gain_sums.shape, F32),
            pltpu.VMEM((flips,) + gain_sums.shape, F32),
        ]
        + [pltpu.VMEM(shape, BF16) for shape in part_shapes]
        + [
            dma((chunks, 2, pack)),
            dma((chunks, 2, pack)),
            dma((chunks, 2, pack)),
            dma((chunks,)),
            dma((chunks,)),
            dma((chunks,)),
            dma((flips,)),
            dma((flips,)),
        ]
        + [dma(shape) for _ in range(4) for shape in counts],
        compiler_params=pltpu.CompilerParams(
            collective_id=1, has_side_effects=True, vmem_limit_bytes=48 * 1024 * 1024
        ),
        name="reduce_grads",
    )(*grads, gain_sums)
    return out.reshape(len(units), UNIT_ROWS, UNIT_COLS), gain_out


def rms_scale(values):
    return lax.rsqrt(jnp.mean(values * values, axis=-1, keepdims=True) + EPSILON)


def rotation(positions, head_size):
    half_size = head_size // 2
    steps_range = jnp.arange(half_size, dtype=jnp.float32)
    frequency = jnp.exp(steps_range * (-2.0 * math.log(ROPE_BASE) / head_size))
    angles = positions.astype(jnp.float32)[:, None] * frequency[None, :]
    return (jnp.cos(angles), jnp.sin(angles))


def rotate(values, cosine_table, sine_table):
    half_size = cosine_table.shape[1]
    shaped = values.reshape(values.shape[0], -1, 2 * half_size)
    first_half = shaped[..., :half_size]
    second_half = shaped[..., half_size:]
    cos_rows = cosine_table[:, None, :]
    sin_rows = sine_table[:, None, :]
    turned = jnp.concatenate(
        [
            first_half * cos_rows - second_half * sin_rows,
            second_half * cos_rows + first_half * sin_rows,
        ],
        axis=-1,
    )
    return turned.reshape(values.shape)


def rotate_back(values, cosine_table, sine_table):
    half_size = cosine_table.shape[1]
    shaped = values.reshape(values.shape[0], -1, 2 * half_size)
    first_half = shaped[..., :half_size]
    second_half = shaped[..., half_size:]
    cos_rows = cosine_table[:, None, :]
    sin_rows = sine_table[:, None, :]
    turned = jnp.concatenate(
        [
            first_half * cos_rows + second_half * sin_rows,
            second_half * cos_rows - first_half * sin_rows,
        ],
        axis=-1,
    )
    return turned.reshape(values.shape)


def sequence_mask(lengths, assignment, device, slot_count):
    owned_lengths = jnp.where(assignment == device, lengths, 0)
    seq_ends = jnp.cumsum(owned_lengths)
    slot_ids = jnp.arange(slot_count, dtype=jnp.int32)
    labels = jnp.sum((seq_ends[None, :] <= slot_ids[:, None]).astype(jnp.int32), axis=1)
    allowed = (labels[:, None] == labels[None, :]) & (slot_ids[None, :] <= slot_ids[:, None])
    valid_rows = (slot_ids < seq_ends[-1]).astype(jnp.float32)[:, None]
    return (allowed, valid_rows)


def by_group(values, groups):
    return jnp.moveaxis(values.reshape(values.shape[0], groups, -1, HDIM), 1, 0)


def from_group(values):
    moved = jnp.moveaxis(values, 0, 1)
    return moved.reshape(moved.shape[0], -1)


def norm_back(grad_normed, values, scale_rows, gain):
    scaled_grad = gain * grad_normed
    gain_grad = jnp.sum(grad_normed * values * scale_rows, axis=0)
    grad_values = scale_rows * scaled_grad - values * scale_rows**3 * jnp.mean(
        scaled_grad * values, axis=-1, keepdims=True
    )
    return (gain_grad, grad_values)


def per_device(
    tokens,
    cotangent,
    lengths,
    assignment,
    positions,
    attention_gain,
    query_weight,
    key_weight,
    value_weight,
    out_weight,
    feedforward_gain,
    gate_weight,
    up_weight,
    down_weight,
):
    slot_count = tokens.shape[0]
    heads_per = math.gcd(HEADS, 4)
    groups = HEADS // heads_per
    inv_root = 1.0 / math.sqrt(HDIM)
    device = lax.axis_index("shard") * lax.axis_size("replica") + lax.axis_index("replica")
    allowed, valid_rows = sequence_mask(lengths, assignment, device, slot_count)
    cosine_table, sine_table = rotation(positions, HDIM)
    width = tokens.shape[1]
    inner = gate_weight.shape[1]
    gain_rows = jnp.zeros((16, 256), BF16)
    gain_rows = gain_rows.at[0, : attention_gain.shape[0]].set(attention_gain)
    gain_rows = gain_rows.at[1, : feedforward_gain.shape[0]].set(feedforward_gain)
    w_qkv, w_out, w_gate_up, w_down, gains = gather_weights(
        [query_weight, key_weight, value_weight, out_weight, gate_weight, up_weight, down_weight],
        gain_rows,
    )
    gain_one = gains[:, 0, : attention_gain.shape[0]].reshape(-1)
    gain_two = gains[:, 1, : feedforward_gain.shape[0]].reshape(-1)
    values = tokens.astype(jnp.float32)
    scale_one = rms_scale(values)
    normed = (values * scale_one * gain_one.astype(jnp.float32)).astype(jnp.bfloat16)
    qkv = jnp.dot(normed, w_qkv, preferred_element_type=jnp.float32)
    query_lin, key_lin = qkv[:, :width], qkv[:, width : 2 * width]
    value_low = qkv[:, 2 * width :].astype(jnp.bfloat16)
    query_rot = rotate(query_lin, cosine_table, sine_table).astype(jnp.bfloat16)
    key_rot = rotate(key_lin, cosine_table, sine_table).astype(jnp.bfloat16)
    query_groups = by_group(query_rot, groups)
    key_groups = by_group(key_rot, groups)
    value_groups = by_group(value_low, groups)

    def attend(group_in):
        query_part, key_part, value_part = group_in
        scores = (
            jnp.einsum("qhd,khd->hqk", query_part, key_part, preferred_element_type=jnp.float32)
            * inv_root
        )
        scores = jnp.where(allowed[None], scores, -jnp.inf)
        row_peak = jnp.max(scores, axis=-1, keepdims=True)
        exponent = jnp.exp(scores - row_peak)
        row_total = jnp.sum(exponent, axis=-1, keepdims=True)
        probability = (exponent / row_total).astype(jnp.bfloat16)
        mixed_values = jnp.einsum(
            "hqk,khd->qhd", probability, value_part, preferred_element_type=jnp.float32
        )
        return (mixed_values, row_peak[..., 0] + jnp.log(row_total[..., 0]))

    mixed_groups, log_totals = lax.map(attend, (query_groups, key_groups, value_groups))
    attended = from_group(mixed_groups).astype(jnp.bfloat16)
    hidden_one = values + jnp.dot(attended, w_out, preferred_element_type=jnp.float32)
    scale_two = rms_scale(hidden_one)
    normed_two = (hidden_one * scale_two * gain_two.astype(jnp.float32)).astype(jnp.bfloat16)
    gate_up = jnp.dot(normed_two, w_gate_up, preferred_element_type=jnp.float32)
    gate, upward = gate_up[:, :inner], gate_up[:, inner:]
    sigmoid_gate = jax.nn.sigmoid(gate)
    activated = gate * sigmoid_gate
    hidden = (activated * upward).astype(jnp.bfloat16)
    branch_two = jnp.dot(hidden, w_down, preferred_element_type=jnp.float32)
    output = ((hidden_one + branch_two) * valid_rows).astype(jnp.bfloat16)
    grad_out = cotangent.astype(jnp.float32) * valid_rows
    grad_branch_two = grad_out.astype(jnp.bfloat16)
    grad_down = jnp.einsum(
        "nf,nd->fd", hidden, grad_branch_two, preferred_element_type=jnp.float32
    ).astype(BF16)
    grad_hidden = jnp.einsum(
        "nd,fd->nf", grad_branch_two, w_down, preferred_element_type=jnp.float32
    )
    grad_gate = (grad_hidden * upward * sigmoid_gate * (1.0 + gate * (1.0 - sigmoid_gate))).astype(
        jnp.bfloat16
    )
    grad_up = (grad_hidden * activated).astype(jnp.bfloat16)
    grad_gate_weight = jnp.einsum(
        "nd,nf->df", normed_two, grad_gate, preferred_element_type=jnp.float32
    ).astype(BF16)
    grad_up_weight = jnp.einsum(
        "nd,nf->df", normed_two, grad_up, preferred_element_type=jnp.float32
    ).astype(BF16)
    grad_normed_two = jnp.einsum(
        "nf,df->nd", grad_gate, w_gate_up[:, :inner], preferred_element_type=jnp.float32
    ) + jnp.einsum("nf,df->nd", grad_up, w_gate_up[:, inner:], preferred_element_type=jnp.float32)
    grad_gain_two, grad_norm_two = norm_back(
        grad_normed_two, hidden_one, scale_two, gain_two.astype(jnp.float32)
    )
    grad_hidden_one = grad_out + grad_norm_two
    grad_branch_one = grad_hidden_one.astype(jnp.bfloat16)
    grad_out_weight = jnp.einsum(
        "nd,ne->de", attended, grad_branch_one, preferred_element_type=jnp.float32
    ).astype(BF16)
    grad_attended = jnp.einsum(
        "ne,de->nd", grad_branch_one, w_out, preferred_element_type=jnp.float32
    ).astype(jnp.bfloat16)
    grad_groups = by_group(grad_attended, groups)

    def attend_back(group_in):
        query_part, key_part, value_part, grad_part, log_total = group_in
        scores = (
            jnp.einsum("qhd,khd->hqk", query_part, key_part, preferred_element_type=jnp.float32)
            * inv_root
        )
        scores = jnp.where(allowed[None], scores, -jnp.inf)
        probability = jnp.exp(scores - log_total[..., None])
        probability_low = probability.astype(jnp.bfloat16)
        grad_value = jnp.einsum(
            "hqk,qhd->khd", probability_low, grad_part, preferred_element_type=jnp.float32
        )
        grad_probability = jnp.einsum(
            "qhd,khd->hqk", grad_part, value_part, preferred_element_type=jnp.float32
        )
        row_dot = jnp.sum(probability * grad_probability, axis=-1, keepdims=True)
        grad_scores = (probability * (grad_probability - row_dot)).astype(jnp.bfloat16)
        grad_query = (
            jnp.einsum("hqk,khd->qhd", grad_scores, key_part, preferred_element_type=jnp.float32)
            * inv_root
        )
        grad_key = (
            jnp.einsum("hqk,qhd->khd", grad_scores, query_part, preferred_element_type=jnp.float32)
            * inv_root
        )
        return (grad_query, grad_key, grad_value)

    grad_query_groups, grad_key_groups, grad_value_groups = lax.map(
        attend_back, (query_groups, key_groups, value_groups, grad_groups, log_totals)
    )
    grad_query_lin = rotate_back(from_group(grad_query_groups), cosine_table, sine_table).astype(
        jnp.bfloat16
    )
    grad_key_lin = rotate_back(from_group(grad_key_groups), cosine_table, sine_table).astype(
        jnp.bfloat16
    )
    grad_value_lin = from_group(grad_value_groups).astype(jnp.bfloat16)
    grad_query_weight = jnp.einsum(
        "nd,ne->de", normed, grad_query_lin, preferred_element_type=jnp.float32
    ).astype(BF16)
    grad_key_weight = jnp.einsum(
        "nd,ne->de", normed, grad_key_lin, preferred_element_type=jnp.float32
    ).astype(BF16)
    grad_value_weight = jnp.einsum(
        "nd,ne->de", normed, grad_value_lin, preferred_element_type=jnp.float32
    ).astype(BF16)
    grad_normed = jnp.einsum(
        "ne,de->nd", grad_query_lin, w_qkv[:, 0 * width : 1 * width], preferred_element_type=jnp.float32
    )
    grad_normed = grad_normed + jnp.einsum(
        "ne,de->nd", grad_key_lin, w_qkv[:, 1 * width : 2 * width], preferred_element_type=jnp.float32
    )
    grad_normed = grad_normed + jnp.einsum(
        "ne,de->nd", grad_value_lin, w_qkv[:, 2 * width : 3 * width], preferred_element_type=jnp.float32
    )
    grad_gain_one, grad_norm_one = norm_back(
        grad_normed, values, scale_one, gain_one.astype(jnp.float32)
    )
    input_grad = grad_hidden_one + grad_norm_one
    gain_sums = jnp.concatenate(
        [grad_gain_one[None], grad_gain_two[None], jnp.zeros((6, width), F32)], axis=0
    )
    sums, gain_sums = reduce_grads(
        [
            grad_down,
            grad_gate_weight,
            grad_up_weight,
            grad_out_weight,
            grad_query_weight,
            grad_key_weight,
            grad_value_weight,
        ],
        gain_sums,
    )
    sums = sums.astype(F32)
    blocks = inner // UNIT_COLS
    down_sum = sums[:blocks].reshape(-1, width)
    gate_sum = jnp.concatenate([sums[blocks + j] for j in range(blocks)], axis=1)
    up_sum = jnp.concatenate([sums[2 * blocks + j] for j in range(blocks)], axis=1)
    out_sum, query_sum, key_sum, value_sum = (sums[3 * blocks + j] for j in range(4))
    share = attention_gain.shape[0]
    my_gains = lax.dynamic_slice(gain_sums, (0, lax.axis_index("shard") * share), (2, share))
    return (
        output,
        input_grad,
        my_gains[0],
        query_sum,
        key_sum,
        value_sum,
        out_sum,
        my_gains[1],
        gate_sum,
        up_sum,
        down_sum,
    )


def solution(mesh):
    return jax.shard_map(
        per_device,
        mesh=mesh,
        in_specs=(
            P(("shard", "replica"), None),
            P(("shard", "replica"), None),
            P(),
            P(),
            P(("shard", "replica")),
            P("shard"),
            P("shard", None),
            P("shard", None),
            P("shard", None),
            P("shard", None),
            P("shard"),
            P("shard", None),
            P("shard", None),
            P("shard", None),
        ),
        out_specs=(
            P(("shard", "replica"), None),
            P(("shard", "replica"), None),
            P("shard"),
            P("shard", None),
            P("shard", None),
            P("shard", None),
            P("shard", None),
            P("shard"),
            P("shard", None),
            P("shard", None),
            P("shard", None),
        ),
        check_vma=False,
    )
```

```python
import functools
import math

import jax
import jax.numpy as jnp
from jax import lax
from jax.experimental import pallas as pl
from jax.experimental.pallas import tpu as pltpu
from jax.sharding import PartitionSpec as P

HEADS = 12
HDIM = 64
EPSILON = 1e-05
ROPE_BASE = 10000.0
MESH = pl.DeviceIdType.MESH
F32 = jnp.float32
BF16 = jnp.bfloat16
DMA = pltpu.SemaphoreType.DMA

ROWS = 192
COLS = 768
UNITS = 16
FBLOCKS = 4
SHARDS = 4
TILE = 256


def toggle(index, stride):
    return index + (1 - 2 * ((index // stride) % 2)) * stride


def ring(index, members, stride):
    place = (index // stride) % members
    base = index - place * stride
    return place, [base + ((place + step) % members) * stride for step in range(1, members)]


def at(shard, replica):
    return {"shard": shard, "replica": replica}


def greet(peers):
    barrier = pltpu.get_barrier_semaphore()
    for peer in peers:
        pl.semaphore_signal(barrier, inc=1, device_id=peer, device_id_type=MESH)
    pl.semaphore_wait(barrier, len(peers))


def remote(source, target, send, receive, peer):
    return pltpu.make_async_remote_copy(
        src_ref=source,
        dst_ref=target,
        send_sem=send,
        recv_sem=receive,
        device_id=peer,
        device_id_type=MESH,
    )


def mult(start, step):
    return start if isinstance(start, int) else pl.multiple_of(start, step)


def span(start, size, step=16):
    return pl.ds(mult(start, step), size)


def replica_factors(count):
    if count == 8:
        return [(2, 1), (4, 2)], 1
    assert count == 32
    return [(2, 16), (4, 4), (4, 1)], 4


def dot(a, b):
    return jnp.dot(a, b, preferred_element_type=F32)


def dot_nt(a, b):
    return lax.dot_general(a, b, (((1,), (1,)), ((), ())), preferred_element_type=F32)


def dot_tn(a, b):
    return lax.dot_general(a, b, (((0,), (0,)), ((), ())), preferred_element_type=F32)


def flat(block):
    return block.reshape(-1, block.shape[-1])


def scale_of(values):
    return lax.rsqrt(jnp.mean(values * values, axis=-1, keepdims=True) + EPSILON)


def half_swap(values):
    lane = lax.broadcasted_iota(jnp.int32, values.shape, 1)
    return jnp.where(lane % 64 < 32, pltpu.roll(values, 96, 1), pltpu.roll(values, 32, 1))


def head_mask(which):
    lane = lax.broadcasted_iota(jnp.int32, (1, 128), 1)
    return jnp.where((lane < 64) == (which == 0), 1.0, 0.0).astype(BF16)


def norm_back(grad_normed, values, gain):
    scale = scale_of(values)
    scaled = gain * grad_normed
    gain_grad = jnp.sum(grad_normed * values * scale, axis=0, keepdims=True)
    mean = jnp.mean(scaled * values, axis=-1, keepdims=True)
    return gain_grad, scale * scaled - values * (scale * scale * scale) * mean


def forward_kernel(
    length, x_hbm, tables_hbm, gain_hbm, q_hbm, k_hbm, v_hbm, o_hbm, g_hbm, u_hbm, d_hbm,
    w_out, qkv_out, nt_out, n2t_out, at_out, ht_out, hid_out, a_out, b_out, h1_out, lse_out, gain_out,
    w, x, tables, gains, gain, normed, normed_t, qkv, bias, attended, lse, h1, ht, hid, a, b,
    load, x_out, x_in, y_out, y_in, p_out, p_in, f_out, f_in, g_out, g_in, w_store, store, f_store,
):
    shard, replica = lax.axis_index("shard"), lax.axis_index("replica")
    partner, across = toggle(shard, 1), toggle(shard, 2)
    opposite = toggle(across, 1)
    beside = toggle(replica, 1)
    side = replica % 2
    tokens, width = x.shape

    sources = [q_hbm, k_hbm, v_hbm, o_hbm]
    for block in range(FBLOCKS):
        columns = pl.ds(block * COLS, COLS)
        sources += [g_hbm.at[:, columns], u_hbm.at[:, columns]]
    sources += [d_hbm.at[pl.ds(piece * ROWS, ROWS)] for piece in range(UNITS - len(sources))]
    loads = [
        pltpu.make_async_copy(source, w.at[unit, shard], load.at[unit])
        for unit, source in enumerate(sources)
    ]
    x_load = pltpu.make_async_copy(x_hbm, x, load.at[UNITS])
    gain_load = pltpu.make_async_copy(gain_hbm, gains.at[shard], load.at[UNITS + 1])
    table_load = pltpu.make_async_copy(tables_hbm, tables, load.at[UNITS + 2])
    gain_load.start()
    for copy in loads:
        copy.start()
    x_load.start()
    table_load.start()

    shard_peers = [at(partner, replica), at(across, replica), at(opposite, replica)]
    greet(shard_peers + [at(shard, beside)])

    gain_load.wait()
    gain_copies = [
        remote(gains.at[shard], gains.at[shard], g_out.at[number], g_in.at[number], peer)
        for number, peer in enumerate(shard_peers)
    ]
    for copy in gain_copies:
        copy.start()

    half = ROWS // 2

    def part(unit, owner, which):
        return w.at[unit, owner, span(which * half, half)]

    def cross(unit):
        piece = part(unit, shard, side)
        return remote(piece, piece, x_out.at[unit], x_in.at[unit], at(across, replica))

    def share(unit):
        piece = w.at[unit, shard]
        return remote(piece, piece, p_out.at[unit], p_in.at[unit], at(partner, replica))

    def hand(unit):
        piece = part(unit, across, side)
        return remote(piece, piece, y_out.at[unit], y_in.at[unit], at(shard, beside))

    def forward(unit, number):
        piece = part(unit, across, side if number == 0 else 1 - side)
        return remote(piece, piece, f_out.at[number, unit], f_in.at[number, unit], at(partner, replica))

    def keep(unit):
        return pltpu.make_async_copy(w.at[unit], w_out.at[unit], w_store.at[unit])

    for unit in range(UNITS):
        loads[unit].wait()
        cross(unit).start()
        share(unit).start()

    def tick(time):
        @pl.when(time < UNITS)
        def _():
            cross(time).wait_recv()
            hand(time).start()
            forward(time, 0).start()

        @pl.when((time >= 1) & (time < UNITS + 1))
        def _():
            hand(time - 1).wait_recv()
            forward(time - 1, 1).start()

        @pl.when((time >= 2) & (time < UNITS + 2))
        def _():
            unit = time - 2
            share(unit).wait_recv()
            forward(unit, 0).wait_recv()
            forward(unit, 1).wait_recv()
            keep(unit).start()

    def ticks(first, last):
        def body(time, carry):
            tick(time)
            return carry

        lax.fori_loop(first, last, body, 0)

    stores = []

    def save(source, target):
        copy = pltpu.make_async_copy(source, target, store.at[len(stores)])
        copy.start()
        stores.append(copy)

    row = lax.broadcasted_iota(jnp.int32, (tokens, tokens), 0)
    column = lax.broadcasted_iota(jnp.int32, (tokens, tokens), 1)
    seen = (column <= row) & ((row < length[0]) | (column >= length[0]))
    bias[...] = jnp.where(seen, 0.0, -jnp.inf)

    x_load.wait()
    for copy in gain_copies:
        copy.wait_recv()
    gain[...] = gains[0] + gains[1] + gains[2] + gains[3]
    save(gain, gain_out)
    values = x[...].astype(F32)
    normed[...] = (values * scale_of(values) * gain[0:1]).astype(BF16)
    normed_t[0] = normed[...].T
    save(normed_t.at[0], nt_out)
    table_load.wait()
    ticks(0, 5)

    def project(step, carry):
        which, tile = step // (tokens // TILE), step % (tokens // TILE)
        rows = span(tile * TILE, TILE)
        product = dot(normed[rows], flat(w[which]))
        cosine = jnp.where(which < 2, tables[0, rows], 1.0)
        sine = jnp.where(which < 2, tables[1, rows], 0.0)
        for pair in range(width // 128):
            columns = slice(pair * 128, pair * 128 + 128)
            piece = product[:, columns]
            qkv[which, rows, columns] = (piece * cosine + half_swap(piece) * sine).astype(BF16)
        return carry

    lax.fori_loop(0, 3 * (tokens // TILE), project, 0)
    save(qkv, qkv_out)
    lse[...] = jnp.zeros_like(lse)

    def attend(pair, carry):
        columns = span(pair * 128, 128, 128)
        for tile in range(tokens // TILE):
            rows = pl.ds(tile * TILE, TILE)
            keys = (tile + 1) * TILE
            query = qkv[0, rows, columns]
            key = qkv[1, 0:keys, columns]
            value = qkv[2, 0:keys, columns]
            mixed = []
            logs = lse[rows]
            lane = lax.broadcasted_iota(jnp.int32, logs.shape, 1)
            for which in range(2):
                scores = dot_nt(query * head_mask(which), key) * (1.0 / math.sqrt(HDIM))
                scores = scores + bias[rows, 0:keys]
                peak = jnp.max(scores, axis=-1, keepdims=True)
                exponent = jnp.exp(scores - peak)
                total = jnp.sum(exponent, axis=-1, keepdims=True)
                probability = (exponent * (1.0 / total)).astype(BF16)
                mixed.append(dot(probability, value))
                logs = jnp.where(lane == 2 * pair + which, peak + jnp.log(total), logs)
            lse[rows] = logs
            first = lax.broadcasted_iota(jnp.int32, mixed[0].shape, 1) < 64
            attended[rows, columns] = jnp.where(first, mixed[0], mixed[1]).astype(BF16)
        tick(5 + pair)
        return carry

    lax.fori_loop(0, HEADS // 2, attend, 0)
    normed_t[1] = attended[...].T
    save(normed_t.at[1], at_out)
    save(lse, lse_out)
    for tile in range(tokens // TILE):
        rows = pl.ds(tile * TILE, TILE)
        hidden_one = x[rows].astype(F32) + dot(attended[rows], flat(w[3]))
        h1[rows] = hidden_one
        normed[rows] = (hidden_one * scale_of(hidden_one) * gain[1:2]).astype(BF16)
    save(h1, h1_out)
    normed_t[2] = normed[...].T
    save(normed_t.at[2], n2t_out)

    def f_copies(block):
        pairs = [
            (hid.at[block], hid_out.at[block]),
            (a.at[block], a_out.at[block]),
            (b.at[block], b_out.at[block]),
            (ht.at[:, block], ht_out.at[:, block]),
        ]
        return [
            pltpu.make_async_copy(source, target, f_store.at[block, number])
            for number, (source, target) in enumerate(pairs)
        ]

    def feed(block, carry):
        def rows_of(tile, inner):
            rows = span(tile * TILE, TILE)
            gate = dot(normed[rows], flat(w[4 + 2 * block]))
            upward = dot(normed[rows], flat(w[5 + 2 * block]))
            sigmoid = jax.nn.sigmoid(gate)
            activated = gate * sigmoid
            hid[block, rows] = (activated * upward).astype(BF16)
            a[block, rows] = (upward * sigmoid * (1.0 + gate * (1.0 - sigmoid))).astype(BF16)
            b[block, rows] = activated.astype(BF16)
            return inner

        lax.fori_loop(0, tokens // TILE, rows_of, 0)
        turned = hid[block].T
        for piece in range(FBLOCKS):
            ht[piece, block] = turned[piece * ROWS : (piece + 1) * ROWS]
        for copy in f_copies(block):
            copy.start()
        tick(11 + block)
        return carry

    lax.fori_loop(0, FBLOCKS, feed, 0)
    ticks(11 + FBLOCKS, UNITS + 2)

    def settle(unit, carry):
        cross(unit).wait_send()
        share(unit).wait_send()
        hand(unit).wait_send()
        forward(unit, 0).wait_send()
        forward(unit, 1).wait_send()
        keep(unit).wait()
        return carry

    lax.fori_loop(0, UNITS, settle, 0)
    for copy in gain_copies:
        copy.wait_send()
    for copy in stores:
        copy.wait()
    for block in range(FBLOCKS):
        for copy in f_copies(block):
            copy.wait()


def forward_pass(length, tokens, tables, gain_rows, weights):
    count, width = tokens.shape
    shape = jax.ShapeDtypeStruct
    outs = (
        shape((UNITS, SHARDS, ROWS, COLS), BF16),
        shape((3, count, width), BF16),
        shape((width, count), BF16),
        shape((width, count), BF16),
        shape((width, count), BF16),
        shape((FBLOCKS, FBLOCKS, ROWS, count), BF16),
        shape((FBLOCKS, count, COLS), BF16),
        shape((FBLOCKS, count, COLS), BF16),
        shape((FBLOCKS, count, COLS), BF16),
        shape((count, width), F32),
        shape((count, 128), F32),
        shape(gain_rows.shape, F32),
    )
    anywhere = pl.BlockSpec(memory_space=pl.ANY)
    return pl.pallas_call(
        forward_kernel,
        out_shape=outs,
        in_specs=[pl.BlockSpec(memory_space=pltpu.SMEM)] + [anywhere] * 10,
        out_specs=[anywhere] * len(outs),
        scratch_shapes=[
            pltpu.VMEM((UNITS, SHARDS, ROWS, COLS), BF16),
            pltpu.VMEM((count, width), BF16),
            pltpu.VMEM(tables.shape, F32),
            pltpu.VMEM((SHARDS,) + gain_rows.shape, F32),
            pltpu.VMEM(gain_rows.shape, F32),
            pltpu.VMEM((count, width), BF16),
            pltpu.VMEM((3, width, count), BF16),
            pltpu.VMEM((3, count, width), BF16),
            pltpu.VMEM((count, count), F32),
            pltpu.VMEM((count, width), BF16),
            pltpu.VMEM((count, 128), F32),
            pltpu.VMEM((count, width), F32),
            pltpu.VMEM((FBLOCKS, FBLOCKS, ROWS, count), BF16),
            pltpu.VMEM((FBLOCKS, count, COLS), BF16),
            pltpu.VMEM((FBLOCKS, count, COLS), BF16),
            pltpu.VMEM((FBLOCKS, count, COLS), BF16),
            DMA((UNITS + 3,)),
            DMA((UNITS,)), DMA((UNITS,)), DMA((UNITS,)), DMA((UNITS,)), DMA((UNITS,)), DMA((UNITS,)),
            DMA((2, UNITS)), DMA((2, UNITS)), DMA((3,)), DMA((3,)),
            DMA((UNITS,)), DMA((8,)), DMA((FBLOCKS, 4)),
        ],
        compiler_params=pltpu.CompilerParams(
            collective_id=0, has_side_effects=True, vmem_limit_bytes=60 * 1024 * 1024
        ),
        name="forward_gather",
    )(length, tokens, tables, gain_rows, *weights)


def backward_kernel(
    factors, pack,
    length, x_hbm, cot_hbm, tables_hbm, gain_hbm, w_hbm, qkv_hbm, nt_hbm, n2t_hbm, at_hbm, ht_hbm,
    hid_hbm, a_hbm, b_hbm, h1_hbm, lse_hbm,
    sums_out, gain_out, output_out, grad_out,
    *refs,
):
    levels = len(factors)
    (grads, near, far, gain_sum, gain_got, x, gbt, gain, turned, h1, acc, result, out_low) = refs[:13]
    parts = refs[13 : 13 + levels]
    sems = refs[13 + levels :]
    load, s_load, near_out, near_in, far_out, far_in, store, gain_send, gain_recv = sems[:9]
    down_out, down_in, up_out, up_in = (
        sems[9 + kind * levels : 9 + (kind + 1) * levels] for kind in range(4)
    )
    shard, replica = lax.axis_index("shard"), lax.axis_index("replica")
    partner, across = toggle(shard, 1), toggle(shard, 2)
    opposite = toggle(across, 1)
    tokens, width = x.shape
    groups = [ring(replica, members, stride) for members, stride in factors]
    flips = [at(partner, replica), at(across, replica)]
    stride, replicas = 1, math.prod(members for members, _ in factors)
    while stride < replicas:
        flips.append(at(shard, toggle(replica, stride)))
        stride *= 2

    def fetch(source, target, number):
        copy = pltpu.make_async_copy(source, target, load.at[number])
        copy.start()
        return copy

    cot_load = fetch(cot_hbm, gbt, 0)
    n2t_load = fetch(n2t_hbm, turned.at[0], 1)
    h1_load = fetch(h1_hbm, h1, 2)
    x_load = fetch(x_hbm, x, 3)
    gain_load = fetch(gain_hbm, gain, 4)
    at_load = fetch(at_hbm, turned.at[1], 5)
    nt_load = fetch(nt_hbm, turned.at[2], 6)

    greet(
        [at(partner, replica), at(across, replica)]
        + [at(shard, other) for _, others in groups for other in others]
    )

    chunks = UNITS // pack

    def region(chunk, places):
        unit, units, row, rows, column, columns = chunk * pack, pack, 0, ROWS, 0, COLS
        for level, place in enumerate(places):
            if level == levels - 1:
                rows, columns = rows // 2, columns // 2
                row = row + (place // 2) * rows
                column = column + (place % 2) * columns
                continue
            members = factors[level][0]
            by_unit = math.gcd(units, members)
            by_row = members // by_unit
            units, rows = units // by_unit, rows // by_row
            unit = unit + (place // by_row) * units
            row = row + (place % by_row) * rows
        return pl.ds(unit, units), span(row, rows), span(column, columns, 128)

    my_places = [place for place, _ in groups]

    def view(owner, chunk, places):
        units, rows, columns = region(chunk, places)
        return grads.at[units, owner, rows, columns]

    def near_copy(unit, which):
        return remote(
            grads.at[unit, opposite if which == 0 else partner],
            near.at[unit, which],
            near_out.at[unit, which],
            near_in.at[unit, which],
            at(partner, replica),
        )

    def far_copy(unit):
        return remote(
            grads.at[unit, across], far.at[unit], far_out.at[unit], far_in.at[unit], at(across, replica)
        )

    def down_copy(level, chunk, step):
        members = factors[level][0]
        place, others = groups[level]
        theirs = (place + step + 1) % members
        return remote(
            view(shard, chunk, my_places[:level] + [theirs]),
            parts[level].at[chunk, step],
            down_out[level].at[chunk, step],
            down_in[level].at[chunk, step],
            at(shard, others[step]),
        )

    def up_copy(level, chunk, step):
        piece = view(partner, chunk, my_places[: level + 1])
        return remote(
            piece,
            piece,
            up_out[level].at[chunk, step],
            up_in[level].at[chunk, step],
            at(shard, groups[level][1][step]),
        )

    def store_copy(chunk):
        units = pl.ds(chunk * pack, pack)
        return pltpu.make_async_copy(grads.at[units, partner], sums_out.at[units], store.at[chunk])

    def over(level, act):
        for step in range(factors[level][0] - 1):
            act(step)

    def give(unit):
        for which in range(2):
            near_copy(unit, which).start()

    def plus(*terms):
        total = terms[0].astype(F32)
        for term in terms[1:]:
            total = total + term.astype(F32)
        return total.astype(BF16)

    def take_near(unit):
        near_copy(unit, 0).wait_recv()
        grads[unit, across] = plus(grads[unit, across], near[unit, 0])
        far_copy(unit).start()
        near_copy(unit, 1).wait_recv()
        grads[unit, shard] = plus(grads[unit, shard], near[unit, 1])

    def take_far(chunk):
        for piece in range(pack):
            unit = chunk * pack + piece
            near_copy(unit, 0).wait_send()
            near_copy(unit, 1).wait_send()
            far_copy(unit).wait_recv()
            grads[unit, shard] = plus(grads[unit, shard], far[unit])
        over(0, lambda step: down_copy(0, chunk, step).start())

    def take_down(level, chunk):
        over(level, lambda step: down_copy(level, chunk, step).wait_recv())
        places = my_places[: level + 1]
        terms = [view(shard, chunk, places)[...]]
        terms += [parts[level][chunk, step] for step in range(factors[level][0] - 1)]
        total = plus(*terms)
        if level + 1 < levels:
            view(shard, chunk, places)[...] = total
            over(level + 1, lambda step: down_copy(level + 1, chunk, step).start())
        else:
            view(partner, chunk, places)[...] = total
            over(level, lambda step: up_copy(level, chunk, step).start())

    def take_up(level, chunk):
        over(level, lambda step: up_copy(level, chunk, step).wait_recv())
        if level > 0:
            over(level - 1, lambda step: up_copy(level - 1, chunk, step).start())
        else:
            store_copy(chunk).start()

    stages = [take_far]
    stages += [functools.partial(take_down, level) for level in range(levels)]
    stages += [functools.partial(take_up, level) for level in reversed(range(levels))]
    last_post = pack * (chunks + len(stages) - 1)

    def post(time):
        step = (time + 1) // pack - 1
        for lag, stage in enumerate(stages):
            good = (step >= lag) & (step < chunks + lag) & ((time + 1) % pack == 0)
            pl.when(good)(functools.partial(stage, step - lag))

    def posts(first, last):
        def body(time, carry):
            post(time)
            return carry

        lax.fori_loop(first, last, body, 0)

    def gain_copy(step):
        return remote(
            gain_sum.at[step], gain_got.at[step], gain_send.at[step], gain_recv.at[step], flips[step]
        )

    row = lax.broadcasted_iota(jnp.int32, (tokens, 1), 0)
    valid = jnp.where(row < length[0], 1.0, 0.0)

    def feed_forward(ht, down_w, gate_w, up_w, hid, a, b, grad_pair):
        def stream(block):
            slot = block % 2
            pairs = [
                (w_hbm.at[pl.ds(UNITS - FBLOCKS, FBLOCKS), block], down_w.at[slot]),
                (w_hbm.at[4 + 2 * block], gate_w.at[slot]),
                (w_hbm.at[5 + 2 * block], up_w.at[slot]),
                (hid_hbm.at[block], hid.at[slot]),
                (a_hbm.at[block], a.at[slot]),
                (b_hbm.at[block], b.at[slot]),
            ]
            return [
                pltpu.make_async_copy(source, target, s_load.at[slot, number])
                for number, (source, target) in enumerate(pairs)
            ]

        ht_load = fetch(ht_hbm, ht, 7)
        for copy in stream(0):
            copy.start()
        cot_load.wait()
        gbt[...] = (gbt[...].astype(F32) * valid).astype(BF16)
        ht_load.wait()

        def down_grads(unit, carry):
            for owner in range(SHARDS // 2):
                pair = pl.ds(2 * owner, 2)
                product = dot(flat(ht[unit, pair]), gbt[...]).astype(BF16)
                grads[unit, pair] = product.reshape(2, ROWS, COLS)
            give(unit)
            return carry

        lax.fori_loop(0, FBLOCKS, down_grads, 0)
        n2t_load.wait()
        acc[...] = jnp.zeros_like(acc)
        result[...] = jnp.zeros_like(result)

        def block_step(block, carry):
            slot = block % 2

            @pl.when(block + 1 < FBLOCKS)
            def _():
                for copy in stream(block + 1):
                    copy.start()

            for copy in stream(block):
                copy.wait()

            def rows_of(tile, inner):
                rows = span(tile * TILE, TILE)
                grad_hidden = dot_nt(gbt[rows], flat(down_w[slot]))
                grad_pair[0, rows] = (grad_hidden * a[slot, rows].astype(F32)).astype(BF16)
                grad_pair[1, rows] = (grad_hidden * b[slot, rows].astype(F32)).astype(BF16)
                return inner

            lax.fori_loop(0, tokens // TILE, rows_of, 0)
            pl.when(block == 0)(lambda: take_near(0))

            def kind_of(kind, inner):
                unit = FBLOCKS + 2 * block + kind
                for owner in range(SHARDS // 2):
                    pair = pl.ds(2 * owner, 2)
                    product = dot(
                        turned[0, pl.ds(2 * owner * ROWS, 2 * ROWS)], grad_pair[kind]
                    ).astype(BF16)
                    grads[unit, pair] = product.reshape(2, ROWS, COLS)
                give(unit)
                return inner

            lax.fori_loop(0, 2, kind_of, 0)

            @pl.when(block == 0)
            def _():
                for unit in range(1, FBLOCKS):
                    take_near(unit)

            def back_rows(tile, inner):
                rows = span(tile * TILE, TILE)
                acc[rows] += dot_nt(grad_pair[0, rows], flat(gate_w[slot])) + dot_nt(
                    grad_pair[1, rows], flat(up_w[slot])
                )
                result[rows] += dot(hid[slot, rows], flat(down_w[slot]))
                return inner

            lax.fori_loop(0, tokens // TILE, back_rows, 0)
            take_near(FBLOCKS + 2 * block)
            take_near(FBLOCKS + 2 * block + 1)
            post(block)
            return carry

        lax.fori_loop(0, FBLOCKS, block_step, 0)

    pl.run_scoped(
        feed_forward,
        pltpu.VMEM((FBLOCKS, FBLOCKS, ROWS, tokens), BF16),
        pltpu.VMEM((2, FBLOCKS, ROWS, COLS), BF16),
        pltpu.VMEM((2, SHARDS, ROWS, COLS), BF16),
        pltpu.VMEM((2, SHARDS, ROWS, COLS), BF16),
        pltpu.VMEM((2, tokens, COLS), BF16),
        pltpu.VMEM((2, tokens, COLS), BF16),
        pltpu.VMEM((2, tokens, COLS), BF16),
        pltpu.VMEM((2, tokens, COLS), BF16),
    )

    def attention(attn_w, tables, qkv, lse, bias, grad_attended, grad_qkv):
        w_load = fetch(w_hbm.at[pl.ds(0, 4)], attn_w, 8)
        qkv_load = fetch(qkv_hbm, qkv, 9)
        lse_load = fetch(lse_hbm, lse, 10)
        table_load = fetch(tables_hbm, tables, 11)
        h1_load.wait()
        gain_load.wait()

        gain_grad = jnp.zeros((1, width), F32)
        for tile in range(tokens // TILE):
            rows = pl.ds(tile * TILE, TILE)
            good = jnp.where(
                lax.broadcasted_iota(jnp.int32, (TILE, 1), 0) + tile * TILE < length[0], 1.0, 0.0
            )
            out_low[rows] = ((h1[rows] + result[rows]) * good).astype(BF16)
            gain_piece, back = norm_back(acc[rows], h1[rows], gain[1:2])
            gain_grad = gain_grad + gain_piece
            grad_one = gbt[rows].astype(F32) + back
            result[rows] = grad_one
            gbt[rows] = grad_one.astype(BF16)
        gain_sum[0] = jnp.zeros_like(gain_sum[0])
        gain_sum[0, 1:2] = gain_grad
        output_store = pltpu.make_async_copy(out_low, output_out, load.at[12])
        output_store.start()
        at_load.wait()
        for owner in range(SHARDS // 2):
            pair = pl.ds(2 * owner, 2)
            product = dot(turned[1, pl.ds(2 * owner * ROWS, 2 * ROWS)], gbt[...]).astype(BF16)
            grads[UNITS - 4, pair] = product.reshape(2, ROWS, COLS)
        give(UNITS - 4)
        w_load.wait()
        for tile in range(tokens // TILE):
            rows = pl.ds(tile * TILE, TILE)
            grad_attended[rows] = dot_nt(gbt[rows], flat(attn_w[3])).astype(BF16)
        take_near(UNITS - 4)
        post(FBLOCKS)

        key_row = lax.broadcasted_iota(jnp.int32, (tokens, tokens), 0)
        query_column = lax.broadcasted_iota(jnp.int32, (tokens, tokens), 1)
        seen = (key_row <= query_column) & ((query_column < length[0]) | (key_row >= length[0]))
        bias[...] = jnp.where(seen, 0.0, -jnp.inf)
        qkv_load.wait()
        lse_load.wait()
        table_load.wait()
        inv_root = 1.0 / math.sqrt(HDIM)

        def attend_back(pair, carry):
            columns = span(pair * 128, 128, 128)
            grad_key = [jnp.zeros((TILE, 128), F32) for _ in range(tokens // TILE)]
            grad_value = [jnp.zeros((TILE, 128), F32) for _ in range(tokens // TILE)]
            for tile in range(tokens // TILE):
                rows = pl.ds(tile * TILE, TILE)
                query = qkv[0, rows, columns]
                grad_mixed = grad_attended[rows, columns]
                grad_query = jnp.zeros((TILE, 128), F32)
                for which in range(2):
                    mask = head_mask(which)
                    query_one = query * mask
                    mixed_one = grad_mixed * mask
                    log_row = lse[2 * pair + which, :, rows]
                    probs, grad_probs = [], []
                    row_dot = jnp.zeros((1, TILE), F32)
                    for block in range(tile + 1):
                        keys = pl.ds(block * TILE, TILE)
                        scores = dot_nt(qkv[1, keys, columns], query_one) * inv_root
                        prob = jnp.exp(scores + bias[keys, rows] - log_row)
                        grad_value[block] += dot(prob.astype(BF16), mixed_one)
                        grad_prob = dot_nt(qkv[2, keys, columns], mixed_one)
                        row_dot = row_dot + jnp.sum(prob * grad_prob, axis=0, keepdims=True)
                        probs.append(prob)
                        grad_probs.append(grad_prob)
                    for block in range(tile + 1):
                        keys = pl.ds(block * TILE, TILE)
                        grad_scores = (probs[block] * (grad_probs[block] - row_dot)).astype(BF16)
                        grad_key[block] += dot(grad_scores, query_one)
                        grad_query += dot_tn(grad_scores, qkv[1, keys, columns] * mask)
                grad_query = grad_query * inv_root
                grad_query = grad_query * tables[0, rows] - half_swap(grad_query) * tables[1, rows]
                grad_qkv[0, rows, columns] = grad_query.astype(BF16)
            for block in range(tokens // TILE):
                keys = pl.ds(block * TILE, TILE)
                back = grad_key[block] * inv_root
                back = back * tables[0, keys] - half_swap(back) * tables[1, keys]
                grad_qkv[1, keys, columns] = back.astype(BF16)
                grad_qkv[2, keys, columns] = grad_value[block].astype(BF16)
            post(FBLOCKS + 1 + pair)
            return carry

        lax.fori_loop(0, HEADS // 2, attend_back, 0)
        nt_load.wait()

        def projection(which, carry):
            for owner in range(SHARDS // 2):
                pair = pl.ds(2 * owner, 2)
                product = dot(
                    turned[2, pl.ds(2 * owner * ROWS, 2 * ROWS)], grad_qkv[which]
                ).astype(BF16)
                grads[UNITS - 3 + which, pair] = product.reshape(2, ROWS, COLS)
            give(UNITS - 3 + which)
            return carry

        lax.fori_loop(0, 3, projection, 0)
        acc[...] = jnp.zeros_like(acc)

        def input_back(which, carry):
            for tile in range(tokens // TILE):
                rows = pl.ds(tile * TILE, TILE)
                acc[rows] += dot_nt(grad_qkv[which, rows], flat(attn_w[which]))
            take_near(UNITS - 3 + which)
            return carry

        lax.fori_loop(0, 3, input_back, 0)
        x_load.wait()
        gain_grad = jnp.zeros((1, width), F32)
        for tile in range(tokens // TILE):
            rows = pl.ds(tile * TILE, TILE)
            gain_piece, back = norm_back(acc[rows], x[rows].astype(F32), gain[0:1])
            gain_grad = gain_grad + gain_piece
            result[rows] = result[rows] + back
        gain_sum[0, 0:1] = gain_grad
        grad_store = pltpu.make_async_copy(result, grad_out, load.at[13])
        grad_store.start()
        output_store.wait()
        grad_store.wait()

    pl.run_scoped(
        attention,
        pltpu.VMEM((4, SHARDS, ROWS, COLS), BF16),
        pltpu.VMEM((2, tokens, 128), F32),
        pltpu.VMEM((3, tokens, width), BF16),
        pltpu.VMEM((HEADS, 1, tokens), F32),
        pltpu.VMEM((tokens, tokens), F32),
        pltpu.VMEM((tokens, width), BF16),
        pltpu.VMEM((3, tokens, width), BF16),
    )

    first = FBLOCKS + 1 + HEADS // 2
    gain_copy(0).start()

    def rest(time, carry):
        post(time)
        for step in range(len(flips)):

            @pl.when(time == first + 1 + step)
            def _():
                gain_copy(step).wait_recv()
                gain_sum[step + 1] = gain_sum[step] + gain_got[step]
                if step + 1 < len(flips):
                    gain_copy(step + 1).start()

        return carry

    assert first + 1 + len(flips) <= last_post
    lax.fori_loop(first, last_post, rest, 0)
    gain_out[...] = gain_sum[len(flips)]

    def settle(chunk, carry):
        for piece in range(pack):
            far_copy(chunk * pack + piece).wait_send()
        for level in range(levels):
            over(level, lambda step: down_copy(level, chunk, step).wait_send())
            over(level, lambda step: up_copy(level, chunk, step).wait_send())
        store_copy(chunk).wait()
        return carry

    lax.fori_loop(0, chunks, settle, 0)
    for step in range(len(flips)):
        gain_copy(step).wait_send()


def backward_pass(length, tokens, cotangent, tables, gain, saved):
    count, width = tokens.shape
    replicas = lax.axis_size("replica")
    factors, pack = replica_factors(replicas)
    levels = len(factors)
    chunks = UNITS // pack
    flips = 2 + replicas.bit_length() - 1
    part_shapes = []
    units, rows, columns = pack, ROWS, COLS
    for level, (members, _) in enumerate(factors):
        if level == levels - 1:
            rows, columns = rows // 2, columns // 2
        else:
            by_unit = math.gcd(units, members)
            units, rows = units // by_unit, rows // (members // by_unit)
        part_shapes.append((chunks, members - 1, units, rows, columns))
    counts = [(chunks, members - 1) for members, _ in factors]
    anywhere = pl.BlockSpec(memory_space=pl.ANY)
    shape = jax.ShapeDtypeStruct
    return pl.pallas_call(
        functools.partial(backward_kernel, factors, pack),
        out_shape=(
            shape((UNITS, ROWS, COLS), BF16),
            shape(gain.shape, F32),
            shape((count, width), BF16),
            shape((count, width), F32),
        ),
        in_specs=[pl.BlockSpec(memory_space=pltpu.SMEM)] + [anywhere] * (4 + len(saved)),
        out_specs=[anywhere, pl.BlockSpec(memory_space=pltpu.VMEM), anywhere, anywhere],
        scratch_shapes=[
            pltpu.VMEM((UNITS, SHARDS, ROWS, COLS), BF16),
            pltpu.VMEM((UNITS, 2, ROWS, COLS), BF16),
            pltpu.VMEM((UNITS, ROWS, COLS), BF16),
            pltpu.VMEM((flips + 1,) + gain.shape, F32),
            pltpu.VMEM((flips,) + gain.shape, F32),
            pltpu.VMEM((count, width), BF16),
            pltpu.VMEM((count, width), BF16),
            pltpu.VMEM(gain.shape, F32),
            pltpu.VMEM((3, width, count), BF16),
            pltpu.VMEM((count, width), F32),
            pltpu.VMEM((count, width), F32),
            pltpu.VMEM((count, width), F32),
            pltpu.VMEM((count, width), BF16),
        ]
        + [pltpu.VMEM(part, BF16) for part in part_shapes]
        + [
            DMA((14,)), DMA((2, 6)), DMA((UNITS, 2)), DMA((UNITS, 2)), DMA((UNITS,)), DMA((UNITS,)),
            DMA((chunks,)), DMA((flips,)), DMA((flips,)),
        ]
        + [DMA(count_) for _ in range(4) for count_ in counts],
        compiler_params=pltpu.CompilerParams(
            collective_id=1, has_side_effects=True, vmem_limit_bytes=67043328
        ),
        name="backward_reduce",
    )(length, tokens, cotangent, tables, gain, *saved)


def widen_kernel(units, *refs):
    outs, (low, wide, in_sem, out_sem) = refs[:7], refs[7:]
    down, gate, up, out, query, key, value = outs
    targets = [down.at[pl.ds(piece * ROWS, ROWS)] for piece in range(FBLOCKS)]
    for block in range(FBLOCKS):
        columns = pl.ds(block * COLS, COLS)
        targets += [gate.at[:, columns], up.at[:, columns]]
    targets += [out, query, key, value]
    ins = [
        pltpu.make_async_copy(units.at[unit], low.at[unit], in_sem.at[unit]) for unit in range(UNITS)
    ]
    puts = [
        pltpu.make_async_copy(wide.at[unit], target, out_sem.at[unit])
        for unit, target in enumerate(targets)
    ]
    for copy in ins:
        copy.start()
    for unit in range(UNITS):
        ins[unit].wait()
        wide[unit] = low[unit].astype(F32)
        puts[unit].start()
    for copy in puts:
        copy.wait()


def widen(units):
    shape = jax.ShapeDtypeStruct
    small, broad = shape((ROWS, COLS), F32), shape((ROWS, FBLOCKS * COLS), F32)
    anywhere = pl.BlockSpec(memory_space=pl.ANY)
    return pl.pallas_call(
        widen_kernel,
        out_shape=(shape((FBLOCKS * ROWS, COLS), F32), broad, broad, small, small, small, small),
        in_specs=[anywhere],
        out_specs=[anywhere] * 7,
        scratch_shapes=[
            pltpu.VMEM((UNITS, ROWS, COLS), BF16),
            pltpu.VMEM((UNITS, ROWS, COLS), F32),
            DMA((UNITS,)),
            DMA((UNITS,)),
        ],
        compiler_params=pltpu.CompilerParams(vmem_limit_bytes=24 * 1024 * 1024),
        name="widen",
    )(units)


def per_device(
    tokens, cotangent, lengths, assignment, positions, attention_gain, query_weight, key_weight,
    value_weight, out_weight, feedforward_gain, gate_weight, up_weight, down_weight,
):
    width = tokens.shape[1]
    share = attention_gain.shape[0]
    shard = lax.axis_index("shard")
    device = shard * lax.axis_size("replica") + lax.axis_index("replica")
    length = jnp.sum(jnp.where(assignment == device, lengths, 0)).reshape(1)

    half = HDIM // 2
    lane = jnp.arange(128)
    frequency = jnp.exp((lane % half).astype(F32) * (-2.0 * math.log(ROPE_BASE) / HDIM))
    angles = positions.astype(F32)[:, None] * frequency[None, :]
    sign = jnp.where(lane % HDIM < half, -1.0, 1.0)
    tables = jnp.stack([jnp.cos(angles), jnp.sin(angles) * sign[None, :]])

    gain_rows = jnp.stack([attention_gain, feedforward_gain]).astype(F32)
    gain_rows = lax.dynamic_update_slice(jnp.zeros((8, width), F32), gain_rows, (0, shard * share))

    w, qkv, nt, n2t, att, ht, hid, a, b, h1, lse, gain = forward_pass(
        length,
        tokens,
        tables,
        gain_rows,
        [query_weight, key_weight, value_weight, out_weight, gate_weight, up_weight, down_weight],
    )
    lse = lse[:, :HEADS].T.reshape(HEADS, 1, -1)
    sums, gain_sums, output, input_grad = backward_pass(
        length, tokens, cotangent, tables, gain, [w, qkv, nt, n2t, att, ht, hid, a, b, h1, lse]
    )
    down, gate, up, out, query, key, value = widen(sums)
    mine = lax.dynamic_slice(gain_sums, (0, shard * share), (2, share))
    return output, input_grad, mine[0], query, key, value, out, mine[1], gate, up, down


def solution(mesh):
    return jax.shard_map(
        per_device,
        mesh=mesh,
        in_specs=(
            P(("shard", "replica"), None),
            P(("shard", "replica"), None),
            P(),
            P(),
            P(("shard", "replica")),
            P("shard"),
            P("shard", None),
            P("shard", None),
            P("shard", None),
            P("shard", None),
            P("shard"),
            P("shard", None),
            P("shard", None),
            P("shard", None),
        ),
        out_specs=(
            P(("shard", "replica"), None),
            P(("shard", "replica"), None),
            P("shard"),
            P("shard", None),
            P("shard", None),
            P("shard", None),
            P("shard", None),
            P("shard"),
            P("shard", None),
            P("shard", None),
            P("shard", None),
        ),
        check_vma=False,
    )
```

```python
import functools
import math

import jax
import jax.numpy as jnp
from jax import lax
from jax.experimental import pallas as pl
from jax.experimental.pallas import tpu as pltpu
from jax.sharding import PartitionSpec as P

HEADS = 12
HDIM = 64
EPSILON = 1e-05
ROPE_BASE = 10000.0
MESH = pl.DeviceIdType.MESH
F32 = jnp.float32
BF16 = jnp.bfloat16
DMA = pltpu.SemaphoreType.DMA

ROWS = 192
COLS = 768
UNITS = 16
FBLOCKS = 4
SHARDS = 4
TILE = 256


def toggle(index, stride):
    return index + (1 - 2 * ((index // stride) % 2)) * stride


def ring(index, members, stride):
    place = (index // stride) % members
    base = index - place * stride
    return place, [base + ((place + step) % members) * stride for step in range(1, members)]


def at(shard, replica):
    return {"shard": shard, "replica": replica}


def greet(peers):
    barrier = pltpu.get_barrier_semaphore()
    for peer in peers:
        pl.semaphore_signal(barrier, inc=1, device_id=peer, device_id_type=MESH)
    pl.semaphore_wait(barrier, len(peers))


def remote(source, target, send, receive, peer):
    return pltpu.make_async_remote_copy(
        src_ref=source,
        dst_ref=target,
        send_sem=send,
        recv_sem=receive,
        device_id=peer,
        device_id_type=MESH,
    )


def mult(start, step):
    return start if isinstance(start, int) else pl.multiple_of(start, step)


def span(start, size, step=16):
    return pl.ds(mult(start, step), size)


def replica_factors(count):
    if count == 8:
        return [(2, 1), (4, 2)], 1
    assert count == 32
    return [(2, 16), (4, 4), (4, 1)], 4


def dot(a, b):
    return jnp.dot(a, b, preferred_element_type=F32)


def dot_nt(a, b):
    return lax.dot_general(a, b, (((1,), (1,)), ((), ())), preferred_element_type=F32)


def dot_tn(a, b):
    return lax.dot_general(a, b, (((0,), (0,)), ((), ())), preferred_element_type=F32)


def flat(block):
    return block.reshape(-1, block.shape[-1])


def scale_of(values):
    return lax.rsqrt(jnp.mean(values * values, axis=-1, keepdims=True) + EPSILON)


def half_swap(values):
    lane = lax.broadcasted_iota(jnp.int32, values.shape, 1)
    return jnp.where(lane % 64 < 32, pltpu.roll(values, 96, 1), pltpu.roll(values, 32, 1))


def head_mask(which):
    lane = lax.broadcasted_iota(jnp.int32, (1, 128), 1)
    return jnp.where((lane < 64) == (which == 0), 1.0, 0.0).astype(BF16)


def own_length(lengths, assignment, device):
    total = jnp.int32(0)
    for number in range(lengths.shape[0]):
        total = total + jnp.where(assignment[number] == device, lengths[number], 0)
    return total


def rotation(start, length, tokens):
    row = lax.broadcasted_iota(jnp.int32, (tokens, 128), 0)
    lane = lax.broadcasted_iota(jnp.int32, (1, 128), 1)
    half = HDIM // 2
    frequency = jnp.exp((lane % half).astype(F32) * (-2.0 * math.log(ROPE_BASE) / HDIM))
    angles = jnp.where(row < length, row + start, 0).astype(F32) * frequency
    return jnp.cos(angles), jnp.sin(angles) * jnp.where(lane % HDIM < half, -1.0, 1.0)


def norm_back(grad_normed, values, gain):
    scale = scale_of(values)
    scaled = gain * grad_normed
    gain_grad = jnp.sum(grad_normed * values * scale, axis=0, keepdims=True)
    mean = jnp.mean(scaled * values, axis=-1, keepdims=True)
    return gain_grad, scale * scaled - values * (scale * scale * scale) * mean


def forward_kernel(
    lengths, assignment, positions, x_hbm, gain_hbm, q_hbm, k_hbm, v_hbm, o_hbm, g_hbm, u_hbm, d_hbm,
    w_out, qkv_out, nt_out, n2t_out, at_out, ht_out, hid_out, a_out, b_out, h1_out, lse_out, gain_out,
    tables_out,
    w, x, tables, gains, gain, normed, normed_t, qkv, bias, attended, lse, lse_t, h1, ht, hid, a, b,
    load, x_out, x_in, y_out, y_in, z_out, z_in, d_out, d_in, p_out, p_in, f_out, f_in, g_out, g_in,
    w_store, store, f_store,
):
    shard, replica = lax.axis_index("shard"), lax.axis_index("replica")
    partner, across = toggle(shard, 1), toggle(shard, 2)
    opposite = toggle(across, 1)
    beside, behind = toggle(replica, 1), toggle(replica, 2)
    mine = replica % 4
    quarter_beside, quarter_behind = toggle(mine, 1), toggle(mine, 2)
    quarter_last = toggle(quarter_beside, 2)
    tokens, width = x.shape

    sources = [q_hbm, k_hbm, v_hbm, o_hbm]
    for block in range(FBLOCKS):
        columns = pl.ds(block * COLS, COLS)
        sources += [g_hbm.at[:, columns], u_hbm.at[:, columns]]
    sources += [d_hbm.at[pl.ds(piece * ROWS, ROWS)] for piece in range(UNITS - len(sources))]
    loads = [
        pltpu.make_async_copy(source, w.at[unit, shard], load.at[unit])
        for unit, source in enumerate(sources)
    ]
    x_load = pltpu.make_async_copy(x_hbm, x, load.at[UNITS])
    gain_load = pltpu.make_async_copy(gain_hbm, gains.at[shard], load.at[UNITS + 1])
    gain_load.start()
    for copy in loads:
        copy.start()
    x_load.start()

    shard_peers = [at(partner, replica), at(across, replica), at(opposite, replica)]
    greet(shard_peers + [at(shard, beside), at(shard, behind)])

    gain_load.wait()
    gain_copies = [
        remote(gains.at[shard], gains.at[shard], g_out.at[number], g_in.at[number], peer)
        for number, peer in enumerate(shard_peers)
    ]
    for copy in gain_copies:
        copy.start()

    quarter = ROWS // 4

    def part(unit, owner, which):
        return w.at[unit, owner, span(which * quarter, quarter)]

    def cross(unit):
        piece = part(unit, shard, mine)
        return remote(piece, piece, x_out.at[unit], x_in.at[unit], at(across, replica))

    def share(unit):
        piece = w.at[unit, shard]
        return remote(piece, piece, p_out.at[unit], p_in.at[unit], at(partner, replica))

    def hand_beside(unit):
        piece = part(unit, across, mine)
        return remote(piece, piece, y_out.at[unit], y_in.at[unit], at(shard, beside))

    def hand_behind(unit):
        piece = part(unit, across, mine)
        return remote(piece, piece, z_out.at[unit], z_in.at[unit], at(shard, behind))

    def hand_on(unit, odd):
        piece = part(unit, across, quarter_beside if odd else quarter_behind)
        peer = at(shard, behind if odd else beside)
        return remote(piece, piece, d_out.at[unit], d_in.at[unit], peer)

    def by_parity(unit, act):
        for odd in range(2):
            pl.when(unit % 2 == odd)(functools.partial(act, odd))

    def forward(unit, number):
        which = (mine, quarter_beside, quarter_behind, quarter_last)[number]
        piece = part(unit, across, which)
        return remote(piece, piece, f_out.at[number, unit], f_in.at[number, unit], at(partner, replica))

    def keep(unit):
        return pltpu.make_async_copy(w.at[unit], w_out.at[unit], w_store.at[unit])

    for unit in range(UNITS):
        loads[unit].wait()
        cross(unit).start()
        share(unit).start()

    def take_cross(unit):
        cross(unit).wait_recv()
        hand_beside(unit).start()
        hand_behind(unit).start()
        forward(unit, 0).start()

    def take_hands(unit):
        hand_behind(unit).wait_recv()
        hand_beside(unit).wait_recv()
        by_parity(unit, lambda odd: hand_on(unit, odd).start())
        forward(unit, 1).start()
        forward(unit, 2).start()

    def take_last(unit):
        by_parity(unit, lambda odd: hand_on(unit, odd).wait_recv())
        forward(unit, 3).start()

    def complete(unit):
        share(unit).wait_recv()
        for number in range(4):
            forward(unit, number).wait_recv()
        keep(unit).start()

    stages = [(0, take_cross), (2, take_hands), (4, take_last), (5, complete)]

    def tick(time):
        for lag, stage in stages:
            pl.when((time >= lag) & (time < UNITS + lag))(functools.partial(stage, time - lag))

    def ticks(first, last):
        def body(time, carry):
            tick(time)
            return carry

        lax.fori_loop(first, last, body, 0)

    stores = []

    def save(source, target):
        copy = pltpu.make_async_copy(source, target, store.at[len(stores)])
        copy.start()
        stores.append(copy)

    row = lax.broadcasted_iota(jnp.int32, (tokens, tokens), 0)
    column = lax.broadcasted_iota(jnp.int32, (tokens, tokens), 1)
    device = shard * lax.axis_size("replica") + replica
    length = own_length(lengths, assignment, device)
    seen = (column <= row) & ((row < length) | (column >= length))
    bias[...] = jnp.where(seen, 0.0, -jnp.inf)

    x_load.wait()
    for copy in gain_copies:
        copy.wait_recv()
    gain[...] = gains[0] + gains[1] + gains[2] + gains[3]
    save(gain, gain_out)
    values = x[...].astype(F32)
    normed[...] = (values * scale_of(values) * gain[0:1]).astype(BF16)
    normed_t[0] = normed[...].T
    save(normed_t.at[0], nt_out)
    tables[0], tables[1] = rotation(positions[0], length, tokens)
    save(tables, tables_out)
    ticks(0, 8)

    def project(step, carry):
        which, tile = step // (tokens // TILE), step % (tokens // TILE)
        rows = span(tile * TILE, TILE)
        product = dot(normed[rows], flat(w[which]))
        cosine = jnp.where(which < 2, tables[0, rows], 1.0)
        sine = jnp.where(which < 2, tables[1, rows], 0.0)
        for pair in range(width // 128):
            columns = slice(pair * 128, pair * 128 + 128)
            piece = product[:, columns]
            qkv[which, rows, columns] = (piece * cosine + half_swap(piece) * sine).astype(BF16)
        return carry

    lax.fori_loop(0, 3 * (tokens // TILE), project, 0)
    save(qkv, qkv_out)
    tick(8)
    lse[...] = jnp.zeros_like(lse)

    def attend(pair, carry):
        columns = span(pair * 128, 128, 128)
        for tile in range(tokens // TILE):
            rows = pl.ds(tile * TILE, TILE)
            keys = (tile + 1) * TILE
            query = qkv[0, rows, columns]
            key = qkv[1, 0:keys, columns]
            value = qkv[2, 0:keys, columns]
            mixed = []
            logs = lse[rows]
            lane = lax.broadcasted_iota(jnp.int32, logs.shape, 1)
            for which in range(2):
                scores = dot_nt(query * head_mask(which), key) * (1.0 / math.sqrt(HDIM))
                scores = scores + bias[rows, 0:keys]
                peak = jnp.max(scores, axis=-1, keepdims=True)
                exponent = jnp.exp(scores - peak)
                total = jnp.sum(exponent, axis=-1, keepdims=True)
                probability = (exponent * (1.0 / total)).astype(BF16)
                mixed.append(dot(probability, value))
                logs = jnp.where(lane == 2 * pair + which, peak + jnp.log(total), logs)
            lse[rows] = logs
            first = lax.broadcasted_iota(jnp.int32, mixed[0].shape, 1) < 64
            attended[rows, columns] = jnp.where(first, mixed[0], mixed[1]).astype(BF16)
        tick(9 + pair)
        return carry

    lax.fori_loop(0, HEADS // 2, attend, 0)
    normed_t[1] = attended[...].T
    save(normed_t.at[1], at_out)
    lse_t[...] = lse[...].T
    save(lse_t, lse_out)
    for tile in range(tokens // TILE):
        rows = pl.ds(tile * TILE, TILE)
        hidden_one = x[rows].astype(F32) + dot(attended[rows], flat(w[3]))
        h1[rows] = hidden_one
        normed[rows] = (hidden_one * scale_of(hidden_one) * gain[1:2]).astype(BF16)
    save(h1, h1_out)
    normed_t[2] = normed[...].T
    save(normed_t.at[2], n2t_out)

    def f_copies(block):
        pairs = [
            (hid.at[block], hid_out.at[block]),
            (a.at[block], a_out.at[block]),
            (b.at[block], b_out.at[block]),
            (ht.at[:, block], ht_out.at[:, block]),
        ]
        return [
            pltpu.make_async_copy(source, target, f_store.at[block, number])
            for number, (source, target) in enumerate(pairs)
        ]

    def feed(block, carry):
        def rows_of(tile, inner):
            rows = span(tile * TILE, TILE)
            gate = dot(normed[rows], flat(w[4 + 2 * block]))
            upward = dot(normed[rows], flat(w[5 + 2 * block]))
            sigmoid = jax.nn.sigmoid(gate)
            activated = gate * sigmoid
            hid[block, rows] = (activated * upward).astype(BF16)
            a[block, rows] = (upward * sigmoid * (1.0 + gate * (1.0 - sigmoid))).astype(BF16)
            b[block, rows] = activated.astype(BF16)
            return inner

        lax.fori_loop(0, tokens // TILE, rows_of, 0)
        turned = hid[block].T
        for piece in range(FBLOCKS):
            ht[piece, block] = turned[piece * ROWS : (piece + 1) * ROWS]
        for copy in f_copies(block):
            copy.start()
        tick(15 + block)
        return carry

    lax.fori_loop(0, FBLOCKS, feed, 0)
    ticks(15 + FBLOCKS, UNITS + 5)

    def settle(unit, carry):
        cross(unit).wait_send()
        share(unit).wait_send()
        hand_beside(unit).wait_send()
        hand_behind(unit).wait_send()
        by_parity(unit, lambda odd: hand_on(unit, odd).wait_send())
        for number in range(4):
            forward(unit, number).wait_send()
        keep(unit).wait()
        return carry

    lax.fori_loop(0, UNITS, settle, 0)
    for copy in gain_copies:
        copy.wait_send()
    for copy in stores:
        copy.wait()
    for block in range(FBLOCKS):
        for copy in f_copies(block):
            copy.wait()


def forward_pass(scalars, tokens, gain_rows, weights):
    count, width = tokens.shape
    shape = jax.ShapeDtypeStruct
    outs = (
        shape((UNITS, SHARDS, ROWS, COLS), BF16),
        shape((3, count, width), BF16),
        shape((width, count), BF16),
        shape((width, count), BF16),
        shape((width, count), BF16),
        shape((FBLOCKS, FBLOCKS, ROWS, count), BF16),
        shape((FBLOCKS, count, COLS), BF16),
        shape((FBLOCKS, count, COLS), BF16),
        shape((FBLOCKS, count, COLS), BF16),
        shape((count, width), F32),
        shape((128, count), F32),
        shape(gain_rows.shape, F32),
        shape((2, count, 128), F32),
    )
    anywhere = pl.BlockSpec(memory_space=pl.ANY)
    return pl.pallas_call(
        forward_kernel,
        out_shape=outs,
        in_specs=[pl.BlockSpec(memory_space=pltpu.SMEM)] * 3 + [anywhere] * 9,
        out_specs=[anywhere] * len(outs),
        scratch_shapes=[
            pltpu.VMEM((UNITS, SHARDS, ROWS, COLS), BF16),
            pltpu.VMEM((count, width), BF16),
            pltpu.VMEM((2, count, 128), F32),
            pltpu.VMEM((SHARDS,) + gain_rows.shape, F32),
            pltpu.VMEM(gain_rows.shape, F32),
            pltpu.VMEM((count, width), BF16),
            pltpu.VMEM((3, width, count), BF16),
            pltpu.VMEM((3, count, width), BF16),
            pltpu.VMEM((count, count), F32),
            pltpu.VMEM((count, width), BF16),
            pltpu.VMEM((count, 128), F32),
            pltpu.VMEM((128, count), F32),
            pltpu.VMEM((count, width), F32),
            pltpu.VMEM((FBLOCKS, FBLOCKS, ROWS, count), BF16),
            pltpu.VMEM((FBLOCKS, count, COLS), BF16),
            pltpu.VMEM((FBLOCKS, count, COLS), BF16),
            pltpu.VMEM((FBLOCKS, count, COLS), BF16),
            DMA((UNITS + 2,)),
        ]
        + [DMA((UNITS,))] * 10
        + [
            DMA((4, UNITS)), DMA((4, UNITS)), DMA((3,)), DMA((3,)),
            DMA((UNITS,)), DMA((8,)), DMA((FBLOCKS, 4)),
        ],
        compiler_params=pltpu.CompilerParams(
            collective_id=0, has_side_effects=True, vmem_limit_bytes=60 * 1024 * 1024
        ),
        name="forward_gather",
    )(*scalars, tokens, gain_rows, *weights)


def backward_kernel(
    factors, pack,
    early, lengths, assignment, x_hbm, cot_hbm, w_hbm, qkv_hbm, nt_hbm, n2t_hbm, at_hbm, ht_hbm,
    hid_hbm, a_hbm, b_hbm, h1_hbm, lse_hbm, gain_hbm, tables_hbm,
    sums_out, gain_out, output_out, grad_out,
    *refs,
):
    levels = len(factors)
    (grads, near, far, gain_sum, gain_got, x, gbt, gain, turned, h1, acc, result, out_low) = refs[:13]
    parts = refs[13 : 13 + levels]
    both = refs[13 + levels]
    sems = refs[14 + levels :]
    (load, s_load, near_out, near_in, far_out, far_in, store, gain_send, gain_recv) = sems[:9]
    both_out, both_in, ht_sem = sems[9:12]
    down_out, down_in, up_out, up_in = (
        sems[12 + kind * levels : 12 + (kind + 1) * levels] for kind in range(4)
    )
    shard, replica = lax.axis_index("shard"), lax.axis_index("replica")
    partner, across = toggle(shard, 1), toggle(shard, 2)
    opposite = toggle(across, 1)
    tokens, width = x.shape
    length = own_length(lengths, assignment, shard * lax.axis_size("replica") + replica)
    groups = [ring(replica, members, stride) for members, stride in factors]
    flips = [at(partner, replica), at(across, replica)]
    stride, replicas = 1, math.prod(members for members, _ in factors)
    while stride < replicas:
        flips.append(at(shard, toggle(replica, stride)))
        stride *= 2

    def fetch(source, target, number):
        copy = pltpu.make_async_copy(source, target, load.at[number])
        copy.start()
        return copy

    cot_load = fetch(cot_hbm, gbt, 0)
    n2t_load = fetch(n2t_hbm, turned.at[0], 1)
    h1_load = fetch(h1_hbm, h1, 2)
    x_load = fetch(x_hbm, x, 3)
    gain_load = fetch(gain_hbm, gain, 4)
    at_load = fetch(at_hbm, turned.at[1], 5)
    nt_load = fetch(nt_hbm, turned.at[2], 6)

    greet(
        [at(partner, replica), at(across, replica)]
        + [at(shard, other) for _, others in groups for other in others]
    )

    chunks = UNITS // pack

    def region(chunk, places):
        unit, units, row, rows, column, columns = chunk * pack, pack, 0, ROWS, 0, COLS
        for level, place in enumerate(places):
            if level == levels - 1:
                rows, columns = rows // 2, columns // 2
                row = row + (place // 2) * rows
                column = column + (place % 2) * columns
                continue
            members = factors[level][0]
            by_unit = math.gcd(units, members)
            by_row = members // by_unit
            units, rows = units // by_unit, rows // by_row
            unit = unit + (place // by_row) * units
            row = row + (place % by_row) * rows
        return pl.ds(unit, units), span(row, rows), span(column, columns, 128)

    my_places = [place for place, _ in groups]

    def view(owner, chunk, places):
        units, rows, columns = region(chunk, places)
        return grads.at[units, owner, rows, columns]

    def near_copy(unit, which):
        return remote(
            grads.at[unit, opposite if which == 0 else partner],
            near.at[unit, which],
            near_out.at[unit, which],
            near_in.at[unit, which],
            at(partner, replica),
        )

    def far_copy(unit):
        return remote(
            grads.at[unit, across], far.at[unit], far_out.at[unit], far_in.at[unit], at(across, replica)
        )

    def is_early(unit):
        return (unit >= early[0]) & (unit < early[1])

    def when_early(unit, act, otherwise):
        if early[0] == early[1]:
            otherwise()
            return
        pl.when(is_early(unit))(act)
        pl.when((unit < early[0]) | (unit >= early[1]))(otherwise)

    def kept_half(ref, unit):
        rows = ROWS // 2
        return ref.at[unit, span(my_places[0] * rows, rows)]

    def both_copy(unit, which):
        rows = ROWS // 2
        theirs = span((1 - my_places[0]) * rows, rows)
        return remote(
            grads.at[unit, across if which == 0 else shard, theirs],
            both.at[unit - early[0], which],
            both_out.at[unit - early[0], which],
            both_in.at[unit - early[0], which],
            at(shard, groups[0][1][0]),
        )

    def far_half(unit):
        rows = ROWS // 2
        return remote(
            grads.at[unit, across, span(my_places[0] * rows, rows)],
            kept_half(far, unit),
            far_out.at[unit],
            far_in.at[unit],
            at(across, replica),
        )

    def take_both(unit):
        rows = span(my_places[0] * (ROWS // 2), ROWS // 2)
        both_copy(unit, 0).wait_recv()
        grads[unit, across, rows] = plus(grads[unit, across, rows], both[unit - early[0], 0])
        far_half(unit).start()
        both_copy(unit, 1).wait_recv()
        grads[unit, shard, rows] = plus(grads[unit, shard, rows], both[unit - early[0], 1])

    def down_copy(level, chunk, step):
        members = factors[level][0]
        place, others = groups[level]
        theirs = (place + step + 1) % members
        return remote(
            view(shard, chunk, my_places[:level] + [theirs]),
            parts[level].at[chunk, step],
            down_out[level].at[chunk, step],
            down_in[level].at[chunk, step],
            at(shard, others[step]),
        )

    def up_copy(level, chunk, step):
        piece = view(partner, chunk, my_places[: level + 1])
        return remote(
            piece,
            piece,
            up_out[level].at[chunk, step],
            up_in[level].at[chunk, step],
            at(shard, groups[level][1][step]),
        )

    def store_copy(chunk):
        units = pl.ds(chunk * pack, pack)
        return pltpu.make_async_copy(grads.at[units, partner], sums_out.at[units], store.at[chunk])

    def over(level, act):
        for step in range(factors[level][0] - 1):
            act(step)

    def give(unit):
        for which in range(2):
            near_copy(unit, which).start()

    def plus(*terms):
        total = terms[0].astype(F32)
        for term in terms[1:]:
            total = total + term.astype(F32)
        return total.astype(BF16)

    def take_near(unit):
        near_copy(unit, 0).wait_recv()
        grads[unit, across] = plus(grads[unit, across], near[unit, 0])
        when_early(unit, lambda: both_copy(unit, 0).start(), lambda: far_copy(unit).start())
        near_copy(unit, 1).wait_recv()
        grads[unit, shard] = plus(grads[unit, shard], near[unit, 1])
        when_early(unit, lambda: both_copy(unit, 1).start(), lambda: None)

    def take_far(chunk):
        for piece in range(pack):
            unit = chunk * pack + piece
            near_copy(unit, 0).wait_send()
            near_copy(unit, 1).wait_send()

            def whole():
                far_copy(unit).wait_recv()
                grads[unit, shard] = plus(grads[unit, shard], far[unit])

            def half():
                rows = span(my_places[0] * (ROWS // 2), ROWS // 2)
                far_half(unit).wait_recv()
                grads[unit, shard, rows] = plus(grads[unit, shard, rows], kept_half(far, unit)[...])

            when_early(unit, half, whole)

        when_early(
            chunk,
            lambda: over(1, lambda step: down_copy(1, chunk, step).start()),
            lambda: over(0, lambda step: down_copy(0, chunk, step).start()),
        )

    def take_down(level, chunk):
        over(level, lambda step: down_copy(level, chunk, step).wait_recv())
        places = my_places[: level + 1]
        terms = [view(shard, chunk, places)[...]]
        terms += [parts[level][chunk, step] for step in range(factors[level][0] - 1)]
        total = plus(*terms)
        if level + 1 < levels:
            view(shard, chunk, places)[...] = total
            over(level + 1, lambda step: down_copy(level + 1, chunk, step).start())
        else:
            view(partner, chunk, places)[...] = total
            over(level, lambda step: up_copy(level, chunk, step).start())

    def take_up(level, chunk):
        over(level, lambda step: up_copy(level, chunk, step).wait_recv())
        if level > 0:
            over(level - 1, lambda step: up_copy(level - 1, chunk, step).start())
        else:
            store_copy(chunk).start()

    def take_first(chunk):
        when_early(chunk, lambda: None, lambda: take_down(0, chunk))

    stages = [take_far, take_first]
    stages += [functools.partial(take_down, level) for level in range(1, levels)]
    stages += [functools.partial(take_up, level) for level in reversed(range(levels))]
    last_post = pack * (chunks + len(stages) - 1)

    def post(time):
        step = (time + 1) // pack - 1
        for lag, stage in enumerate(stages):
            good = (step >= lag) & (step < chunks + lag) & ((time + 1) % pack == 0)
            pl.when(good)(functools.partial(stage, step - lag))

    def posts(first, last):
        def body(time, carry):
            post(time)
            return carry

        lax.fori_loop(first, last, body, 0)

    def gain_copy(step):
        return remote(
            gain_sum.at[step], gain_got.at[step], gain_send.at[step], gain_recv.at[step], flips[step]
        )

    row = lax.broadcasted_iota(jnp.int32, (tokens, 1), 0)
    valid = jnp.where(row < length, 1.0, 0.0)

    def feed_forward(ht, down_w, gate_w, up_w, hid, grad_pair):
        def stream(block):
            slot = block % 2
            pairs = [
                (w_hbm.at[pl.ds(UNITS - FBLOCKS, FBLOCKS), block], down_w.at[slot]),
                (w_hbm.at[4 + 2 * block], gate_w.at[slot]),
                (w_hbm.at[5 + 2 * block], up_w.at[slot]),
                (hid_hbm.at[block], hid.at[slot]),
                (a_hbm.at[block], grad_pair.at[slot, 0]),
                (b_hbm.at[block], grad_pair.at[slot, 1]),
            ]
            return [
                pltpu.make_async_copy(source, target, s_load.at[slot, number])
                for number, (source, target) in enumerate(pairs)
            ]

        ht_loads = [
            pltpu.make_async_copy(ht_hbm.at[unit], ht.at[unit], ht_sem.at[unit])
            for unit in range(FBLOCKS)
        ]
        for copy in ht_loads:
            copy.start()
        for copy in stream(0):
            copy.start()
        cot_load.wait()
        gbt[...] = (gbt[...].astype(F32) * valid).astype(BF16)

        def down_grads(unit, carry):
            pltpu.make_async_copy(ht_hbm.at[unit], ht.at[unit], ht_sem.at[unit]).wait()
            for owner in range(SHARDS // 2):
                pair = pl.ds(2 * owner, 2)
                product = dot(flat(ht[unit, pair]), gbt[...]).astype(BF16)
                grads[unit, pair] = product.reshape(2, ROWS, COLS)
            give(unit)
            pl.when(unit >= 1)(lambda: take_near(unit - 1))
            return carry

        lax.fori_loop(0, FBLOCKS, down_grads, 0)
        n2t_load.wait()
        acc[...] = jnp.zeros_like(acc)
        result[...] = jnp.zeros_like(result)

        def block_step(block, carry):
            slot = block % 2

            @pl.when(block + 1 < FBLOCKS)
            def _():
                for copy in stream(block + 1):
                    copy.start()

            for copy in stream(block):
                copy.wait()

            def rows_of(tile, inner):
                rows = span(tile * TILE, TILE)
                grad_hidden = dot_nt(gbt[rows], flat(down_w[slot]))
                grad_pair[slot, 0, rows] = (
                    grad_hidden * grad_pair[slot, 0, rows].astype(F32)
                ).astype(BF16)
                grad_pair[slot, 1, rows] = (
                    grad_hidden * grad_pair[slot, 1, rows].astype(F32)
                ).astype(BF16)
                return inner

            lax.fori_loop(0, tokens // TILE, rows_of, 0)
            pl.when(block == 0)(lambda: take_near(FBLOCKS - 1))

            def kind_of(kind, inner):
                unit = FBLOCKS + 2 * block + kind
                for owner in range(SHARDS // 2):
                    pair = pl.ds(2 * owner, 2)
                    product = dot(
                        turned[0, pl.ds(2 * owner * ROWS, 2 * ROWS)], grad_pair[slot, kind]
                    ).astype(BF16)
                    grads[unit, pair] = product.reshape(2, ROWS, COLS)
                give(unit)
                return inner

            lax.fori_loop(0, 2, kind_of, 0)

            @pl.when(block == 0)
            def _():
                for unit in range(*early):
                    take_both(unit)

            def back_rows(tile, inner):
                rows = span(tile * TILE, TILE)
                acc[rows] += dot_nt(grad_pair[slot, 0, rows], flat(gate_w[slot])) + dot_nt(
                    grad_pair[slot, 1, rows], flat(up_w[slot])
                )
                result[rows] += dot(hid[slot, rows], flat(down_w[slot]))
                return inner

            lax.fori_loop(0, tokens // TILE, back_rows, 0)
            take_near(FBLOCKS + 2 * block)
            take_near(FBLOCKS + 2 * block + 1)
            post(block)
            return carry

        lax.fori_loop(0, FBLOCKS, block_step, 0)

    pl.run_scoped(
        feed_forward,
        pltpu.VMEM((FBLOCKS, FBLOCKS, ROWS, tokens), BF16),
        pltpu.VMEM((2, FBLOCKS, ROWS, COLS), BF16),
        pltpu.VMEM((2, SHARDS, ROWS, COLS), BF16),
        pltpu.VMEM((2, SHARDS, ROWS, COLS), BF16),
        pltpu.VMEM((2, tokens, COLS), BF16),
        pltpu.VMEM((2, 2, tokens, COLS), BF16),
    )

    def attention(attn_w, tables, qkv, lse, bias, grad_attended, grad_qkv):
        w_load = fetch(w_hbm.at[pl.ds(0, 4)], attn_w, 8)
        qkv_load = fetch(qkv_hbm, qkv, 9)
        lse_load = fetch(lse_hbm.at[pl.ds(0, 16)], lse, 10)
        table_load = fetch(tables_hbm, tables, 11)
        h1_load.wait()
        gain_load.wait()

        gain_grad = jnp.zeros((1, width), F32)
        for tile in range(tokens // TILE):
            rows = pl.ds(tile * TILE, TILE)
            good = jnp.where(
                lax.broadcasted_iota(jnp.int32, (TILE, 1), 0) + tile * TILE < length, 1.0, 0.0
            )
            out_low[rows] = ((h1[rows] + result[rows]) * good).astype(BF16)
            gain_piece, back = norm_back(acc[rows], h1[rows], gain[1:2])
            gain_grad = gain_grad + gain_piece
            grad_one = gbt[rows].astype(F32) + back
            result[rows] = grad_one
            gbt[rows] = grad_one.astype(BF16)
        gain_sum[0] = jnp.zeros_like(gain_sum[0])
        gain_sum[0, 1:2] = gain_grad
        output_store = pltpu.make_async_copy(out_low, output_out, load.at[12])
        output_store.start()
        at_load.wait()
        for owner in range(SHARDS // 2):
            pair = pl.ds(2 * owner, 2)
            product = dot(turned[1, pl.ds(2 * owner * ROWS, 2 * ROWS)], gbt[...]).astype(BF16)
            grads[UNITS - 4, pair] = product.reshape(2, ROWS, COLS)
        give(UNITS - 4)
        w_load.wait()
        for tile in range(tokens // TILE):
            rows = pl.ds(tile * TILE, TILE)
            grad_attended[rows] = dot_nt(gbt[rows], flat(attn_w[3])).astype(BF16)
        take_near(UNITS - 4)
        post(FBLOCKS)

        key_row = lax.broadcasted_iota(jnp.int32, (tokens, tokens), 0)
        query_column = lax.broadcasted_iota(jnp.int32, (tokens, tokens), 1)
        seen = (key_row <= query_column) & ((query_column < length) | (key_row >= length))
        bias[...] = jnp.where(seen, 0.0, -jnp.inf)
        qkv_load.wait()
        lse_load.wait()
        table_load.wait()
        inv_root = 1.0 / math.sqrt(HDIM)

        def attend_back(pair, carry):
            columns = span(pair * 128, 128, 128)
            grad_key = [jnp.zeros((TILE, 128), F32) for _ in range(tokens // TILE)]
            grad_value = [jnp.zeros((TILE, 128), F32) for _ in range(tokens // TILE)]
            for tile in range(tokens // TILE):
                rows = pl.ds(tile * TILE, TILE)
                query = qkv[0, rows, columns]
                grad_mixed = grad_attended[rows, columns]
                grad_query = jnp.zeros((TILE, 128), F32)
                for which in range(2):
                    mask = head_mask(which)
                    query_one = query * mask
                    mixed_one = grad_mixed * mask
                    log_row = lse[pl.ds(2 * pair + which, 1), rows]
                    probs, grad_probs = [], []
                    row_dot = jnp.zeros((1, TILE), F32)
                    for block in range(tile + 1):
                        keys = pl.ds(block * TILE, TILE)
                        scores = dot_nt(qkv[1, keys, columns], query_one) * inv_root
                        prob = jnp.exp(scores + bias[keys, rows] - log_row)
                        grad_value[block] += dot(prob.astype(BF16), mixed_one)
                        grad_prob = dot_nt(qkv[2, keys, columns], mixed_one)
                        row_dot = row_dot + jnp.sum(prob * grad_prob, axis=0, keepdims=True)
                        probs.append(prob)
                        grad_probs.append(grad_prob)
                    for block in range(tile + 1):
                        keys = pl.ds(block * TILE, TILE)
                        grad_scores = (probs[block] * (grad_probs[block] - row_dot)).astype(BF16)
                        grad_key[block] += dot(grad_scores, query_one)
                        grad_query += dot_tn(grad_scores, qkv[1, keys, columns] * mask)
                grad_query = grad_query * inv_root
                grad_query = grad_query * tables[0, rows] - half_swap(grad_query) * tables[1, rows]
                grad_qkv[0, rows, columns] = grad_query.astype(BF16)
            for block in range(tokens // TILE):
                keys = pl.ds(block * TILE, TILE)
                back = grad_key[block] * inv_root
                back = back * tables[0, keys] - half_swap(back) * tables[1, keys]
                grad_qkv[1, keys, columns] = back.astype(BF16)
                grad_qkv[2, keys, columns] = grad_value[block].astype(BF16)
            post(FBLOCKS + 1 + pair)
            return carry

        lax.fori_loop(0, HEADS // 2, attend_back, 0)
        nt_load.wait()

        def projection(which, carry):
            for owner in range(SHARDS // 2):
                pair = pl.ds(2 * owner, 2)
                product = dot(
                    turned[2, pl.ds(2 * owner * ROWS, 2 * ROWS)], grad_qkv[which]
                ).astype(BF16)
                grads[UNITS - 3 + which, pair] = product.reshape(2, ROWS, COLS)
            give(UNITS - 3 + which)
            return carry

        lax.fori_loop(0, 3, projection, 0)
        acc[...] = jnp.zeros_like(acc)

        def input_back(which, carry):
            for tile in range(tokens // TILE):
                rows = pl.ds(tile * TILE, TILE)
                acc[rows] += dot_nt(grad_qkv[which, rows], flat(attn_w[which]))
            take_near(UNITS - 3 + which)
            return carry

        lax.fori_loop(0, 3, input_back, 0)
        x_load.wait()
        gain_grad = jnp.zeros((1, width), F32)
        for tile in range(tokens // TILE):
            rows = pl.ds(tile * TILE, TILE)
            gain_piece, back = norm_back(acc[rows], x[rows].astype(F32), gain[0:1])
            gain_grad = gain_grad + gain_piece
            result[rows] = result[rows] + back
        gain_sum[0, 0:1] = gain_grad
        grad_store = pltpu.make_async_copy(result, grad_out, load.at[13])
        grad_store.start()
        output_store.wait()
        grad_store.wait()

    pl.run_scoped(
        attention,
        pltpu.VMEM((4, SHARDS, ROWS, COLS), BF16),
        pltpu.VMEM((2, tokens, 128), F32),
        pltpu.VMEM((3, tokens, width), BF16),
        pltpu.VMEM((16, tokens), F32),
        pltpu.VMEM((tokens, tokens), F32),
        pltpu.VMEM((tokens, width), BF16),
        pltpu.VMEM((3, tokens, width), BF16),
    )

    first = FBLOCKS + 1 + HEADS // 2
    gain_copy(0).start()

    def rest(time, carry):
        post(time)
        for step in range(len(flips)):

            @pl.when(time == first + 1 + step)
            def _():
                gain_copy(step).wait_recv()
                gain_sum[step + 1] = gain_sum[step] + gain_got[step]
                if step + 1 < len(flips):
                    gain_copy(step + 1).start()

        return carry

    assert first + 1 + len(flips) <= last_post
    lax.fori_loop(first, last_post, rest, 0)
    gain_out[...] = gain_sum[len(flips)]

    def settle(chunk, carry):
        for piece in range(pack):
            unit = chunk * pack + piece
            when_early(
                unit, lambda: far_half(unit).wait_send(), lambda: far_copy(unit).wait_send()
            )

        def both_sends():
            both_copy(chunk, 0).wait_send()
            both_copy(chunk, 1).wait_send()

        when_early(
            chunk, both_sends, lambda: over(0, lambda step: down_copy(0, chunk, step).wait_send())
        )
        for level in range(levels):
            if level > 0:
                over(level, lambda step: down_copy(level, chunk, step).wait_send())
            over(level, lambda step: up_copy(level, chunk, step).wait_send())
        store_copy(chunk).wait()
        return carry

    lax.fori_loop(0, chunks, settle, 0)
    for step in range(len(flips)):
        gain_copy(step).wait_send()


def backward_pass(scalars, tokens, cotangent, saved):
    count, width = tokens.shape
    replicas = lax.axis_size("replica")
    factors, pack = replica_factors(replicas)
    levels = len(factors)
    chunks = UNITS // pack
    flips = 2 + replicas.bit_length() - 1
    early = (0, 0) if pack == 1 else (0, 0)
    spare = max(early[1] - early[0], 1)
    gain = saved[-2]
    part_shapes = []
    units, rows, columns = pack, ROWS, COLS
    for level, (members, _) in enumerate(factors):
        if level == levels - 1:
            rows, columns = rows // 2, columns // 2
        else:
            by_unit = math.gcd(units, members)
            units, rows = units // by_unit, rows // (members // by_unit)
        part_shapes.append((chunks, members - 1, units, rows, columns))
    counts = [(chunks, members - 1) for members, _ in factors]
    anywhere = pl.BlockSpec(memory_space=pl.ANY)
    shape = jax.ShapeDtypeStruct
    return pl.pallas_call(
        functools.partial(backward_kernel, factors, pack, early),
        out_shape=(
            shape((UNITS, ROWS, COLS), BF16),
            shape(gain.shape, F32),
            shape((count, width), BF16),
            shape((count, width), F32),
        ),
        in_specs=[pl.BlockSpec(memory_space=pltpu.SMEM)] * 2 + [anywhere] * (2 + len(saved)),
        out_specs=[anywhere, pl.BlockSpec(memory_space=pltpu.VMEM), anywhere, anywhere],
        scratch_shapes=[
            pltpu.VMEM((UNITS, SHARDS, ROWS, COLS), BF16),
            pltpu.VMEM((UNITS, 2, ROWS, COLS), BF16),
            pltpu.VMEM((UNITS, ROWS, COLS), BF16),
            pltpu.VMEM((flips + 1,) + gain.shape, F32),
            pltpu.VMEM((flips,) + gain.shape, F32),
            pltpu.VMEM((count, width), BF16),
            pltpu.VMEM((count, width), BF16),
            pltpu.VMEM(gain.shape, F32),
            pltpu.VMEM((3, width, count), BF16),
            pltpu.VMEM((count, width), F32),
            pltpu.VMEM((count, width), F32),
            pltpu.VMEM((count, width), F32),
            pltpu.VMEM((count, width), BF16),
        ]
        + [pltpu.VMEM(part, BF16) for part in part_shapes]
        + [
            pltpu.VMEM((spare, 2, ROWS // 2, COLS), BF16),

            DMA((14,)), DMA((2, 6)), DMA((UNITS, 2)), DMA((UNITS, 2)), DMA((UNITS,)), DMA((UNITS,)),
            DMA((chunks,)), DMA((flips,)), DMA((flips,)), DMA((spare, 2)), DMA((spare, 2)), DMA((FBLOCKS,)),
        ]
        + [DMA(count_) for _ in range(4) for count_ in counts],
        compiler_params=pltpu.CompilerParams(
            collective_id=1, has_side_effects=True, vmem_limit_bytes=67043328
        ),
        name="backward_reduce",
    )(*scalars, tokens, cotangent, *saved)


def finish_kernel(
    sums, gain_sums, output_in, grad_in,
    down, gate, up, out, query, key, value, gain_one, gain_two, output, grad,
    low, wide, held_output, held_grad, in_sem, out_sem,
):
    targets = [down.at[pl.ds(piece * ROWS, ROWS)] for piece in range(FBLOCKS)]
    for block in range(FBLOCKS):
        columns = pl.ds(block * COLS, COLS)
        targets += [gate.at[:, columns], up.at[:, columns]]
    targets += [out, query, key, value]
    moves = [(output_in, held_output, output), (grad_in, held_grad, grad)]
    ins = [
        pltpu.make_async_copy(sums.at[unit], low.at[unit], in_sem.at[unit]) for unit in range(UNITS)
    ]
    ins += [
        pltpu.make_async_copy(source, held, in_sem.at[UNITS + number])
        for number, (source, held, _) in enumerate(moves)
    ]
    puts = [
        pltpu.make_async_copy(wide.at[unit], target, out_sem.at[unit])
        for unit, target in enumerate(targets)
    ]
    puts += [
        pltpu.make_async_copy(held, target, out_sem.at[UNITS + number])
        for number, (_, held, target) in enumerate(moves)
    ]
    for copy in ins[UNITS:] + ins[:UNITS]:
        copy.start()
    share = gain_sums.shape[1] // SHARDS
    shard = lax.axis_index("shard")
    turned = pltpu.roll(gain_sums[...], (SHARDS - shard) % SHARDS * share, 1)
    gain_one[...] = turned[0:1, :share]
    gain_two[...] = turned[1:2, :share]
    for number in range(UNITS, UNITS + len(moves)):
        ins[number].wait()
        puts[number].start()
    for unit in range(UNITS):
        ins[unit].wait()
        wide[unit] = low[unit].astype(F32)
        puts[unit].start()
    for copy in puts:
        copy.wait()


def finish(sums, gain_sums, output, input_grad):
    shape = jax.ShapeDtypeStruct
    small, broad = shape((ROWS, COLS), F32), shape((ROWS, FBLOCKS * COLS), F32)
    share = shape((1, gain_sums.shape[1] // SHARDS), F32)
    hbm, vmem = pl.BlockSpec(memory_space=pltpu.HBM), pl.BlockSpec(memory_space=pltpu.VMEM)
    return pl.pallas_call(
        finish_kernel,
        out_shape=(
            shape((FBLOCKS * ROWS, COLS), F32), broad, broad, small, small, small, small, share, share,
            shape(output.shape, output.dtype), shape(input_grad.shape, F32),
        ),
        in_specs=[hbm, vmem, hbm, hbm],
        out_specs=[hbm] * 7 + [vmem] * 2 + [hbm] * 2,
        scratch_shapes=[
            pltpu.VMEM((UNITS, ROWS, COLS), BF16),
            pltpu.VMEM((UNITS, ROWS, COLS), F32),
            pltpu.VMEM(output.shape, output.dtype),
            pltpu.VMEM(input_grad.shape, F32),
            DMA((UNITS + 2,)),
            DMA((UNITS + 2,)),
        ],
        compiler_params=pltpu.CompilerParams(vmem_limit_bytes=67043328),
        name="finish",
    )(sums, gain_sums, output, input_grad)


def per_device(
    tokens, cotangent, lengths, assignment, positions, attention_gain, query_weight, key_weight,
    value_weight, out_weight, feedforward_gain, gate_weight, up_weight, down_weight,
):
    shard = lax.axis_index("shard")
    lane = lax.broadcasted_iota(jnp.int32, (8, tokens.shape[1]), 1)
    row = lax.broadcasted_iota(jnp.int32, (8, tokens.shape[1]), 0)
    share = attention_gain.shape[0]
    spread = [
        jnp.broadcast_to(gain, (SHARDS, share)).reshape(1, -1).astype(F32)
        for gain in (attention_gain, feedforward_gain)
    ]
    gain_rows = jnp.where(
        (lane // share == shard) & (row < 2), jnp.where(row == 0, spread[0], spread[1]), 0.0
    )
    saved = forward_pass(
        [lengths, assignment, positions],
        tokens,
        gain_rows,
        [query_weight, key_weight, value_weight, out_weight, gate_weight, up_weight, down_weight],
    )
    sums, gain_sums, output, input_grad = backward_pass(
        [lengths, assignment], tokens, cotangent, saved
    )
    down, gate, up, out, query, key, value, gain_one, gain_two, output, input_grad = finish(
        sums, gain_sums, output, input_grad
    )
    return (
        output,
        input_grad,
        gain_one.reshape(-1),
        query,
        key,
        value,
        out,
        gain_two.reshape(-1),
        gate,
        up,
        down,
    )


def solution(mesh):
    return jax.shard_map(
        per_device,
        mesh=mesh,
        in_specs=(
            P(("shard", "replica"), None),
            P(("shard", "replica"), None),
            P(),
            P(),
            P(("shard", "replica")),
            P("shard"),
            P("shard", None),
            P("shard", None),
            P("shard", None),
            P("shard", None),
            P("shard"),
            P("shard", None),
            P("shard", None),
            P("shard", None),
        ),
        out_specs=(
            P(("shard", "replica"), None),
            P(("shard", "replica"), None),
            P("shard"),
            P("shard", None),
            P("shard", None),
            P("shard", None),
            P("shard", None),
            P("shard"),
            P("shard", None),
            P("shard", None),
            P("shard", None),
        ),
        check_vma=False,
    )
```

```python
import functools
import math

import jax
import jax.numpy as jnp
from jax import lax
from jax.experimental import pallas as pl
from jax.experimental.pallas import tpu as pltpu
from jax.sharding import PartitionSpec as P

HEADS = 12
HDIM = 64
EPSILON = 1e-05
ROPE_BASE = 10000.0
MESH = pl.DeviceIdType.MESH
F32 = jnp.float32
BF16 = jnp.bfloat16
DMA = pltpu.SemaphoreType.DMA

ROWS = 192
COLS = 768
UNITS = 16
FBLOCKS = 4
SHARDS = 4
TILE = 256
TALL = 512


def toggle(index, stride):
    return index + (1 - 2 * ((index // stride) % 2)) * stride


def ring(index, members, stride):
    place = (index // stride) % members
    base = index - place * stride
    return place, [base + ((place + step) % members) * stride for step in range(1, members)]


def at(shard, replica):
    return {"shard": shard, "replica": replica}


def greet(peers):
    barrier = pltpu.get_barrier_semaphore()
    for peer in peers:
        pl.semaphore_signal(barrier, inc=1, device_id=peer, device_id_type=MESH)
    pl.semaphore_wait(barrier, len(peers))


def remote(source, target, send, receive, peer):
    return pltpu.make_async_remote_copy(
        src_ref=source,
        dst_ref=target,
        send_sem=send,
        recv_sem=receive,
        device_id=peer,
        device_id_type=MESH,
    )


def mult(start, step):
    return start if isinstance(start, int) else pl.multiple_of(start, step)


def span(start, size, step=16):
    return pl.ds(mult(start, step), size)


class Levels:
    def __init__(self, replica, count):
        self.replica = replica
        if count == 8:
            self.pack, self.members, self.strides = 1, [2, 4], [1, 2]
            self.cuts = [("rows", 2), ("quarters", 4)]
        else:
            assert count == 32
            self.pack, self.members, self.strides = 4, [2, 4, 4], [16, 4, 1]
            self.cuts = [("units", 2), ("halves", 4), ("quarters", 4)]
        self.count = len(self.members)
        self.whole = UNITS // self.pack
        self.items = [(chunk, None) for chunk in range(self.whole)]
        self.items += [
            (chunk, third) for chunk in range(self.whole, UNITS // self.pack) for third in range(3)
        ]

    def item(self, chunk, third):
        return chunk if third is None else self.whole + 3 * (chunk - self.whole) + third

    def group(self, level, chunk):
        return ring(self.replica, self.members[level], self.strides[level])

    def places(self, chunk):
        return [self.group(level, chunk)[0] for level in range(self.count)]

    def size(self, level):
        units, rows, columns = self.pack, ROWS, COLS
        for kind, _ in self.cuts[:level]:
            if kind == "units":
                units = units // 2
            elif kind == "rows":
                rows = rows // 2
            elif kind == "columns":
                columns = columns // 2
            elif kind == "halves":
                units, rows = units // 2, rows // 2
            else:
                rows, columns = rows // 2, columns // 2
        return units, rows, columns

    def region(self, chunk, third, places):
        unit, row, column = chunk * self.pack, 0, 0
        parts = 1
        if third is not None:
            parts, column = 3, third * (COLS // 3)
        for level, place in enumerate(places):
            kind = self.cuts[level][0]
            units, rows, columns = self.size(level + 1)
            columns = columns // parts
            if kind == "units":
                unit = unit + place * units
            elif kind == "rows":
                row = row + place * rows
            elif kind == "columns":
                column = column + place * columns
            elif kind == "halves":
                unit, row = unit + place // 2 * units, row + place % 2 * rows
            else:
                row, column = row + place // 2 * rows, column + place % 2 * columns
        units, rows, columns = self.size(len(places))
        return pl.ds(unit, units), span(row, rows), span(column, columns // parts, 128)


def dot(a, b):
    return jnp.dot(a, b, preferred_element_type=F32)


def dot_nt(a, b):
    return lax.dot_general(a, b, (((1,), (1,)), ((), ())), preferred_element_type=F32)


def dot_tn(a, b):
    return lax.dot_general(a, b, (((0,), (0,)), ((), ())), preferred_element_type=F32)


def flat(block):
    return block.reshape(-1, block.shape[-1])


def scale_of(values):
    return lax.rsqrt(jnp.mean(values * values, axis=-1, keepdims=True) + EPSILON)


def half_swap(values):
    lane = lax.broadcasted_iota(jnp.int32, values.shape, 1)
    return jnp.where(lane % 64 < 32, pltpu.roll(values, 96, 1), pltpu.roll(values, 32, 1))


def head_mask(which):
    lane = lax.broadcasted_iota(jnp.int32, (1, 128), 1)
    return jnp.where((lane < 64) == (which == 0), 1.0, 0.0).astype(BF16)


def own_length(lengths, assignment, device):
    total = jnp.int32(0)
    for number in range(lengths.shape[0]):
        total = total + jnp.where(assignment[number] == device, lengths[number], 0)
    return total


def rotation(start, length, tokens):
    row = lax.broadcasted_iota(jnp.int32, (tokens, 128), 0)
    lane = lax.broadcasted_iota(jnp.int32, (1, 128), 1)
    half = HDIM // 2
    frequency = jnp.exp((lane % half).astype(F32) * (-2.0 * math.log(ROPE_BASE) / HDIM))
    angles = jnp.where(row < length, row + start, 0).astype(F32) * frequency
    return jnp.cos(angles), jnp.sin(angles) * jnp.where(lane % HDIM < half, -1.0, 1.0)


def norm_back(grad_normed, values, gain):
    scale = scale_of(values)
    scaled = gain * grad_normed
    gain_grad = jnp.sum(grad_normed * values * scale, axis=0, keepdims=True)
    mean = jnp.mean(scaled * values, axis=-1, keepdims=True)
    return gain_grad, scale * scaled - values * (scale * scale * scale) * mean


def forward_kernel(
    lengths, assignment, positions, x_hbm, gain_hbm, q_hbm, k_hbm, v_hbm, o_hbm, g_hbm, u_hbm, d_hbm,
    w_out, qkv_out, nt_out, n2t_out, at_out, ht_out, hid_out, a_out, b_out, h1_out, lse_out, gain_out,
    tables_out,
    w, x, tables, gains, gain, normed, normed_t, qkv, bias, attended, lse, lse_t, h1, ht, hid, a, b,
    load, x_out, x_in, y_out, y_in, z_out, z_in, d_out, d_in, p_out, p_in, f_out, f_in, g_out, g_in,
    w_store, store, f_store,
):
    shard, replica = lax.axis_index("shard"), lax.axis_index("replica")
    partner, across = toggle(shard, 1), toggle(shard, 2)
    opposite = toggle(across, 1)
    beside, behind = toggle(replica, 1), toggle(replica, 2)
    mine = replica % 4
    quarter_beside, quarter_behind = toggle(mine, 1), toggle(mine, 2)
    quarter_last = toggle(quarter_beside, 2)
    tokens, width = x.shape

    sources = [q_hbm, k_hbm, v_hbm, o_hbm]
    for block in range(FBLOCKS):
        columns = pl.ds(block * COLS, COLS)
        sources += [g_hbm.at[:, columns], u_hbm.at[:, columns]]
    sources += [d_hbm.at[pl.ds(piece * ROWS, ROWS)] for piece in range(UNITS - len(sources))]
    loads = [
        pltpu.make_async_copy(source, w.at[unit, shard], load.at[unit])
        for unit, source in enumerate(sources)
    ]
    x_load = pltpu.make_async_copy(x_hbm, x, load.at[UNITS])
    gain_load = pltpu.make_async_copy(gain_hbm, gains.at[shard], load.at[UNITS + 1])
    gain_load.start()
    for copy in loads:
        copy.start()
    x_load.start()

    shard_peers = [at(partner, replica), at(across, replica), at(opposite, replica)]
    greet(shard_peers + [at(shard, beside), at(shard, behind)])

    gain_load.wait()
    gain_copies = [
        remote(gains.at[shard], gains.at[shard], g_out.at[number], g_in.at[number], peer)
        for number, peer in enumerate(shard_peers)
    ]
    for copy in gain_copies:
        copy.start()

    quarter = ROWS // 4

    def part(unit, owner, which):
        return w.at[unit, owner, span(which * quarter, quarter)]

    def cross(unit):
        piece = part(unit, shard, mine)
        return remote(piece, piece, x_out.at[unit], x_in.at[unit], at(across, replica))

    def share(unit):
        piece = w.at[unit, shard]
        return remote(piece, piece, p_out.at[unit], p_in.at[unit], at(partner, replica))

    def hand_beside(unit):
        piece = part(unit, across, mine)
        return remote(piece, piece, y_out.at[unit], y_in.at[unit], at(shard, beside))

    def hand_behind(unit):
        piece = part(unit, across, mine)
        return remote(piece, piece, z_out.at[unit], z_in.at[unit], at(shard, behind))

    def hand_on(unit, odd):
        piece = part(unit, across, quarter_beside if odd else quarter_behind)
        peer = at(shard, behind if odd else beside)
        return remote(piece, piece, d_out.at[unit], d_in.at[unit], peer)

    def by_parity(unit, act):
        for odd in range(2):
            pl.when(unit % 2 == odd)(functools.partial(act, odd))

    def forward(unit, number):
        which = (mine, quarter_beside, quarter_behind, quarter_last)[number]
        piece = part(unit, across, which)
        return remote(piece, piece, f_out.at[number, unit], f_in.at[number, unit], at(partner, replica))

    def keep(unit):
        return pltpu.make_async_copy(w.at[unit], w_out.at[unit], w_store.at[unit])

    for unit in range(UNITS):
        loads[unit].wait()
        cross(unit).start()
        share(unit).start()

    def take_cross(unit):
        cross(unit).wait_recv()
        hand_beside(unit).start()
        hand_behind(unit).start()
        forward(unit, 0).start()

    def take_hands(unit):
        hand_behind(unit).wait_recv()
        hand_beside(unit).wait_recv()
        by_parity(unit, lambda odd: hand_on(unit, odd).start())
        forward(unit, 1).start()
        forward(unit, 2).start()

    def take_last(unit):
        by_parity(unit, lambda odd: hand_on(unit, odd).wait_recv())
        forward(unit, 3).start()

    def complete(unit):
        share(unit).wait_recv()
        for number in range(4):
            forward(unit, number).wait_recv()
        keep(unit).start()

    stages = [(0, take_cross), (2, take_hands), (4, take_last), (5, complete)]

    def tick(time):
        for lag, stage in stages:
            pl.when((time >= lag) & (time < UNITS + lag))(functools.partial(stage, time - lag))

    def ticks(first, last):
        def body(time, carry):
            tick(time)
            return carry

        lax.fori_loop(first, last, body, 0)

    stores = []

    def save(source, target):
        copy = pltpu.make_async_copy(source, target, store.at[len(stores)])
        copy.start()
        stores.append(copy)

    row = lax.broadcasted_iota(jnp.int32, (tokens, tokens), 0)
    column = lax.broadcasted_iota(jnp.int32, (tokens, tokens), 1)
    device = shard * lax.axis_size("replica") + replica
    length = own_length(lengths, assignment, device)
    seen = (column <= row) & ((row < length) | (column >= length))
    bias[...] = jnp.where(seen, 0.0, -jnp.inf)

    x_load.wait()
    for copy in gain_copies:
        copy.wait_recv()
    gain[...] = gains[0] + gains[1] + gains[2] + gains[3]
    save(gain, gain_out)
    values = x[...].astype(F32)
    normed[...] = (values * scale_of(values) * gain[0:1]).astype(BF16)
    normed_t[0] = normed[...].T
    save(normed_t.at[0], nt_out)
    tables[0], tables[1] = rotation(positions[0], length, tokens)
    save(tables, tables_out)
    ticks(0, 8)

    def project(step, carry):
        which, tile = step // (tokens // TILE), step % (tokens // TILE)
        rows = span(tile * TILE, TILE)
        product = dot(normed[rows], flat(w[which]))
        cosine = jnp.where(which < 2, tables[0, rows], 1.0)
        sine = jnp.where(which < 2, tables[1, rows], 0.0)
        for pair in range(width // 128):
            columns = slice(pair * 128, pair * 128 + 128)
            piece = product[:, columns]
            qkv[which, rows, columns] = (piece * cosine + half_swap(piece) * sine).astype(BF16)
        return carry

    lax.fori_loop(0, 3 * (tokens // TILE), project, 0)
    save(qkv, qkv_out)
    tick(8)
    lse[...] = jnp.zeros_like(lse)

    def attend(pair, carry):
        columns = span(pair * 128, 128, 128)
        for tile in range(tokens // TILE):
            rows = pl.ds(tile * TILE, TILE)
            keys = (tile + 1) * TILE
            query = qkv[0, rows, columns]
            key = qkv[1, 0:keys, columns]
            value = qkv[2, 0:keys, columns]
            mixed = []
            logs = lse[rows]
            lane = lax.broadcasted_iota(jnp.int32, logs.shape, 1)
            for which in range(2):
                scores = dot_nt(query * head_mask(which), key) * (1.0 / math.sqrt(HDIM))
                scores = scores + bias[rows, 0:keys]
                peak = jnp.max(scores, axis=-1, keepdims=True)
                exponent = jnp.exp(scores - peak)
                total = jnp.sum(exponent, axis=-1, keepdims=True)
                probability = (exponent * (1.0 / total)).astype(BF16)
                mixed.append(dot(probability, value))
                logs = jnp.where(lane == 2 * pair + which, peak + jnp.log(total), logs)
            lse[rows] = logs
            first = lax.broadcasted_iota(jnp.int32, mixed[0].shape, 1) < 64
            attended[rows, columns] = jnp.where(first, mixed[0], mixed[1]).astype(BF16)
        tick(9 + pair)
        return carry

    lax.fori_loop(0, HEADS // 2, attend, 0)
    normed_t[1] = attended[...].T
    save(normed_t.at[1], at_out)
    lse_t[...] = lse[...].T
    save(lse_t, lse_out)
    for tile in range(tokens // TILE):
        rows = pl.ds(tile * TILE, TILE)
        hidden_one = x[rows].astype(F32) + dot(attended[rows], flat(w[3]))
        h1[rows] = hidden_one
        normed[rows] = (hidden_one * scale_of(hidden_one) * gain[1:2]).astype(BF16)
    save(h1, h1_out)
    normed_t[2] = normed[...].T
    save(normed_t.at[2], n2t_out)

    def f_copies(block):
        pairs = [
            (hid.at[block], hid_out.at[block]),
            (a.at[block], a_out.at[block]),
            (b.at[block], b_out.at[block]),
            (ht.at[:, block], ht_out.at[:, block]),
        ]
        return [
            pltpu.make_async_copy(source, target, f_store.at[block, number])
            for number, (source, target) in enumerate(pairs)
        ]

    def feed(block, carry):
        def rows_of(tile, inner):
            rows = span(tile * TILE, TILE)
            gate = dot(normed[rows], flat(w[4 + 2 * block]))
            upward = dot(normed[rows], flat(w[5 + 2 * block]))
            sigmoid = jax.nn.sigmoid(gate)
            activated = gate * sigmoid
            hid[block, rows] = (activated * upward).astype(BF16)
            a[block, rows] = (upward * sigmoid * (1.0 + gate * (1.0 - sigmoid))).astype(BF16)
            b[block, rows] = activated.astype(BF16)
            return inner

        lax.fori_loop(0, tokens // TILE, rows_of, 0)
        turned = hid[block].T
        for piece in range(FBLOCKS):
            ht[piece, block] = turned[piece * ROWS : (piece + 1) * ROWS]
        for copy in f_copies(block):
            copy.start()
        tick(15 + block)
        return carry

    lax.fori_loop(0, FBLOCKS, feed, 0)
    ticks(15 + FBLOCKS, UNITS + 5)

    def settle(unit, carry):
        cross(unit).wait_send()
        share(unit).wait_send()
        hand_beside(unit).wait_send()
        hand_behind(unit).wait_send()
        by_parity(unit, lambda odd: hand_on(unit, odd).wait_send())
        for number in range(4):
            forward(unit, number).wait_send()
        keep(unit).wait()
        return carry

    lax.fori_loop(0, UNITS, settle, 0)
    for copy in gain_copies:
        copy.wait_send()
    for copy in stores:
        copy.wait()
    for block in range(FBLOCKS):
        for copy in f_copies(block):
            copy.wait()


def forward_pass(scalars, tokens, gain_rows, weights):
    count, width = tokens.shape
    shape = jax.ShapeDtypeStruct
    outs = (
        shape((UNITS, SHARDS, ROWS, COLS), BF16),
        shape((3, count, width), BF16),
        shape((width, count), BF16),
        shape((width, count), BF16),
        shape((width, count), BF16),
        shape((FBLOCKS, FBLOCKS, ROWS, count), BF16),
        shape((FBLOCKS, count, COLS), BF16),
        shape((FBLOCKS, count, COLS), BF16),
        shape((FBLOCKS, count, COLS), BF16),
        shape((count, width), F32),
        shape((128, count), F32),
        shape(gain_rows.shape, F32),
        shape((2, count, 128), F32),
    )
    anywhere = pl.BlockSpec(memory_space=pl.ANY)
    return pl.pallas_call(
        forward_kernel,
        out_shape=outs,
        in_specs=[pl.BlockSpec(memory_space=pltpu.SMEM)] * 3 + [anywhere] * 9,
        out_specs=[anywhere] * len(outs),
        scratch_shapes=[
            pltpu.VMEM((UNITS, SHARDS, ROWS, COLS), BF16),
            pltpu.VMEM((count, width), BF16),
            pltpu.VMEM((2, count, 128), F32),
            pltpu.VMEM((SHARDS,) + gain_rows.shape, F32),
            pltpu.VMEM(gain_rows.shape, F32),
            pltpu.VMEM((count, width), BF16),
            pltpu.VMEM((3, width, count), BF16),
            pltpu.VMEM((3, count, width), BF16),
            pltpu.VMEM((count, count), F32),
            pltpu.VMEM((count, width), BF16),
            pltpu.VMEM((count, 128), F32),
            pltpu.VMEM((128, count), F32),
            pltpu.VMEM((count, width), F32),
            pltpu.VMEM((FBLOCKS, FBLOCKS, ROWS, count), BF16),
            pltpu.VMEM((FBLOCKS, count, COLS), BF16),
            pltpu.VMEM((FBLOCKS, count, COLS), BF16),
            pltpu.VMEM((FBLOCKS, count, COLS), BF16),
            DMA((UNITS + 2,)),
        ]
        + [DMA((UNITS,))] * 10
        + [
            DMA((4, UNITS)), DMA((4, UNITS)), DMA((3,)), DMA((3,)),
            DMA((UNITS,)), DMA((8,)), DMA((FBLOCKS, 4)),
        ],
        compiler_params=pltpu.CompilerParams(
            collective_id=0, has_side_effects=True, vmem_limit_bytes=60 * 1024 * 1024
        ),
        name="forward_gather",
    )(*scalars, tokens, gain_rows, *weights)


def backward_kernel(
    replicas,
    lengths, assignment, x_hbm, cot_hbm, w_hbm, qkv_hbm, nt_hbm, n2t_hbm, at_hbm, ht_hbm,
    hid_hbm, a_hbm, b_hbm, h1_hbm, lse_hbm, gain_hbm, tables_hbm,
    sums_out, gain_out, output_out, grad_out,
    *refs,
):
    shard, replica = lax.axis_index("shard"), lax.axis_index("replica")
    order = Levels(replica, replicas)
    levels, pack = order.count, order.pack
    (grads, near, far, gain_sum, gain_got, gbt, gain, n2t, h1, acc, result) = refs[:11]
    parts = refs[11 : 11 + levels]
    sems = refs[11 + levels :]
    (load, s_load, near_out, near_in, far_out, far_in, store, gain_send, gain_recv) = sems[:9]
    ht_sem = sems[9]
    down_out, down_in, up_out, up_in = (
        sems[10 + kind * levels : 10 + (kind + 1) * levels] for kind in range(4)
    )
    partner, across = toggle(shard, 1), toggle(shard, 2)
    opposite = toggle(across, 1)
    tokens, width = gbt.shape
    length = own_length(lengths, assignment, shard * lax.axis_size("replica") + replica)
    flips = [at(partner, replica), at(across, replica)]
    stride = 1
    while stride < replicas:
        flips.append(at(shard, toggle(replica, stride)))
        stride *= 2

    def fetch(source, target, number):
        copy = pltpu.make_async_copy(source, target, load.at[number])
        copy.start()
        return copy

    cot_load = fetch(cot_hbm, gbt, 0)
    n2t_load = fetch(n2t_hbm, n2t, 1)
    h1_load = fetch(h1_hbm, h1, 2)
    gain_load = fetch(gain_hbm, gain, 4)

    greet(
        [at(partner, replica), at(across, replica)]
        + [at(shard, other) for level in range(levels) for other in order.group(level, 0)[1]]
    )

    chunks = UNITS // pack

    def view(owner, chunk, third, places):
        units, rows, columns = order.region(chunk, third, places)
        return grads.at[units, owner, rows, columns]

    def near_copy(unit, which):
        return remote(
            grads.at[unit, opposite if which == 0 else partner],
            near.at[unit, which],
            near_out.at[unit, which],
            near_in.at[unit, which],
            at(partner, replica),
        )

    def columns_of(third, width):
        return pl.ds(0, width) if third is None else pl.ds(third * (width // 3), width // 3)

    def far_copy(unit, third=None):
        columns = columns_of(third, COLS)
        item = order.item(unit, third)
        return remote(
            grads.at[unit, across, :, columns],
            far.at[unit, :, columns],
            far_out.at[item],
            far_in.at[item],
            at(across, replica),
        )

    def part(level, chunk, third, step):
        width = order.size(level + 1)[2]
        return parts[level].at[chunk, step, :, :, columns_of(third, width)]

    def down_copy(level, chunk, step, third=None):
        members = order.members[level]
        place, others = order.group(level, chunk)
        theirs = (place + step + 1) % members
        item = order.item(chunk, third)
        return remote(
            view(shard, chunk, third, order.places(chunk)[:level] + [theirs]),
            part(level, chunk, third, step),
            down_out[level].at[item, step],
            down_in[level].at[item, step],
            at(shard, others[step]),
        )

    def up_copy(level, chunk, step, third=None):
        piece = view(partner, chunk, third, order.places(chunk)[: level + 1])
        item = order.item(chunk, third)
        return remote(
            piece,
            piece,
            up_out[level].at[item, step],
            up_in[level].at[item, step],
            at(shard, order.group(level, chunk)[1][step]),
        )

    def store_copy(chunk, third=None):
        units = pl.ds(chunk * pack, pack)
        columns = columns_of(third, COLS)
        return pltpu.make_async_copy(
            grads.at[units, partner, :, columns],
            sums_out.at[units, :, columns],
            store.at[order.item(chunk, third)],
        )

    def over(level, act):
        for step in range(order.members[level] - 1):
            act(step)

    def give(unit):
        for which in range(2):
            near_copy(unit, which).start()

    def plus(*terms):
        total = terms[0].astype(F32)
        for term in terms[1:]:
            total = total + term.astype(F32)
        return total.astype(BF16)

    def take_near(unit):
        near_copy(unit, 0).wait_recv()
        grads[unit, across] = plus(grads[unit, across], near[unit, 0])
        if pack > 1:
            far_copy(unit).start()
        else:
            pl.when(unit < order.whole)(lambda: far_copy(unit).start())

            @pl.when(unit >= order.whole)
            def _():
                for third in range(3):
                    far_copy(unit, third).start()

        near_copy(unit, 1).wait_recv()
        grads[unit, shard] = plus(grads[unit, shard], near[unit, 1])

    def take_far(chunk, third=None):
        for piece in range(pack):
            unit = chunk * pack + piece
            if third is None or third == 0:
                near_copy(unit, 0).wait_send()
                near_copy(unit, 1).wait_send()
            far_copy(unit, third).wait_recv()
            columns = columns_of(third, COLS)
            grads[unit, shard, :, columns] = plus(
                grads[unit, shard, :, columns], far[unit, :, columns]
            )
        over(0, lambda step: down_copy(0, chunk, step, third).start())

    def take_down(level, chunk, third=None):
        over(level, lambda step: down_copy(level, chunk, step, third).wait_recv())
        places = order.places(chunk)[: level + 1]
        terms = [view(shard, chunk, third, places)[...]]
        terms += [part(level, chunk, third, step)[...] for step in range(order.members[level] - 1)]
        total = plus(*terms)
        if level + 1 < levels:
            view(shard, chunk, third, places)[...] = total
            over(level + 1, lambda step: down_copy(level + 1, chunk, step, third).start())
        else:
            view(partner, chunk, third, places)[...] = total
            over(level, lambda step: up_copy(level, chunk, step, third).start())

    def take_up(level, chunk, third=None):
        over(level, lambda step: up_copy(level, chunk, step, third).wait_recv())
        if level > 0:
            over(level - 1, lambda step: up_copy(level - 1, chunk, step, third).start())
        else:
            store_copy(chunk, third).start()

    stages = [take_far]
    stages += [functools.partial(take_down, level) for level in range(levels)]
    stages += [functools.partial(take_up, level) for level in reversed(range(levels))]

    def post(time):
        step = (time + 1) // pack - 1
        for lag, stage in enumerate(stages):
            good = (step >= lag) & (step < chunks + lag) & ((time + 1) % pack == 0)
            pl.when(good)(functools.partial(stage, step - lag))

    def remaining(first):
        arrival, found = 0.0, []
        for chunk, third in order.items:
            pace = 1.0 if third is None else 1.0 / 3
            arrival += pace
            wait = (0.0, 1.02, 2.02, 3.02, 4.02) if third is None else (0.0, 0.68, 1.36, 2.04, 2.72)
            for lag, stage in enumerate(stages):
                if chunk + lag >= first:
                    found.append((arrival + wait[lag], lag, len(found), stage, chunk, third))
        return [entry[3:] for entry in sorted(found, key=lambda entry: entry[:3])]

    def gain_copy(step):
        return remote(
            gain_sum.at[step], gain_got.at[step], gain_send.at[step], gain_recv.at[step], flips[step]
        )

    row = lax.broadcasted_iota(jnp.int32, (tokens, 1), 0)
    valid = jnp.where(row < length, 1.0, 0.0)

    def down_phase(ht):
        ht_loads = [
            pltpu.make_async_copy(ht_hbm.at[unit], ht.at[unit], ht_sem.at[unit])
            for unit in range(FBLOCKS)
        ]
        for copy in ht_loads:
            copy.start()
        cot_load.wait()
        gbt[...] = (gbt[...].astype(F32) * valid).astype(BF16)

        def down_grads(unit, carry):
            pltpu.make_async_copy(ht_hbm.at[unit], ht.at[unit], ht_sem.at[unit]).wait()
            product = dot(flat(ht[unit]), gbt[...]).astype(BF16)
            grads[unit] = product.reshape(SHARDS, ROWS, COLS)
            give(unit)
            pl.when(unit >= 1)(lambda: take_near(unit - 1))
            return carry

        lax.fori_loop(0, FBLOCKS, down_grads, 0)

    def feed_forward(down_w, gate_w, up_w, hid, grad_pair):
        def stream(block):
            slot = block % 2
            pairs = [
                (w_hbm.at[pl.ds(UNITS - FBLOCKS, FBLOCKS), block], down_w.at[slot]),
                (w_hbm.at[4 + 2 * block], gate_w.at[slot]),
                (w_hbm.at[5 + 2 * block], up_w.at[slot]),
                (hid_hbm.at[block], hid.at[slot]),
                (a_hbm.at[block], grad_pair.at[slot, 0]),
                (b_hbm.at[block], grad_pair.at[slot, 1]),
            ]
            return [
                pltpu.make_async_copy(source, target, s_load.at[slot, number])
                for number, (source, target) in enumerate(pairs)
            ]

        for copy in stream(0):
            copy.start()
        n2t_load.wait()
        acc[...] = jnp.zeros_like(acc)
        result[...] = jnp.zeros_like(result)

        def block_step(block, carry):
            slot = block % 2

            @pl.when(block + 1 < FBLOCKS)
            def _():
                for copy in stream(block + 1):
                    copy.start()

            for copy in stream(block):
                copy.wait()

            grad_hidden = dot_nt(gbt[...], flat(down_w[slot]))
            grad_pair[slot, 0] = (grad_hidden * grad_pair[slot, 0].astype(F32)).astype(BF16)
            grad_pair[slot, 1] = (grad_hidden * grad_pair[slot, 1].astype(F32)).astype(BF16)
            pl.when(block == 0)(lambda: take_near(FBLOCKS - 1))

            def kind_of(kind, inner):
                unit = FBLOCKS + 2 * block + kind
                product = dot(n2t[...], grad_pair[slot, kind]).astype(BF16)
                grads[unit] = product.reshape(SHARDS, ROWS, COLS)
                give(unit)
                return inner

            lax.fori_loop(0, 2, kind_of, 0)

            post(2 * block - block // 3)
            acc[...] += dot_nt(grad_pair[slot, 0], flat(gate_w[slot])) + dot_nt(
                grad_pair[slot, 1], flat(up_w[slot])
            )
            result[...] += dot(hid[slot], flat(down_w[slot]))
            take_near(FBLOCKS + 2 * block)
            take_near(FBLOCKS + 2 * block + 1)
            pl.when(block != 2)(lambda: post(2 * block + 1 - block // 3))
            return carry

        lax.fori_loop(0, FBLOCKS, block_step, 0)

    pl.run_scoped(down_phase, pltpu.VMEM((FBLOCKS, FBLOCKS, ROWS, tokens), BF16))
    pl.run_scoped(
        feed_forward,
        pltpu.VMEM((2, FBLOCKS, ROWS, COLS), BF16),
        pltpu.VMEM((2, SHARDS, ROWS, COLS), BF16),
        pltpu.VMEM((2, SHARDS, ROWS, COLS), BF16),
        pltpu.VMEM((2, tokens, COLS), BF16),
        pltpu.VMEM((2, 2, tokens, COLS), BF16),
    )

    def attention(attn_w, tables, qkv, lse, bias, grad_attended, grad_qkv, turned, x, out_low):
        at_load = fetch(at_hbm, turned.at[0], 5)
        w_load = fetch(w_hbm.at[pl.ds(0, 4)], attn_w, 8)
        qkv_load = fetch(qkv_hbm, qkv, 9)
        lse_load = fetch(lse_hbm.at[pl.ds(0, 16)], lse, 10)
        table_load = fetch(tables_hbm, tables, 11)
        nt_load = fetch(nt_hbm, turned.at[1], 6)
        x_load = fetch(x_hbm, x, 3)
        h1_load.wait()
        gain_load.wait()

        gain_grad = jnp.zeros((1, width), F32)
        for tile in range(tokens // TILE):
            rows = pl.ds(tile * TILE, TILE)
            good = jnp.where(
                lax.broadcasted_iota(jnp.int32, (TILE, 1), 0) + tile * TILE < length, 1.0, 0.0
            )
            out_low[rows] = ((h1[rows] + result[rows]) * good).astype(BF16)
            gain_piece, back = norm_back(acc[rows], h1[rows], gain[1:2])
            gain_grad = gain_grad + gain_piece
            grad_one = gbt[rows].astype(F32) + back
            result[rows] = grad_one
            gbt[rows] = grad_one.astype(BF16)
        gain_sum[0] = jnp.zeros_like(gain_sum[0])
        gain_sum[0, 1:2] = gain_grad
        output_store = pltpu.make_async_copy(out_low, output_out, load.at[12])
        output_store.start()
        at_load.wait()
        product = dot(turned[0], gbt[...]).astype(BF16)
        grads[UNITS - 4] = product.reshape(SHARDS, ROWS, COLS)
        give(UNITS - 4)
        w_load.wait()
        for tile in range(tokens // TILE):
            rows = pl.ds(tile * TILE, TILE)
            grad_attended[rows] = dot_nt(gbt[rows], flat(attn_w[3])).astype(BF16)
        take_near(UNITS - 4)
        post(7)

        key_row = lax.broadcasted_iota(jnp.int32, (tokens, tokens), 0)
        query_column = lax.broadcasted_iota(jnp.int32, (tokens, tokens), 1)
        seen = (key_row <= query_column) & ((query_column < length) | (key_row >= length))
        bias[...] = jnp.where(seen, 0.0, -jnp.inf).astype(BF16)
        qkv_load.wait()
        lse_load.wait()
        table_load.wait()
        inv_root = 1.0 / math.sqrt(HDIM)

        def attend_back(pair, carry):
            columns = span(pair * 128, 128, 128)
            grad_key = [jnp.zeros((TILE, 128), F32) for _ in range(tokens // TILE)]
            grad_value = [jnp.zeros((TILE, 128), F32) for _ in range(tokens // TILE)]
            for tile in range(tokens // TILE):
                rows = pl.ds(tile * TILE, TILE)
                query = qkv[0, rows, columns]
                grad_mixed = grad_attended[rows, columns]
                grad_query = jnp.zeros((TILE, 128), F32)
                for which in range(2):
                    mask = head_mask(which)
                    query_one = query * mask
                    mixed_one = grad_mixed * mask
                    log_row = lse[pl.ds(2 * pair + which, 1), rows]
                    probs, grad_probs = [], []
                    row_dot = jnp.zeros((1, TILE), F32)
                    for block in range(tile + 1):
                        keys = pl.ds(block * TILE, TILE)
                        scores = dot_nt(qkv[1, keys, columns], query_one) * inv_root
                        prob = jnp.exp(scores + bias[keys, rows].astype(F32) - log_row)
                        grad_value[block] += dot(prob.astype(BF16), mixed_one)
                        grad_prob = dot_nt(qkv[2, keys, columns], mixed_one)
                        row_dot = row_dot + jnp.sum(prob * grad_prob, axis=0, keepdims=True)
                        probs.append(prob)
                        grad_probs.append(grad_prob)
                    for block in range(tile + 1):
                        keys = pl.ds(block * TILE, TILE)
                        grad_scores = (probs[block] * (grad_probs[block] - row_dot)).astype(BF16)
                        grad_key[block] += dot(grad_scores, query_one)
                        grad_query += dot_tn(grad_scores, qkv[1, keys, columns] * mask)
                grad_query = grad_query * inv_root
                grad_query = grad_query * tables[0, rows] - half_swap(grad_query) * tables[1, rows]
                grad_qkv[0, rows, columns] = grad_query.astype(BF16)
            for block in range(tokens // TILE):
                keys = pl.ds(block * TILE, TILE)
                back = grad_key[block] * inv_root
                back = back * tables[0, keys] - half_swap(back) * tables[1, keys]
                grad_qkv[1, keys, columns] = back.astype(BF16)
                grad_qkv[2, keys, columns] = grad_value[block].astype(BF16)
            pl.when(pair % 2 == 1)(lambda: post(8 + pair // 2))
            return carry

        lax.fori_loop(0, HEADS // 2, attend_back, 0)
        nt_load.wait()

        def projection(which, carry):
            product = dot(turned[1], grad_qkv[which]).astype(BF16)
            grads[UNITS - 3 + which] = product.reshape(SHARDS, ROWS, COLS)
            give(UNITS - 3 + which)
            return carry

        lax.fori_loop(0, 3, projection, 0)
        acc[...] = jnp.zeros_like(acc)

        def input_back(which, carry):
            acc[...] += dot_nt(grad_qkv[which], flat(attn_w[which]))
            take_near(UNITS - 3 + which)
            return carry

        lax.fori_loop(0, 3, input_back, 0)
        x_load.wait()
        gain_grad = jnp.zeros((1, width), F32)
        for tile in range(tokens // TILE):
            rows = pl.ds(tile * TILE, TILE)
            gain_piece, back = norm_back(acc[rows], x[rows].astype(F32), gain[0:1])
            gain_grad = gain_grad + gain_piece
            result[rows] = result[rows] + back
        gain_sum[0, 0:1] = gain_grad
        grad_store = pltpu.make_async_copy(result, grad_out, load.at[13])
        grad_store.start()
        output_store.wait()
        grad_store.wait()

    pl.run_scoped(
        attention,
        pltpu.VMEM((4, SHARDS, ROWS, COLS), BF16),
        pltpu.VMEM((2, tokens, 128), F32),
        pltpu.VMEM((3, tokens, width), BF16),
        pltpu.VMEM((16, tokens), F32),
        pltpu.VMEM((tokens, tokens), BF16),
        pltpu.VMEM((tokens, width), BF16),
        pltpu.VMEM((3, tokens, width), BF16),
        pltpu.VMEM((2, width, tokens), BF16),
        pltpu.VMEM((tokens, width), BF16),
        pltpu.VMEM((tokens, width), BF16),
    )

    first = 11
    gain_copy(0).start()

    def gain_step(step):
        gain_copy(step).wait_recv()
        gain_sum[step + 1] = gain_sum[step] + gain_got[step]
        if step + 1 < len(flips):
            gain_copy(step + 1).start()

    if pack > 1:
        lax.fori_loop(first, pack * (chunks + len(stages) - 1), lambda time, _: (post(time), _)[1], 0)
        for step in range(len(flips)):
            gain_step(step)
    else:
        plan = remaining(first)
        for number, (stage, chunk, third) in enumerate(plan):
            stage(chunk, third)
            left = len(plan) - 1 - number
            if left % 3 == 1 and left // 3 < len(flips):
                gain_step(len(flips) - 1 - left // 3)
    gain_out[...] = gain_sum[len(flips)]

    def settle(chunk, third=None):
        for piece in range(pack):
            far_copy(chunk * pack + piece, third).wait_send()
        for level in range(levels):
            over(level, lambda step: down_copy(level, chunk, step, third).wait_send())
            over(level, lambda step: up_copy(level, chunk, step, third).wait_send())
        store_copy(chunk, third).wait()

    lax.fori_loop(0, order.whole, lambda chunk, _: (settle(chunk), _)[1], 0)
    for chunk, third in order.items[order.whole :]:
        settle(chunk, third)
    for step in range(len(flips)):
        gain_copy(step).wait_send()


def backward_pass(scalars, tokens, cotangent, saved):
    count, width = tokens.shape
    replicas = lax.axis_size("replica")
    order = Levels(0, replicas)
    chunks = UNITS // order.pack
    flips = 2 + replicas.bit_length() - 1
    gain = saved[-2]
    part_shapes = [
        (chunks, members - 1) + order.size(level + 1) for level, members in enumerate(order.members)
    ]
    items = max(len(order.items), UNITS)
    counts = [(items, members - 1) for members in order.members]
    anywhere = pl.BlockSpec(memory_space=pl.ANY)
    shape = jax.ShapeDtypeStruct
    return pl.pallas_call(
        functools.partial(backward_kernel, replicas),
        out_shape=(
            shape((UNITS, ROWS, COLS), BF16),
            shape(gain.shape, F32),
            shape((count, width), BF16),
            shape((count, width), F32),
        ),
        in_specs=[pl.BlockSpec(memory_space=pltpu.SMEM)] * 2 + [anywhere] * (2 + len(saved)),
        out_specs=[anywhere, pl.BlockSpec(memory_space=pltpu.VMEM), anywhere, anywhere],
        scratch_shapes=[
            pltpu.VMEM((UNITS, SHARDS, ROWS, COLS), BF16),
            pltpu.VMEM((UNITS, 2, ROWS, COLS), BF16),
            pltpu.VMEM((UNITS, ROWS, COLS), BF16),
            pltpu.VMEM((flips + 1,) + gain.shape, F32),
            pltpu.VMEM((flips,) + gain.shape, F32),
            pltpu.VMEM((count, width), BF16),
            pltpu.VMEM(gain.shape, F32),
            pltpu.VMEM((width, count), BF16),
            pltpu.VMEM((count, width), F32),
            pltpu.VMEM((count, width), F32),
            pltpu.VMEM((count, width), F32),
        ]
        + [pltpu.VMEM(part, BF16) for part in part_shapes]
        + [

            DMA((14,)), DMA((2, 6)), DMA((UNITS, 2)), DMA((UNITS, 2)), DMA((items,)), DMA((items,)),
            DMA((items,)), DMA((flips,)), DMA((flips,)), DMA((FBLOCKS,)),
        ]
        + [DMA(count_) for _ in range(4) for count_ in counts],
        compiler_params=pltpu.CompilerParams(
            collective_id=1, has_side_effects=True, vmem_limit_bytes=67043328
        ),
        name="backward_reduce",
    )(*scalars, tokens, cotangent, *saved)


def finish_kernel(
    sums, gain_sums, output_in, grad_in,
    down, gate, up, out, query, key, value, gain_one, gain_two, output, grad,
    low, wide, held_output, held_grad, in_sem, out_sem,
):
    targets = [down.at[pl.ds(piece * ROWS, ROWS)] for piece in range(FBLOCKS)]
    for block in range(FBLOCKS):
        columns = pl.ds(block * COLS, COLS)
        targets += [gate.at[:, columns], up.at[:, columns]]
    targets += [out, query, key, value]
    moves = [(output_in, held_output, output), (grad_in, held_grad, grad)]
    ins = [
        pltpu.make_async_copy(sums.at[unit], low.at[unit], in_sem.at[unit]) for unit in range(UNITS)
    ]
    ins += [
        pltpu.make_async_copy(source, held, in_sem.at[UNITS + number])
        for number, (source, held, _) in enumerate(moves)
    ]
    puts = [
        pltpu.make_async_copy(wide.at[unit], target, out_sem.at[unit])
        for unit, target in enumerate(targets)
    ]
    puts += [
        pltpu.make_async_copy(held, target, out_sem.at[UNITS + number])
        for number, (_, held, target) in enumerate(moves)
    ]
    for copy in ins[UNITS:] + ins[:UNITS]:
        copy.start()
    share = gain_sums.shape[1] // SHARDS
    shard = lax.axis_index("shard")
    turned = pltpu.roll(gain_sums[...], (SHARDS - shard) % SHARDS * share, 1)
    gain_one[...] = turned[0:1, :share]
    gain_two[...] = turned[1:2, :share]
    for number in range(UNITS, UNITS + len(moves)):
        ins[number].wait()
        puts[number].start()
    for unit in range(UNITS):
        ins[unit].wait()
        wide[unit] = low[unit].astype(F32)
        puts[unit].start()
    for copy in puts:
        copy.wait()


def finish(sums, gain_sums, output, input_grad):
    shape = jax.ShapeDtypeStruct
    small, broad = shape((ROWS, COLS), F32), shape((ROWS, FBLOCKS * COLS), F32)
    share = shape((1, gain_sums.shape[1] // SHARDS), F32)
    hbm, vmem = pl.BlockSpec(memory_space=pltpu.HBM), pl.BlockSpec(memory_space=pltpu.VMEM)
    return pl.pallas_call(
        finish_kernel,
        out_shape=(
            shape((FBLOCKS * ROWS, COLS), F32), broad, broad, small, small, small, small, share, share,
            shape(output.shape, output.dtype), shape(input_grad.shape, F32),
        ),
        in_specs=[hbm, vmem, hbm, hbm],
        out_specs=[hbm] * 7 + [vmem] * 2 + [hbm] * 2,
        scratch_shapes=[
            pltpu.VMEM((UNITS, ROWS, COLS), BF16),
            pltpu.VMEM((UNITS, ROWS, COLS), F32),
            pltpu.VMEM(output.shape, output.dtype),
            pltpu.VMEM(input_grad.shape, F32),
            DMA((UNITS + 2,)),
            DMA((UNITS + 2,)),
        ],
        compiler_params=pltpu.CompilerParams(vmem_limit_bytes=67043328),
        name="finish",
    )(sums, gain_sums, output, input_grad)


def per_device(
    tokens, cotangent, lengths, assignment, positions, attention_gain, query_weight, key_weight,
    value_weight, out_weight, feedforward_gain, gate_weight, up_weight, down_weight,
):
    shard = lax.axis_index("shard")
    lane = lax.broadcasted_iota(jnp.int32, (8, tokens.shape[1]), 1)
    row = lax.broadcasted_iota(jnp.int32, (8, tokens.shape[1]), 0)
    share = attention_gain.shape[0]
    spread = [
        jnp.broadcast_to(gain, (SHARDS, share)).reshape(1, -1).astype(F32)
        for gain in (attention_gain, feedforward_gain)
    ]
    gain_rows = jnp.where(
        (lane // share == shard) & (row < 2), jnp.where(row == 0, spread[0], spread[1]), 0.0
    )
    saved = forward_pass(
        [lengths, assignment, positions],
        tokens,
        gain_rows,
        [query_weight, key_weight, value_weight, out_weight, gate_weight, up_weight, down_weight],
    )
    sums, gain_sums, output, input_grad = backward_pass(
        [lengths, assignment], tokens, cotangent, saved
    )
    down, gate, up, out, query, key, value, gain_one, gain_two, output, input_grad = finish(
        sums, gain_sums, output, input_grad
    )
    return (
        output,
        input_grad,
        gain_one.reshape(-1),
        query,
        key,
        value,
        out,
        gain_two.reshape(-1),
        gate,
        up,
        down,
    )


def solution(mesh):
    return jax.shard_map(
        per_device,
        mesh=mesh,
        in_specs=(
            P(("shard", "replica"), None),
            P(("shard", "replica"), None),
            P(),
            P(),
            P(("shard", "replica")),
            P("shard"),
            P("shard", None),
            P("shard", None),
            P("shard", None),
            P("shard", None),
            P("shard"),
            P("shard", None),
            P("shard", None),
            P("shard", None),
        ),
        out_specs=(
            P(("shard", "replica"), None),
            P(("shard", "replica"), None),
            P("shard"),
            P("shard", None),
            P("shard", None),
            P("shard", None),
            P("shard", None),
            P("shard"),
            P("shard", None),
            P("shard", None),
            P("shard", None),
        ),
        check_vma=False,
    )
```

```python
import functools
import math

import jax
import jax.numpy as jnp
from jax import lax
from jax.experimental import pallas as pl
from jax.experimental.pallas import tpu as pltpu
from jax.sharding import PartitionSpec as P

HEADS = 12
HDIM = 64
EPSILON = 1e-05
ROPE_BASE = 10000.0
MESH = pl.DeviceIdType.MESH
F32 = jnp.float32
BF16 = jnp.bfloat16
DMA = pltpu.SemaphoreType.DMA

ROWS = 192
COLS = 768
UNITS = 16
FBLOCKS = 4
SHARDS = 4
TILE = 256
TALL = 512


def toggle(index, stride):
    return index + (1 - 2 * ((index // stride) % 2)) * stride


def ring(index, members, stride):
    place = (index // stride) % members
    base = index - place * stride
    return place, [base + ((place + step) % members) * stride for step in range(1, members)]


def at(shard, replica):
    return {"shard": shard, "replica": replica}


def greet(peers):
    barrier = pltpu.get_barrier_semaphore()
    for peer in peers:
        pl.semaphore_signal(barrier, inc=1, device_id=peer, device_id_type=MESH)
    pl.semaphore_wait(barrier, len(peers))


def remote(source, target, send, receive, peer):
    return pltpu.make_async_remote_copy(
        src_ref=source,
        dst_ref=target,
        send_sem=send,
        recv_sem=receive,
        device_id=peer,
        device_id_type=MESH,
    )


def mult(start, step):
    return start if isinstance(start, int) else pl.multiple_of(start, step)


def span(start, size, step=16):
    return pl.ds(mult(start, step), size)


class Levels:
    def __init__(self, replica, count):
        self.replica = replica
        if count == 8:
            self.pack, self.members, self.strides = 1, [2, 4], [1, 2]
            self.cuts = [("rows", 2), ("quarters", 4)]
        else:
            assert count == 32
            self.pack, self.members, self.strides = 4, [2, 4, 4], [16, 4, 1]
            self.cuts = [("units", 2), ("halves", 4), ("quarters", 4)]
        self.count = len(self.members)
        self.whole = UNITS // self.pack
        self.items = [(chunk, None) for chunk in range(self.whole)]
        self.items += [
            (chunk, third) for chunk in range(self.whole, UNITS // self.pack) for third in range(3)
        ]

    def item(self, chunk, third):
        return chunk if third is None else self.whole + 3 * (chunk - self.whole) + third

    def group(self, level, chunk):
        return ring(self.replica, self.members[level], self.strides[level])

    def places(self, chunk):
        return [self.group(level, chunk)[0] for level in range(self.count)]

    def size(self, level):
        units, rows, columns = self.pack, ROWS, COLS
        for kind, _ in self.cuts[:level]:
            if kind == "units":
                units = units // 2
            elif kind == "rows":
                rows = rows // 2
            elif kind == "columns":
                columns = columns // 2
            elif kind == "halves":
                units, rows = units // 2, rows // 2
            else:
                rows, columns = rows // 2, columns // 2
        return units, rows, columns

    def region(self, chunk, third, places):
        unit, row, column = chunk * self.pack, 0, 0
        parts = 1
        if third is not None:
            parts, column = 3, third * (COLS // 3)
        for level, place in enumerate(places):
            kind = self.cuts[level][0]
            units, rows, columns = self.size(level + 1)
            columns = columns // parts
            if kind == "units":
                unit = unit + place * units
            elif kind == "rows":
                row = row + place * rows
            elif kind == "columns":
                column = column + place * columns
            elif kind == "halves":
                unit, row = unit + place // 2 * units, row + place % 2 * rows
            else:
                row, column = row + place // 2 * rows, column + place % 2 * columns
        units, rows, columns = self.size(len(places))
        return pl.ds(unit, units), span(row, rows), span(column, columns // parts, 128)


def dot(a, b):
    return jnp.dot(a, b, preferred_element_type=F32)


def dot_nt(a, b):
    return lax.dot_general(a, b, (((1,), (1,)), ((), ())), preferred_element_type=F32)


def dot_tn(a, b):
    return lax.dot_general(a, b, (((0,), (0,)), ((), ())), preferred_element_type=F32)


def flat(block):
    return block.reshape(-1, block.shape[-1])


def scale_of(values):
    return lax.rsqrt(jnp.mean(values * values, axis=-1, keepdims=True) + EPSILON)


def half_swap(values):
    lane = lax.broadcasted_iota(jnp.int32, values.shape, 1)
    return jnp.where(lane % 64 < 32, pltpu.roll(values, 96, 1), pltpu.roll(values, 32, 1))


def head_mask(which):
    lane = lax.broadcasted_iota(jnp.int32, (1, 128), 1)
    return jnp.where((lane < 64) == (which == 0), 1.0, 0.0).astype(BF16)


def own_length(lengths, assignment, device):
    total = jnp.int32(0)
    for number in range(lengths.shape[0]):
        total = total + jnp.where(assignment[number] == device, lengths[number], 0)
    return total


def rotation(start, length, tokens):
    row = lax.broadcasted_iota(jnp.int32, (tokens, 128), 0)
    lane = lax.broadcasted_iota(jnp.int32, (1, 128), 1)
    half = HDIM // 2
    frequency = jnp.exp((lane % half).astype(F32) * (-2.0 * math.log(ROPE_BASE) / HDIM))
    angles = jnp.where(row < length, row + start, 0).astype(F32) * frequency
    return jnp.cos(angles), jnp.sin(angles) * jnp.where(lane % HDIM < half, -1.0, 1.0)


def norm_back(grad_normed, values, gain):
    scale = scale_of(values)
    scaled = gain * grad_normed
    gain_grad = jnp.sum(grad_normed * values * scale, axis=0, keepdims=True)
    mean = jnp.mean(scaled * values, axis=-1, keepdims=True)
    return gain_grad, scale * scaled - values * (scale * scale * scale) * mean


def forward_kernel(
    lengths, assignment, positions, x_hbm, gain_hbm, q_hbm, k_hbm, v_hbm, o_hbm, g_hbm, u_hbm, d_hbm,
    w_out, qkv_out, nt_out, n2t_out, at_out, ht_out, hid_out, a_out, b_out, h1_out, lse_out, gain_out,
    tables_out,
    w, x, tables, gains, gain, normed, normed_t, qkv, bias, attended, lse, lse_t, h1, ht, hid, a, b,
    load, x_out, x_in, y_out, y_in, z_out, z_in, d_out, d_in, p_out, p_in, f_out, f_in, g_out, g_in,
    w_store, store, f_store,
):
    shard, replica = lax.axis_index("shard"), lax.axis_index("replica")
    partner, across = toggle(shard, 1), toggle(shard, 2)
    opposite = toggle(across, 1)
    beside, behind = toggle(replica, 1), toggle(replica, 2)
    mine = replica % 4
    quarter_beside, quarter_behind = toggle(mine, 1), toggle(mine, 2)
    quarter_last = toggle(quarter_beside, 2)
    tokens, width = x.shape

    sources = [q_hbm, k_hbm, v_hbm, o_hbm]
    for block in range(FBLOCKS):
        columns = pl.ds(block * COLS, COLS)
        sources += [g_hbm.at[:, columns], u_hbm.at[:, columns]]
    sources += [d_hbm.at[pl.ds(piece * ROWS, ROWS)] for piece in range(UNITS - len(sources))]
    loads = [
        pltpu.make_async_copy(source, w.at[unit, shard], load.at[unit])
        for unit, source in enumerate(sources)
    ]
    x_load = pltpu.make_async_copy(x_hbm, x, load.at[UNITS])
    gain_load = pltpu.make_async_copy(gain_hbm, gains.at[shard], load.at[UNITS + 1])
    gain_load.start()
    for copy in loads:
        copy.start()
    x_load.start()

    shard_peers = [at(partner, replica), at(across, replica), at(opposite, replica)]
    greet(shard_peers + [at(shard, beside), at(shard, behind)])

    gain_load.wait()
    gain_copies = [
        remote(gains.at[shard], gains.at[shard], g_out.at[number], g_in.at[number], peer)
        for number, peer in enumerate(shard_peers)
    ]
    for copy in gain_copies:
        copy.start()

    quarter = ROWS // 4

    def part(unit, owner, which):
        return w.at[unit, owner, span(which * quarter, quarter)]

    def cross(unit):
        piece = part(unit, shard, mine)
        return remote(piece, piece, x_out.at[unit], x_in.at[unit], at(across, replica))

    def share(unit):
        piece = w.at[unit, shard]
        return remote(piece, piece, p_out.at[unit], p_in.at[unit], at(partner, replica))

    def hand_beside(unit):
        piece = part(unit, across, mine)
        return remote(piece, piece, y_out.at[unit], y_in.at[unit], at(shard, beside))

    def hand_behind(unit):
        piece = part(unit, across, mine)
        return remote(piece, piece, z_out.at[unit], z_in.at[unit], at(shard, behind))

    def hand_on(unit, odd):
        piece = part(unit, across, quarter_beside if odd else quarter_behind)
        peer = at(shard, behind if odd else beside)
        return remote(piece, piece, d_out.at[unit], d_in.at[unit], peer)

    def by_parity(unit, act):
        for odd in range(2):
            pl.when(unit % 2 == odd)(functools.partial(act, odd))

    def forward(unit, number):
        which = (mine, quarter_beside, quarter_behind, quarter_last)[number]
        piece = part(unit, across, which)
        return remote(piece, piece, f_out.at[number, unit], f_in.at[number, unit], at(partner, replica))

    def keep(unit):
        return pltpu.make_async_copy(w.at[unit], w_out.at[unit], w_store.at[unit])

    for unit in range(UNITS):
        loads[unit].wait()
        cross(unit).start()
        share(unit).start()

    def take_cross(unit):
        cross(unit).wait_recv()
        hand_beside(unit).start()
        hand_behind(unit).start()
        forward(unit, 0).start()

    def take_hands(unit):
        hand_behind(unit).wait_recv()
        hand_beside(unit).wait_recv()
        by_parity(unit, lambda odd: hand_on(unit, odd).start())
        forward(unit, 1).start()
        forward(unit, 2).start()

    def take_last(unit):
        by_parity(unit, lambda odd: hand_on(unit, odd).wait_recv())
        forward(unit, 3).start()

    def complete(unit):
        share(unit).wait_recv()
        for number in range(4):
            forward(unit, number).wait_recv()
        keep(unit).start()

    stages = [(0, take_cross), (2, take_hands), (4, take_last), (5, complete)]

    def tick(time):
        for lag, stage in stages:
            pl.when((time >= lag) & (time < UNITS + lag))(functools.partial(stage, time - lag))

    def ticks(first, last):
        def body(time, carry):
            tick(time)
            return carry

        lax.fori_loop(first, last, body, 0)

    stores = []

    def save(source, target):
        copy = pltpu.make_async_copy(source, target, store.at[len(stores)])
        copy.start()
        stores.append(copy)

    row = lax.broadcasted_iota(jnp.int32, (tokens, tokens), 0)
    column = lax.broadcasted_iota(jnp.int32, (tokens, tokens), 1)
    device = shard * lax.axis_size("replica") + replica
    length = own_length(lengths, assignment, device)
    seen = (column <= row) & ((row < length) | (column >= length))
    bias[...] = jnp.where(seen, 0.0, -jnp.inf)

    x_load.wait()
    for copy in gain_copies:
        copy.wait_recv()
    gain[...] = gains[0] + gains[1] + gains[2] + gains[3]
    save(gain, gain_out)
    values = x[...].astype(F32)
    normed[...] = (values * scale_of(values) * gain[0:1]).astype(BF16)
    normed_t[0] = normed[...].T
    save(normed_t.at[0], nt_out)
    tables[0], tables[1] = rotation(positions[0], length, tokens)
    save(tables, tables_out)
    ticks(0, 8)

    def project(which, carry):
        product = dot(normed[...], flat(w[which]))
        cosine = jnp.where(which < 2, tables[0], 1.0)
        sine = jnp.where(which < 2, tables[1], 0.0)
        for pair in range(width // 128):
            columns = slice(pair * 128, pair * 128 + 128)
            piece = product[:, columns]
            qkv[which, :, columns] = (piece * cosine + half_swap(piece) * sine).astype(BF16)
        return carry

    lax.fori_loop(0, 3, project, 0)
    save(qkv, qkv_out)
    tick(8)
    lse[...] = jnp.zeros_like(lse)

    def attend(pair, carry):
        columns = span(pair * 128, 128, 128)
        for tile in range(tokens // TILE):
            rows = pl.ds(tile * TILE, TILE)
            keys = (tile + 1) * TILE
            query = qkv[0, rows, columns]
            key = qkv[1, 0:keys, columns]
            value = qkv[2, 0:keys, columns]
            mixed = []
            logs = lse[rows]
            lane = lax.broadcasted_iota(jnp.int32, logs.shape, 1)
            for which in range(2):
                scores = dot_nt(query * head_mask(which), key) * (1.0 / math.sqrt(HDIM))
                scores = scores + bias[rows, 0:keys]
                peak = jnp.max(scores, axis=-1, keepdims=True)
                exponent = jnp.exp(scores - peak)
                total = jnp.sum(exponent, axis=-1, keepdims=True)
                probability = (exponent * (1.0 / total)).astype(BF16)
                mixed.append(dot(probability, value))
                logs = jnp.where(lane == 2 * pair + which, peak + jnp.log(total), logs)
            lse[rows] = logs
            first = lax.broadcasted_iota(jnp.int32, mixed[0].shape, 1) < 64
            attended[rows, columns] = jnp.where(first, mixed[0], mixed[1]).astype(BF16)
        tick(9 + pair)
        return carry

    lax.fori_loop(0, HEADS // 2, attend, 0)
    normed_t[1] = attended[...].T
    save(normed_t.at[1], at_out)
    lse_t[...] = lse[...].T
    save(lse_t, lse_out)
    for tile in range(tokens // TILE):
        rows = pl.ds(tile * TILE, TILE)
        hidden_one = x[rows].astype(F32) + dot(attended[rows], flat(w[3]))
        h1[rows] = hidden_one
        normed[rows] = (hidden_one * scale_of(hidden_one) * gain[1:2]).astype(BF16)
    save(h1, h1_out)
    normed_t[2] = normed[...].T
    save(normed_t.at[2], n2t_out)

    def f_copies(block):
        pairs = [
            (hid.at[block], hid_out.at[block]),
            (a.at[block], a_out.at[block]),
            (b.at[block], b_out.at[block]),
            (ht.at[:, block], ht_out.at[:, block]),
        ]
        return [
            pltpu.make_async_copy(source, target, f_store.at[block, number])
            for number, (source, target) in enumerate(pairs)
        ]

    def feed(block, carry):
        def rows_of(tile, inner):
            rows = span(tile * TALL, TALL)
            gate = dot(normed[rows], flat(w[4 + 2 * block]))
            upward = dot(normed[rows], flat(w[5 + 2 * block]))
            sigmoid = jax.nn.sigmoid(gate)
            activated = gate * sigmoid
            hid[block, rows] = (activated * upward).astype(BF16)
            a[block, rows] = (upward * sigmoid * (1.0 + gate * (1.0 - sigmoid))).astype(BF16)
            b[block, rows] = activated.astype(BF16)
            return inner

        lax.fori_loop(0, tokens // TALL, rows_of, 0)
        turned = hid[block].T
        for piece in range(FBLOCKS):
            ht[piece, block] = turned[piece * ROWS : (piece + 1) * ROWS]
        for copy in f_copies(block):
            copy.start()
        tick(15 + block)
        return carry

    lax.fori_loop(0, FBLOCKS, feed, 0)
    ticks(15 + FBLOCKS, UNITS + 5)

    def settle(unit, carry):
        cross(unit).wait_send()
        share(unit).wait_send()
        hand_beside(unit).wait_send()
        hand_behind(unit).wait_send()
        by_parity(unit, lambda odd: hand_on(unit, odd).wait_send())
        for number in range(4):
            forward(unit, number).wait_send()
        keep(unit).wait()
        return carry

    lax.fori_loop(0, UNITS, settle, 0)
    for copy in gain_copies:
        copy.wait_send()
    for copy in stores:
        copy.wait()
    for block in range(FBLOCKS):
        for copy in f_copies(block):
            copy.wait()


def forward_pass(scalars, tokens, gain_rows, weights):
    count, width = tokens.shape
    shape = jax.ShapeDtypeStruct
    outs = (
        shape((UNITS, SHARDS, ROWS, COLS), BF16),
        shape((3, count, width), BF16),
        shape((width, count), BF16),
        shape((width, count), BF16),
        shape((width, count), BF16),
        shape((FBLOCKS, FBLOCKS, ROWS, count), BF16),
        shape((FBLOCKS, count, COLS), BF16),
        shape((FBLOCKS, count, COLS), BF16),
        shape((FBLOCKS, count, COLS), BF16),
        shape((count, width), F32),
        shape((128, count), F32),
        shape(gain_rows.shape, F32),
        shape((2, count, 128), F32),
    )
    anywhere = pl.BlockSpec(memory_space=pl.ANY)
    return pl.pallas_call(
        forward_kernel,
        out_shape=outs,
        in_specs=[pl.BlockSpec(memory_space=pltpu.SMEM)] * 3 + [anywhere] * 9,
        out_specs=[anywhere] * len(outs),
        scratch_shapes=[
            pltpu.VMEM((UNITS, SHARDS, ROWS, COLS), BF16),
            pltpu.VMEM((count, width), BF16),
            pltpu.VMEM((2, count, 128), F32),
            pltpu.VMEM((SHARDS,) + gain_rows.shape, F32),
            pltpu.VMEM(gain_rows.shape, F32),
            pltpu.VMEM((count, width), BF16),
            pltpu.VMEM((3, width, count), BF16),
            pltpu.VMEM((3, count, width), BF16),
            pltpu.VMEM((count, count), F32),
            pltpu.VMEM((count, width), BF16),
            pltpu.VMEM((count, 128), F32),
            pltpu.VMEM((128, count), F32),
            pltpu.VMEM((count, width), F32),
            pltpu.VMEM((FBLOCKS, FBLOCKS, ROWS, count), BF16),
            pltpu.VMEM((FBLOCKS, count, COLS), BF16),
            pltpu.VMEM((FBLOCKS, count, COLS), BF16),
            pltpu.VMEM((FBLOCKS, count, COLS), BF16),
            DMA((UNITS + 2,)),
        ]
        + [DMA((UNITS,))] * 10
        + [
            DMA((4, UNITS)), DMA((4, UNITS)), DMA((3,)), DMA((3,)),
            DMA((UNITS,)), DMA((8,)), DMA((FBLOCKS, 4)),
        ],
        compiler_params=pltpu.CompilerParams(
            collective_id=0, has_side_effects=True, vmem_limit_bytes=60 * 1024 * 1024
        ),
        name="forward_gather",
    )(*scalars, tokens, gain_rows, *weights)


def backward_kernel(
    replicas,
    lengths, assignment, x_hbm, cot_hbm, w_hbm, qkv_hbm, nt_hbm, n2t_hbm, at_hbm, ht_hbm,
    hid_hbm, a_hbm, b_hbm, h1_hbm, lse_hbm, gain_hbm, tables_hbm,
    sums_out, gain_out, output_out, grad_out,
    *refs,
):
    shard, replica = lax.axis_index("shard"), lax.axis_index("replica")
    order = Levels(replica, replicas)
    levels, pack = order.count, order.pack
    (grads, near, far, gain_sum, gain_got, gbt, gain, n2t, h1, acc, result) = refs[:11]
    parts = refs[11 : 11 + levels]
    sems = refs[11 + levels :]
    (load, s_load, near_out, near_in, far_out, far_in, store, gain_send, gain_recv) = sems[:9]
    ht_sem = sems[9]
    down_out, down_in, up_out, up_in = (
        sems[10 + kind * levels : 10 + (kind + 1) * levels] for kind in range(4)
    )
    partner, across = toggle(shard, 1), toggle(shard, 2)
    opposite = toggle(across, 1)
    tokens, width = gbt.shape
    length = own_length(lengths, assignment, shard * lax.axis_size("replica") + replica)
    flips = [at(partner, replica), at(across, replica)]
    stride = 1
    while stride < replicas:
        flips.append(at(shard, toggle(replica, stride)))
        stride *= 2

    def fetch(source, target, number):
        copy = pltpu.make_async_copy(source, target, load.at[number])
        copy.start()
        return copy

    cot_load = fetch(cot_hbm, gbt, 0)
    n2t_load = fetch(n2t_hbm, n2t, 1)
    h1_load = fetch(h1_hbm, h1, 2)
    gain_load = fetch(gain_hbm, gain, 4)

    greet(
        [at(partner, replica), at(across, replica)]
        + [at(shard, other) for level in range(levels) for other in order.group(level, 0)[1]]
    )

    chunks = UNITS // pack

    def view(owner, chunk, third, places):
        units, rows, columns = order.region(chunk, third, places)
        return grads.at[units, owner, rows, columns]

    def near_copy(unit, which):
        return remote(
            grads.at[unit, opposite if which == 0 else partner],
            near.at[unit, which],
            near_out.at[unit, which],
            near_in.at[unit, which],
            at(partner, replica),
        )

    def columns_of(third, width):
        return pl.ds(0, width) if third is None else pl.ds(third * (width // 3), width // 3)

    def far_copy(unit, third=None):
        columns = columns_of(third, COLS)
        item = order.item(unit, third)
        return remote(
            grads.at[unit, across, :, columns],
            far.at[unit, :, columns],
            far_out.at[item],
            far_in.at[item],
            at(across, replica),
        )

    def part(level, chunk, third, step):
        width = order.size(level + 1)[2]
        return parts[level].at[chunk, step, :, :, columns_of(third, width)]

    def down_copy(level, chunk, step, third=None):
        members = order.members[level]
        place, others = order.group(level, chunk)
        theirs = (place + step + 1) % members
        item = order.item(chunk, third)
        return remote(
            view(shard, chunk, third, order.places(chunk)[:level] + [theirs]),
            part(level, chunk, third, step),
            down_out[level].at[item, step],
            down_in[level].at[item, step],
            at(shard, others[step]),
        )

    def up_copy(level, chunk, step, third=None):
        piece = view(partner, chunk, third, order.places(chunk)[: level + 1])
        item = order.item(chunk, third)
        return remote(
            piece,
            piece,
            up_out[level].at[item, step],
            up_in[level].at[item, step],
            at(shard, order.group(level, chunk)[1][step]),
        )

    def store_copy(chunk, third=None):
        units = pl.ds(chunk * pack, pack)
        columns = columns_of(third, COLS)
        return pltpu.make_async_copy(
            grads.at[units, partner, :, columns],
            sums_out.at[units, :, columns],
            store.at[order.item(chunk, third)],
        )

    def over(level, act):
        for step in range(order.members[level] - 1):
            act(step)

    def give(unit):
        for which in range(2):
            near_copy(unit, which).start()

    def plus(*terms):
        total = terms[0].astype(F32)
        for term in terms[1:]:
            total = total + term.astype(F32)
        return total.astype(BF16)

    def take_near(unit):
        near_copy(unit, 0).wait_recv()
        grads[unit, across] = plus(grads[unit, across], near[unit, 0])
        if pack > 1:
            far_copy(unit).start()
        else:
            pl.when(unit < order.whole)(lambda: far_copy(unit).start())

            @pl.when(unit >= order.whole)
            def _():
                for third in range(3):
                    far_copy(unit, third).start()

        near_copy(unit, 1).wait_recv()
        grads[unit, shard] = plus(grads[unit, shard], near[unit, 1])

    def take_far(chunk, third=None):
        for piece in range(pack):
            unit = chunk * pack + piece
            if third is None or third == 0:
                near_copy(unit, 0).wait_send()
                near_copy(unit, 1).wait_send()
            far_copy(unit, third).wait_recv()
            columns = columns_of(third, COLS)
            grads[unit, shard, :, columns] = plus(
                grads[unit, shard, :, columns], far[unit, :, columns]
            )
        over(0, lambda step: down_copy(0, chunk, step, third).start())

    def take_down(level, chunk, third=None):
        over(level, lambda step: down_copy(level, chunk, step, third).wait_recv())
        places = order.places(chunk)[: level + 1]
        terms = [view(shard, chunk, third, places)[...]]
        terms += [part(level, chunk, third, step)[...] for step in range(order.members[level] - 1)]
        total = plus(*terms)
        if level + 1 < levels:
            view(shard, chunk, third, places)[...] = total
            over(level + 1, lambda step: down_copy(level + 1, chunk, step, third).start())
        else:
            view(partner, chunk, third, places)[...] = total
            over(level, lambda step: up_copy(level, chunk, step, third).start())

    def take_up(level, chunk, third=None):
        over(level, lambda step: up_copy(level, chunk, step, third).wait_recv())
        if level > 0:
            over(level - 1, lambda step: up_copy(level - 1, chunk, step, third).start())
        else:
            store_copy(chunk, third).start()

    stages = [take_far]
    stages += [functools.partial(take_down, level) for level in range(levels)]
    stages += [functools.partial(take_up, level) for level in reversed(range(levels))]

    def post(time):
        step = (time + 1) // pack - 1
        for lag, stage in enumerate(stages):
            good = (step >= lag) & (step < chunks + lag) & ((time + 1) % pack == 0)
            pl.when(good)(functools.partial(stage, step - lag))

    def remaining(first):
        arrival, found = 0.0, []
        for chunk, third in order.items:
            pace = 1.0 if third is None else 1.0 / 3
            arrival += pace
            wait = (0.0, 1.02, 2.02, 3.02, 4.02) if third is None else (0.0, 0.68, 1.36, 2.04, 2.72)
            for lag, stage in enumerate(stages):
                if chunk + lag >= first:
                    found.append((arrival + wait[lag], lag, len(found), stage, chunk, third))
        return [entry[3:] for entry in sorted(found, key=lambda entry: entry[:3])]

    def gain_copy(step):
        return remote(
            gain_sum.at[step], gain_got.at[step], gain_send.at[step], gain_recv.at[step], flips[step]
        )

    row = lax.broadcasted_iota(jnp.int32, (tokens, 1), 0)
    valid = jnp.where(row < length, 1.0, 0.0)

    def down_phase(ht):
        ht_loads = [
            pltpu.make_async_copy(ht_hbm.at[unit], ht.at[unit], ht_sem.at[unit])
            for unit in range(FBLOCKS)
        ]
        for copy in ht_loads:
            copy.start()
        cot_load.wait()
        gbt[...] = (gbt[...].astype(F32) * valid).astype(BF16)

        def down_grads(unit, carry):
            pltpu.make_async_copy(ht_hbm.at[unit], ht.at[unit], ht_sem.at[unit]).wait()
            product = dot(flat(ht[unit]), gbt[...]).astype(BF16)
            grads[unit] = product.reshape(SHARDS, ROWS, COLS)
            give(unit)
            pl.when(unit >= 1)(lambda: take_near(unit - 1))
            return carry

        lax.fori_loop(0, FBLOCKS, down_grads, 0)

    def feed_forward(down_w, gate_w, up_w, hid, grad_pair):
        def stream(block):
            slot = block % 2
            pairs = [
                (w_hbm.at[pl.ds(UNITS - FBLOCKS, FBLOCKS), block], down_w.at[slot]),
                (w_hbm.at[4 + 2 * block], gate_w.at[slot]),
                (w_hbm.at[5 + 2 * block], up_w.at[slot]),
                (hid_hbm.at[block], hid.at[slot]),
                (a_hbm.at[block], grad_pair.at[slot, 0]),
                (b_hbm.at[block], grad_pair.at[slot, 1]),
            ]
            return [
                pltpu.make_async_copy(source, target, s_load.at[slot, number])
                for number, (source, target) in enumerate(pairs)
            ]

        for copy in stream(0):
            copy.start()
        n2t_load.wait()
        acc[...] = jnp.zeros_like(acc)
        result[...] = jnp.zeros_like(result)

        def block_step(block, carry):
            slot = block % 2

            @pl.when(block + 1 < FBLOCKS)
            def _():
                for copy in stream(block + 1):
                    copy.start()

            for copy in stream(block):
                copy.wait()

            grad_hidden = dot_nt(gbt[...], flat(down_w[slot]))
            grad_pair[slot, 0] = (grad_hidden * grad_pair[slot, 0].astype(F32)).astype(BF16)
            grad_pair[slot, 1] = (grad_hidden * grad_pair[slot, 1].astype(F32)).astype(BF16)
            pl.when(block == 0)(lambda: take_near(FBLOCKS - 1))

            def kind_of(kind, inner):
                unit = FBLOCKS + 2 * block + kind
                product = dot(n2t[...], grad_pair[slot, kind]).astype(BF16)
                grads[unit] = product.reshape(SHARDS, ROWS, COLS)
                give(unit)
                return inner

            lax.fori_loop(0, 2, kind_of, 0)

            post(2 * block - block // 3)
            acc[...] += dot_nt(grad_pair[slot, 0], flat(gate_w[slot])) + dot_nt(
                grad_pair[slot, 1], flat(up_w[slot])
            )
            result[...] += dot(hid[slot], flat(down_w[slot]))
            take_near(FBLOCKS + 2 * block)
            take_near(FBLOCKS + 2 * block + 1)
            pl.when(block != 2)(lambda: post(2 * block + 1 - block // 3))
            return carry

        lax.fori_loop(0, FBLOCKS, block_step, 0)

    pl.run_scoped(down_phase, pltpu.VMEM((FBLOCKS, FBLOCKS, ROWS, tokens), BF16))
    pl.run_scoped(
        feed_forward,
        pltpu.VMEM((2, FBLOCKS, ROWS, COLS), BF16),
        pltpu.VMEM((2, SHARDS, ROWS, COLS), BF16),
        pltpu.VMEM((2, SHARDS, ROWS, COLS), BF16),
        pltpu.VMEM((2, tokens, COLS), BF16),
        pltpu.VMEM((2, 2, tokens, COLS), BF16),
    )

    def attention(attn_w, tables, qkv, lse, bias, grad_attended, grad_qkv, turned, x, out_low):
        at_load = fetch(at_hbm, turned.at[0], 5)
        w_load = fetch(w_hbm.at[pl.ds(0, 4)], attn_w, 8)
        qkv_load = fetch(qkv_hbm, qkv, 9)
        lse_load = fetch(lse_hbm.at[pl.ds(0, 16)], lse, 10)
        table_load = fetch(tables_hbm, tables, 11)
        nt_load = fetch(nt_hbm, turned.at[1], 6)
        x_load = fetch(x_hbm, x, 3)
        h1_load.wait()
        gain_load.wait()

        gain_grad = jnp.zeros((1, width), F32)
        for tile in range(tokens // TILE):
            rows = pl.ds(tile * TILE, TILE)
            good = jnp.where(
                lax.broadcasted_iota(jnp.int32, (TILE, 1), 0) + tile * TILE < length, 1.0, 0.0
            )
            out_low[rows] = ((h1[rows] + result[rows]) * good).astype(BF16)
            gain_piece, back = norm_back(acc[rows], h1[rows], gain[1:2])
            gain_grad = gain_grad + gain_piece
            grad_one = gbt[rows].astype(F32) + back
            result[rows] = grad_one
            gbt[rows] = grad_one.astype(BF16)
        gain_sum[0] = jnp.zeros_like(gain_sum[0])
        gain_sum[0, 1:2] = gain_grad
        output_store = pltpu.make_async_copy(out_low, output_out, load.at[12])
        output_store.start()
        at_load.wait()
        product = dot(turned[0], gbt[...]).astype(BF16)
        grads[UNITS - 4] = product.reshape(SHARDS, ROWS, COLS)
        give(UNITS - 4)
        w_load.wait()
        for tile in range(tokens // TILE):
            rows = pl.ds(tile * TILE, TILE)
            grad_attended[rows] = dot_nt(gbt[rows], flat(attn_w[3])).astype(BF16)
        take_near(UNITS - 4)
        post(7)

        key_row = lax.broadcasted_iota(jnp.int32, (tokens, tokens), 0)
        query_column = lax.broadcasted_iota(jnp.int32, (tokens, tokens), 1)
        seen = (key_row <= query_column) & ((query_column < length) | (key_row >= length))
        bias[...] = jnp.where(seen, 0.0, -jnp.inf).astype(BF16)
        qkv_load.wait()
        lse_load.wait()
        table_load.wait()
        inv_root = 1.0 / math.sqrt(HDIM)

        def attend_back(pair, carry):
            columns = span(pair * 128, 128, 128)
            grad_key = [jnp.zeros((TILE, 128), F32) for _ in range(tokens // TILE)]
            grad_value = [jnp.zeros((TILE, 128), F32) for _ in range(tokens // TILE)]
            for tile in range(tokens // TILE):
                rows = pl.ds(tile * TILE, TILE)
                query = qkv[0, rows, columns]
                grad_mixed = grad_attended[rows, columns]
                grad_query = jnp.zeros((TILE, 128), F32)
                for which in range(2):
                    mask = head_mask(which)
                    query_one = query * mask
                    mixed_one = grad_mixed * mask
                    log_row = lse[pl.ds(2 * pair + which, 1), rows]
                    probs, grad_probs = [], []
                    row_dot = jnp.zeros((1, TILE), F32)
                    for block in range(tile + 1):
                        keys = pl.ds(block * TILE, TILE)
                        scores = dot_nt(qkv[1, keys, columns], query_one) * inv_root
                        prob = jnp.exp(scores + bias[keys, rows].astype(F32) - log_row)
                        grad_value[block] += dot(prob.astype(BF16), mixed_one)
                        grad_prob = dot_nt(qkv[2, keys, columns], mixed_one)
                        row_dot = row_dot + jnp.sum(prob * grad_prob, axis=0, keepdims=True)
                        probs.append(prob)
                        grad_probs.append(grad_prob)
                    for block in range(tile + 1):
                        keys = pl.ds(block * TILE, TILE)
                        grad_scores = (probs[block] * (grad_probs[block] - row_dot)).astype(BF16)
                        grad_key[block] += dot(grad_scores, query_one)
                        grad_query += dot_tn(grad_scores, qkv[1, keys, columns] * mask)
                grad_query = grad_query * inv_root
                grad_query = grad_query * tables[0, rows] - half_swap(grad_query) * tables[1, rows]
                grad_qkv[0, rows, columns] = grad_query.astype(BF16)
            for block in range(tokens // TILE):
                keys = pl.ds(block * TILE, TILE)
                back = grad_key[block] * inv_root
                back = back * tables[0, keys] - half_swap(back) * tables[1, keys]
                grad_qkv[1, keys, columns] = back.astype(BF16)
                grad_qkv[2, keys, columns] = grad_value[block].astype(BF16)
            pl.when(pair % 2 == 1)(lambda: post(8 + pair // 2))
            return carry

        lax.fori_loop(0, HEADS // 2, attend_back, 0)
        nt_load.wait()

        def projection(which, carry):
            product = dot(turned[1], grad_qkv[which]).astype(BF16)
            grads[UNITS - 3 + which] = product.reshape(SHARDS, ROWS, COLS)
            give(UNITS - 3 + which)
            return carry

        lax.fori_loop(0, 3, projection, 0)
        acc[...] = jnp.zeros_like(acc)

        def input_back(which, carry):
            acc[...] += dot_nt(grad_qkv[which], flat(attn_w[which]))
            take_near(UNITS - 3 + which)
            return carry

        lax.fori_loop(0, 3, input_back, 0)
        x_load.wait()
        gain_grad = jnp.zeros((1, width), F32)
        for tile in range(tokens // TILE):
            rows = pl.ds(tile * TILE, TILE)
            gain_piece, back = norm_back(acc[rows], x[rows].astype(F32), gain[0:1])
            gain_grad = gain_grad + gain_piece
            result[rows] = result[rows] + back
        gain_sum[0, 0:1] = gain_grad
        grad_store = pltpu.make_async_copy(result, grad_out, load.at[13])
        grad_store.start()
        output_store.wait()
        grad_store.wait()

    pl.run_scoped(
        attention,
        pltpu.VMEM((4, SHARDS, ROWS, COLS), BF16),
        pltpu.VMEM((2, tokens, 128), F32),
        pltpu.VMEM((3, tokens, width), BF16),
        pltpu.VMEM((16, tokens), F32),
        pltpu.VMEM((tokens, tokens), BF16),
        pltpu.VMEM((tokens, width), BF16),
        pltpu.VMEM((3, tokens, width), BF16),
        pltpu.VMEM((2, width, tokens), BF16),
        pltpu.VMEM((tokens, width), BF16),
        pltpu.VMEM((tokens, width), BF16),
    )

    first = 11
    gain_copy(0).start()

    def gain_step(step):
        gain_copy(step).wait_recv()
        gain_sum[step + 1] = gain_sum[step] + gain_got[step]
        if step + 1 < len(flips):
            gain_copy(step + 1).start()

    if pack > 1:
        lax.fori_loop(first, pack * (chunks + len(stages) - 1), lambda time, _: (post(time), _)[1], 0)
        for step in range(len(flips)):
            gain_step(step)
    else:
        plan = remaining(first)
        for number, (stage, chunk, third) in enumerate(plan):
            stage(chunk, third)
            left = len(plan) - 1 - number
            if left % 3 == 1 and left // 3 < len(flips):
                gain_step(len(flips) - 1 - left // 3)
    gain_out[...] = gain_sum[len(flips)]

    def settle(chunk, third=None):
        for piece in range(pack):
            far_copy(chunk * pack + piece, third).wait_send()
        for level in range(levels):
            over(level, lambda step: down_copy(level, chunk, step, third).wait_send())
            over(level, lambda step: up_copy(level, chunk, step, third).wait_send())
        store_copy(chunk, third).wait()

    lax.fori_loop(0, order.whole, lambda chunk, _: (settle(chunk), _)[1], 0)
    for chunk, third in order.items[order.whole :]:
        settle(chunk, third)
    for step in range(len(flips)):
        gain_copy(step).wait_send()


def backward_pass(scalars, tokens, cotangent, saved):
    count, width = tokens.shape
    replicas = lax.axis_size("replica")
    order = Levels(0, replicas)
    chunks = UNITS // order.pack
    flips = 2 + replicas.bit_length() - 1
    gain = saved[-2]
    part_shapes = [
        (chunks, members - 1) + order.size(level + 1) for level, members in enumerate(order.members)
    ]
    items = max(len(order.items), UNITS)
    counts = [(items, members - 1) for members in order.members]
    anywhere = pl.BlockSpec(memory_space=pl.ANY)
    shape = jax.ShapeDtypeStruct
    return pl.pallas_call(
        functools.partial(backward_kernel, replicas),
        out_shape=(
            shape((UNITS, ROWS, COLS), BF16),
            shape(gain.shape, F32),
            shape((count, width), BF16),
            shape((count, width), F32),
        ),
        in_specs=[pl.BlockSpec(memory_space=pltpu.SMEM)] * 2 + [anywhere] * (2 + len(saved)),
        out_specs=[anywhere, pl.BlockSpec(memory_space=pltpu.VMEM), anywhere, anywhere],
        scratch_shapes=[
            pltpu.VMEM((UNITS, SHARDS, ROWS, COLS), BF16),
            pltpu.VMEM((UNITS, 2, ROWS, COLS), BF16),
            pltpu.VMEM((UNITS, ROWS, COLS), BF16),
            pltpu.VMEM((flips + 1,) + gain.shape, F32),
            pltpu.VMEM((flips,) + gain.shape, F32),
            pltpu.VMEM((count, width), BF16),
            pltpu.VMEM(gain.shape, F32),
            pltpu.VMEM((width, count), BF16),
            pltpu.VMEM((count, width), F32),
            pltpu.VMEM((count, width), F32),
            pltpu.VMEM((count, width), F32),
        ]
        + [pltpu.VMEM(part, BF16) for part in part_shapes]
        + [

            DMA((14,)), DMA((2, 6)), DMA((UNITS, 2)), DMA((UNITS, 2)), DMA((items,)), DMA((items,)),
            DMA((items,)), DMA((flips,)), DMA((flips,)), DMA((FBLOCKS,)),
        ]
        + [DMA(count_) for _ in range(4) for count_ in counts],
        compiler_params=pltpu.CompilerParams(
            collective_id=1, has_side_effects=True, vmem_limit_bytes=67043328
        ),
        name="backward_reduce",
    )(*scalars, tokens, cotangent, *saved)


def finish_kernel(
    sums, gain_sums, output_in, grad_in,
    down, gate, up, out, query, key, value, gain_one, gain_two, output, grad,
    low, wide, held_output, held_grad, in_sem, out_sem,
):
    targets = [down.at[pl.ds(piece * ROWS, ROWS)] for piece in range(FBLOCKS)]
    for block in range(FBLOCKS):
        columns = pl.ds(block * COLS, COLS)
        targets += [gate.at[:, columns], up.at[:, columns]]
    targets += [out, query, key, value]
    moves = [(output_in, held_output, output), (grad_in, held_grad, grad)]
    ins = [
        pltpu.make_async_copy(sums.at[unit], low.at[unit], in_sem.at[unit]) for unit in range(UNITS)
    ]
    ins += [
        pltpu.make_async_copy(source, held, in_sem.at[UNITS + number])
        for number, (source, held, _) in enumerate(moves)
    ]
    puts = [
        pltpu.make_async_copy(wide.at[unit], target, out_sem.at[unit])
        for unit, target in enumerate(targets)
    ]
    puts += [
        pltpu.make_async_copy(held, target, out_sem.at[UNITS + number])
        for number, (_, held, target) in enumerate(moves)
    ]
    for copy in ins[UNITS:] + ins[:UNITS]:
        copy.start()
    share = gain_sums.shape[1] // SHARDS
    shard = lax.axis_index("shard")
    turned = pltpu.roll(gain_sums[...], (SHARDS - shard) % SHARDS * share, 1)
    gain_one[...] = turned[0:1, :share]
    gain_two[...] = turned[1:2, :share]
    for number in range(UNITS, UNITS + len(moves)):
        ins[number].wait()
        puts[number].start()
    for unit in range(UNITS):
        ins[unit].wait()
        wide[unit] = low[unit].astype(F32)
        puts[unit].start()
    for copy in puts:
        copy.wait()


def finish(sums, gain_sums, output, input_grad):
    shape = jax.ShapeDtypeStruct
    small, broad = shape((ROWS, COLS), F32), shape((ROWS, FBLOCKS * COLS), F32)
    share = shape((1, gain_sums.shape[1] // SHARDS), F32)
    hbm, vmem = pl.BlockSpec(memory_space=pltpu.HBM), pl.BlockSpec(memory_space=pltpu.VMEM)
    return pl.pallas_call(
        finish_kernel,
        out_shape=(
            shape((FBLOCKS * ROWS, COLS), F32), broad, broad, small, small, small, small, share, share,
            shape(output.shape, output.dtype), shape(input_grad.shape, F32),
        ),
        in_specs=[hbm, vmem, hbm, hbm],
        out_specs=[hbm] * 7 + [vmem] * 2 + [hbm] * 2,
        scratch_shapes=[
            pltpu.VMEM((UNITS, ROWS, COLS), BF16),
            pltpu.VMEM((UNITS, ROWS, COLS), F32),
            pltpu.VMEM(output.shape, output.dtype),
            pltpu.VMEM(input_grad.shape, F32),
            DMA((UNITS + 2,)),
            DMA((UNITS + 2,)),
        ],
        compiler_params=pltpu.CompilerParams(vmem_limit_bytes=67043328),
        name="finish",
    )(sums, gain_sums, output, input_grad)


def per_device(
    tokens, cotangent, lengths, assignment, positions, attention_gain, query_weight, key_weight,
    value_weight, out_weight, feedforward_gain, gate_weight, up_weight, down_weight,
):
    shard = lax.axis_index("shard")
    lane = lax.broadcasted_iota(jnp.int32, (8, tokens.shape[1]), 1)
    row = lax.broadcasted_iota(jnp.int32, (8, tokens.shape[1]), 0)
    share = attention_gain.shape[0]
    spread = [
        jnp.broadcast_to(gain, (SHARDS, share)).reshape(1, -1).astype(F32)
        for gain in (attention_gain, feedforward_gain)
    ]
    gain_rows = jnp.where(
        (lane // share == shard) & (row < 2), jnp.where(row == 0, spread[0], spread[1]), 0.0
    )
    saved = forward_pass(
        [lengths, assignment, positions],
        tokens,
        gain_rows,
        [query_weight, key_weight, value_weight, out_weight, gate_weight, up_weight, down_weight],
    )
    sums, gain_sums, output, input_grad = backward_pass(
        [lengths, assignment], tokens, cotangent, saved
    )
    down, gate, up, out, query, key, value, gain_one, gain_two, output, input_grad = finish(
        sums, gain_sums, output, input_grad
    )
    return (
        output,
        input_grad,
        gain_one.reshape(-1),
        query,
        key,
        value,
        out,
        gain_two.reshape(-1),
        gate,
        up,
        down,
    )


def solution(mesh):
    return jax.shard_map(
        per_device,
        mesh=mesh,
        in_specs=(
            P(("shard", "replica"), None),
            P(("shard", "replica"), None),
            P(),
            P(),
            P(("shard", "replica")),
            P("shard"),
            P("shard", None),
            P("shard", None),
            P("shard", None),
            P("shard", None),
            P("shard"),
            P("shard", None),
            P("shard", None),
            P("shard", None),
        ),
        out_specs=(
            P(("shard", "replica"), None),
            P(("shard", "replica"), None),
            P("shard"),
            P("shard", None),
            P("shard", None),
            P("shard", None),
            P("shard", None),
            P("shard"),
            P("shard", None),
            P("shard", None),
            P("shard", None),
        ),
        check_vma=False,
    )
```

```python
import functools
import math

import jax
import jax.numpy as jnp
from jax import lax
from jax.experimental import pallas as pl
from jax.experimental.pallas import tpu as pltpu
from jax.sharding import PartitionSpec as P

HEADS = 12
HDIM = 64
EPSILON = 1e-05
ROPE_BASE = 10000.0
MESH = pl.DeviceIdType.MESH
F32 = jnp.float32
BF16 = jnp.bfloat16
DMA = pltpu.SemaphoreType.DMA

ROWS = 192
COLS = 768
UNITS = 16
FBLOCKS = 4
SHARDS = 4
TILE = 256
TALL = 512


def toggle(index, stride):
    return index + (1 - 2 * ((index // stride) % 2)) * stride


def ring(index, members, stride):
    place = (index // stride) % members
    base = index - place * stride
    return place, [base + ((place + step) % members) * stride for step in range(1, members)]


def at(shard, replica):
    return {"shard": shard, "replica": replica}


def greet(peers):
    barrier = pltpu.get_barrier_semaphore()
    for peer in peers:
        pl.semaphore_signal(barrier, inc=1, device_id=peer, device_id_type=MESH)
    pl.semaphore_wait(barrier, len(peers))


def remote(source, target, send, receive, peer):
    return pltpu.make_async_remote_copy(
        src_ref=source,
        dst_ref=target,
        send_sem=send,
        recv_sem=receive,
        device_id=peer,
        device_id_type=MESH,
    )


def mult(start, step):
    return start if isinstance(start, int) else pl.multiple_of(start, step)


def span(start, size, step=16):
    return pl.ds(mult(start, step), size)


class Levels:
    def __init__(self, replica, count):
        self.replica = replica
        if count == 8:
            self.pack, self.members, self.strides = 1, [2, 4], [1, 2]
            self.cuts = [("rows", 2), ("quarters", 4)]
        else:
            assert count == 32
            self.pack, self.members, self.strides = 4, [2, 4, 4], [16, 4, 1]
            self.cuts = [("units", 2), ("halves", 4), ("quarters", 4)]
        self.count = len(self.members)
        self.whole = UNITS // self.pack
        self.items = [(chunk, None) for chunk in range(self.whole)]
        self.items += [
            (chunk, third) for chunk in range(self.whole, UNITS // self.pack) for third in range(3)
        ]

    def item(self, chunk, third):
        return chunk if third is None else self.whole + 3 * (chunk - self.whole) + third

    def group(self, level, chunk):
        return ring(self.replica, self.members[level], self.strides[level])

    def places(self, chunk):
        return [self.group(level, chunk)[0] for level in range(self.count)]

    def size(self, level):
        units, rows, columns = self.pack, ROWS, COLS
        for kind, _ in self.cuts[:level]:
            if kind == "units":
                units = units // 2
            elif kind == "rows":
                rows = rows // 2
            elif kind == "columns":
                columns = columns // 2
            elif kind == "halves":
                units, rows = units // 2, rows // 2
            else:
                rows, columns = rows // 2, columns // 2
        return units, rows, columns

    def region(self, chunk, third, places):
        unit, row, column = chunk * self.pack, 0, 0
        parts = 1
        if third is not None:
            parts, column = 3, third * (COLS // 3)
        for level, place in enumerate(places):
            kind = self.cuts[level][0]
            units, rows, columns = self.size(level + 1)
            columns = columns // parts
            if kind == "units":
                unit = unit + place * units
            elif kind == "rows":
                row = row + place * rows
            elif kind == "columns":
                column = column + place * columns
            elif kind == "halves":
                unit, row = unit + place // 2 * units, row + place % 2 * rows
            else:
                row, column = row + place // 2 * rows, column + place % 2 * columns
        units, rows, columns = self.size(len(places))
        return pl.ds(unit, units), span(row, rows), span(column, columns // parts, 128)


def dot(a, b):
    return jnp.dot(a, b, preferred_element_type=F32)


def dot_nt(a, b):
    return lax.dot_general(a, b, (((1,), (1,)), ((), ())), preferred_element_type=F32)


def dot_tn(a, b):
    return lax.dot_general(a, b, (((0,), (0,)), ((), ())), preferred_element_type=F32)


def flat(block):
    return block.reshape(-1, block.shape[-1])


def scale_of(values):
    return lax.rsqrt(jnp.mean(values * values, axis=-1, keepdims=True) + EPSILON)


def half_swap(values):
    lane = lax.broadcasted_iota(jnp.int32, values.shape, 1)
    return jnp.where(lane % 64 < 32, pltpu.roll(values, 96, 1), pltpu.roll(values, 32, 1))


def head_mask(which):
    lane = lax.broadcasted_iota(jnp.int32, (1, 128), 1)
    return jnp.where((lane < 64) == (which == 0), 1.0, 0.0).astype(BF16)


def own_length(lengths, assignment, device):
    total = jnp.int32(0)
    for number in range(lengths.shape[0]):
        total = total + jnp.where(assignment[number] == device, lengths[number], 0)
    return total


def rotation(start, length, tokens):
    row = lax.broadcasted_iota(jnp.int32, (tokens, 128), 0)
    lane = lax.broadcasted_iota(jnp.int32, (1, 128), 1)
    half = HDIM // 2
    frequency = jnp.exp((lane % half).astype(F32) * (-2.0 * math.log(ROPE_BASE) / HDIM))
    angles = jnp.where(row < length, row + start, 0).astype(F32) * frequency
    return jnp.cos(angles), jnp.sin(angles) * jnp.where(lane % HDIM < half, -1.0, 1.0)


def norm_back(grad_normed, values, gain):
    scale = scale_of(values)
    scaled = gain * grad_normed
    gain_grad = jnp.sum(grad_normed * values * scale, axis=0, keepdims=True)
    mean = jnp.mean(scaled * values, axis=-1, keepdims=True)
    return gain_grad, scale * scaled - values * (scale * scale * scale) * mean


def forward_kernel(
    lengths, assignment, positions, x_hbm, gain_hbm, q_hbm, k_hbm, v_hbm, o_hbm, g_hbm, u_hbm, d_hbm,
    w_out, qkv_out, nt_out, n2t_out, at_out, ht_out, hid_out, a_out, b_out, h1_out, lse_out, gain_out,
    tables_out,
    w, x, tables, gains, gain, normed, normed_t, qkv, bias, attended, lse, lse_t, h1, ht, hid, a, b,
    load, x_out, x_in, y_out, y_in, z_out, z_in, d_out, d_in, p_out, p_in, f_out, f_in, g_out, g_in,
    w_store, store, f_store,
):
    shard, replica = lax.axis_index("shard"), lax.axis_index("replica")
    partner, across = toggle(shard, 1), toggle(shard, 2)
    opposite = toggle(across, 1)
    beside, behind = toggle(replica, 1), toggle(replica, 2)
    mine = replica % 4
    quarter_beside, quarter_behind = toggle(mine, 1), toggle(mine, 2)
    quarter_last = toggle(quarter_beside, 2)
    tokens, width = x.shape

    sources = [q_hbm, k_hbm, v_hbm, o_hbm]
    for block in range(FBLOCKS):
        columns = pl.ds(block * COLS, COLS)
        sources += [g_hbm.at[:, columns], u_hbm.at[:, columns]]
    sources += [d_hbm.at[pl.ds(piece * ROWS, ROWS)] for piece in range(UNITS - len(sources))]
    loads = [
        pltpu.make_async_copy(source, w.at[unit, shard], load.at[unit])
        for unit, source in enumerate(sources)
    ]
    x_load = pltpu.make_async_copy(x_hbm, x, load.at[UNITS])
    gain_load = pltpu.make_async_copy(gain_hbm, gains.at[shard], load.at[UNITS + 1])
    gain_load.start()
    for copy in loads:
        copy.start()
    x_load.start()

    shard_peers = [at(partner, replica), at(across, replica), at(opposite, replica)]
    greet(shard_peers + [at(shard, beside), at(shard, behind)])

    gain_load.wait()
    gain_copies = [
        remote(gains.at[shard], gains.at[shard], g_out.at[number], g_in.at[number], peer)
        for number, peer in enumerate(shard_peers)
    ]
    for copy in gain_copies:
        copy.start()

    quarter = ROWS // 4

    def part(unit, owner, which):
        return w.at[unit, owner, span(which * quarter, quarter)]

    def cross(unit):
        piece = part(unit, shard, mine)
        return remote(piece, piece, x_out.at[unit], x_in.at[unit], at(across, replica))

    def share(unit):
        piece = w.at[unit, shard]
        return remote(piece, piece, p_out.at[unit], p_in.at[unit], at(partner, replica))

    def hand_beside(unit):
        piece = part(unit, across, mine)
        return remote(piece, piece, y_out.at[unit], y_in.at[unit], at(shard, beside))

    def hand_behind(unit):
        piece = part(unit, across, mine)
        return remote(piece, piece, z_out.at[unit], z_in.at[unit], at(shard, behind))

    def hand_on(unit, odd):
        piece = part(unit, across, quarter_beside if odd else quarter_behind)
        peer = at(shard, behind if odd else beside)
        return remote(piece, piece, d_out.at[unit], d_in.at[unit], peer)

    def by_parity(unit, act):
        for odd in range(2):
            pl.when(unit % 2 == odd)(functools.partial(act, odd))

    def forward(unit, number):
        which = (mine, quarter_beside, quarter_behind, quarter_last)[number]
        piece = part(unit, across, which)
        return remote(piece, piece, f_out.at[number, unit], f_in.at[number, unit], at(partner, replica))

    def keep(unit):
        return pltpu.make_async_copy(w.at[unit], w_out.at[unit], w_store.at[unit])

    for unit in range(UNITS):
        loads[unit].wait()
        cross(unit).start()
        share(unit).start()

    def take_cross(unit):
        cross(unit).wait_recv()
        hand_beside(unit).start()
        hand_behind(unit).start()
        forward(unit, 0).start()

    def take_hands(unit):
        hand_behind(unit).wait_recv()
        hand_beside(unit).wait_recv()
        by_parity(unit, lambda odd: hand_on(unit, odd).start())
        forward(unit, 1).start()
        forward(unit, 2).start()

    def take_last(unit):
        by_parity(unit, lambda odd: hand_on(unit, odd).wait_recv())
        forward(unit, 3).start()

    def complete(unit):
        share(unit).wait_recv()
        for number in range(4):
            forward(unit, number).wait_recv()
        keep(unit).start()

    stages = [(0, take_cross), (2, take_hands), (4, take_last), (5, complete)]

    def tick(time):
        for lag, stage in stages:
            pl.when((time >= lag) & (time < UNITS + lag))(functools.partial(stage, time - lag))

    def ticks(first, last):
        def body(time, carry):
            tick(time)
            return carry

        lax.fori_loop(first, last, body, 0)

    stores = []

    def save(source, target):
        copy = pltpu.make_async_copy(source, target, store.at[len(stores)])
        copy.start()
        stores.append(copy)

    row = lax.broadcasted_iota(jnp.int32, (tokens, tokens), 0)
    column = lax.broadcasted_iota(jnp.int32, (tokens, tokens), 1)
    device = shard * lax.axis_size("replica") + replica
    length = own_length(lengths, assignment, device)
    seen = (column <= row) & ((row < length) | (column >= length))
    bias[...] = jnp.where(seen, 0.0, -jnp.inf)

    x_load.wait()
    for copy in gain_copies:
        copy.wait_recv()
    gain[...] = gains[0] + gains[1] + gains[2] + gains[3]
    save(gain, gain_out)
    values = x[...].astype(F32)
    normed[...] = (values * scale_of(values) * gain[0:1]).astype(BF16)
    normed_t[0] = normed[...].T
    save(normed_t.at[0], nt_out)
    tables[0], tables[1] = rotation(positions[0], length, tokens)
    save(tables, tables_out)
    ticks(0, 8)

    def project(which, carry):
        product = dot(normed[...], flat(w[which]))
        cosine = jnp.where(which < 2, tables[0], 1.0)
        sine = jnp.where(which < 2, tables[1], 0.0)
        for pair in range(width // 128):
            columns = slice(pair * 128, pair * 128 + 128)
            piece = product[:, columns]
            qkv[which, :, columns] = (piece * cosine + half_swap(piece) * sine).astype(BF16)
        return carry

    lax.fori_loop(0, 3, project, 0)
    save(qkv, qkv_out)
    tick(8)
    lse[...] = jnp.zeros_like(lse)

    def attend(pair, carry):
        columns = span(pair * 128, 128, 128)
        for tile in range(tokens // TILE):
            rows = pl.ds(tile * TILE, TILE)
            keys = (tile + 1) * TILE
            query = qkv[0, rows, columns]
            key = qkv[1, 0:keys, columns]
            value = qkv[2, 0:keys, columns]
            mixed = []
            logs = lse[rows]
            lane = lax.broadcasted_iota(jnp.int32, logs.shape, 1)
            for which in range(2):
                scores = dot_nt(query * head_mask(which), key) * (1.0 / math.sqrt(HDIM))
                scores = scores + bias[rows, 0:keys]
                peak = jnp.max(scores, axis=-1, keepdims=True)
                exponent = jnp.exp(scores - peak)
                total = jnp.sum(exponent, axis=-1, keepdims=True)
                probability = (exponent * (1.0 / total)).astype(BF16)
                mixed.append(dot(probability, value))
                logs = jnp.where(lane == 2 * pair + which, peak + jnp.log(total), logs)
            lse[rows] = logs
            first = lax.broadcasted_iota(jnp.int32, mixed[0].shape, 1) < 64
            attended[rows, columns] = jnp.where(first, mixed[0], mixed[1]).astype(BF16)
        tick(9 + pair)
        return carry

    lax.fori_loop(0, HEADS // 2, attend, 0)
    normed_t[1] = attended[...].T
    save(normed_t.at[1], at_out)
    lse_t[...] = lse[...].T
    save(lse_t, lse_out)
    for tile in range(tokens // TILE):
        rows = pl.ds(tile * TILE, TILE)
        hidden_one = x[rows].astype(F32) + dot(attended[rows], flat(w[3]))
        h1[rows] = hidden_one
        normed[rows] = (hidden_one * scale_of(hidden_one) * gain[1:2]).astype(BF16)
    save(h1, h1_out)
    normed_t[2] = normed[...].T
    save(normed_t.at[2], n2t_out)

    def f_copies(block):
        pairs = [
            (hid.at[block], hid_out.at[block]),
            (a.at[block], a_out.at[block]),
            (b.at[block], b_out.at[block]),
            (ht.at[:, block], ht_out.at[:, block]),
        ]
        return [
            pltpu.make_async_copy(source, target, f_store.at[block, number])
            for number, (source, target) in enumerate(pairs)
        ]

    def feed(block, carry):
        def rows_of(tile, inner):
            rows = span(tile * TALL, TALL)
            gate = dot(normed[rows], flat(w[4 + 2 * block]))
            upward = dot(normed[rows], flat(w[5 + 2 * block]))
            sigmoid = jax.nn.sigmoid(gate)
            activated = gate * sigmoid
            hid[block, rows] = (activated * upward).astype(BF16)
            a[block, rows] = (upward * sigmoid * (1.0 + gate * (1.0 - sigmoid))).astype(BF16)
            b[block, rows] = activated.astype(BF16)
            return inner

        lax.fori_loop(0, tokens // TALL, rows_of, 0)
        turned = hid[block].T
        for piece in range(FBLOCKS):
            ht[piece, block] = turned[piece * ROWS : (piece + 1) * ROWS]
        for copy in f_copies(block):
            copy.start()
        tick(15 + block)
        return carry

    lax.fori_loop(0, FBLOCKS, feed, 0)
    ticks(15 + FBLOCKS, UNITS + 5)

    def settle(unit, carry):
        cross(unit).wait_send()
        share(unit).wait_send()
        hand_beside(unit).wait_send()
        hand_behind(unit).wait_send()
        by_parity(unit, lambda odd: hand_on(unit, odd).wait_send())
        for number in range(4):
            forward(unit, number).wait_send()
        keep(unit).wait()
        return carry

    lax.fori_loop(0, UNITS, settle, 0)
    for copy in gain_copies:
        copy.wait_send()
    for copy in stores:
        copy.wait()
    for block in range(FBLOCKS):
        for copy in f_copies(block):
            copy.wait()


def forward_pass(scalars, tokens, gain_rows, weights):
    count, width = tokens.shape
    shape = jax.ShapeDtypeStruct
    outs = (
        shape((UNITS, SHARDS, ROWS, COLS), BF16),
        shape((3, count, width), BF16),
        shape((width, count), BF16),
        shape((width, count), BF16),
        shape((width, count), BF16),
        shape((FBLOCKS, FBLOCKS, ROWS, count), BF16),
        shape((FBLOCKS, count, COLS), BF16),
        shape((FBLOCKS, count, COLS), BF16),
        shape((FBLOCKS, count, COLS), BF16),
        shape((count, width), F32),
        shape((128, count), F32),
        shape(gain_rows.shape, F32),
        shape((2, count, 128), F32),
    )
    anywhere = pl.BlockSpec(memory_space=pl.ANY)
    return pl.pallas_call(
        forward_kernel,
        out_shape=outs,
        in_specs=[pl.BlockSpec(memory_space=pltpu.SMEM)] * 3 + [anywhere] * 9,
        out_specs=[anywhere] * len(outs),
        scratch_shapes=[
            pltpu.VMEM((UNITS, SHARDS, ROWS, COLS), BF16),
            pltpu.VMEM((count, width), BF16),
            pltpu.VMEM((2, count, 128), F32),
            pltpu.VMEM((SHARDS,) + gain_rows.shape, F32),
            pltpu.VMEM(gain_rows.shape, F32),
            pltpu.VMEM((count, width), BF16),
            pltpu.VMEM((3, width, count), BF16),
            pltpu.VMEM((3, count, width), BF16),
            pltpu.VMEM((count, count), F32),
            pltpu.VMEM((count, width), BF16),
            pltpu.VMEM((count, 128), F32),
            pltpu.VMEM((128, count), F32),
            pltpu.VMEM((count, width), F32),
            pltpu.VMEM((FBLOCKS, FBLOCKS, ROWS, count), BF16),
            pltpu.VMEM((FBLOCKS, count, COLS), BF16),
            pltpu.VMEM((FBLOCKS, count, COLS), BF16),
            pltpu.VMEM((FBLOCKS, count, COLS), BF16),
            DMA((UNITS + 2,)),
        ]
        + [DMA((UNITS,))] * 10
        + [
            DMA((4, UNITS)), DMA((4, UNITS)), DMA((3,)), DMA((3,)),
            DMA((UNITS,)), DMA((8,)), DMA((FBLOCKS, 4)),
        ],
        compiler_params=pltpu.CompilerParams(
            collective_id=0, has_side_effects=True, vmem_limit_bytes=60 * 1024 * 1024
        ),
        name="forward_gather",
    )(*scalars, tokens, gain_rows, *weights)


def backward_kernel(
    replicas,
    lengths, assignment, x_hbm, cot_hbm, w_hbm, qkv_hbm, nt_hbm, n2t_hbm, at_hbm, ht_hbm,
    hid_hbm, a_hbm, b_hbm, h1_hbm, lse_hbm, gain_hbm, tables_hbm,
    sums_out, gain_out, output_out, grad_out,
    *refs,
):
    shard, replica = lax.axis_index("shard"), lax.axis_index("replica")
    order = Levels(replica, replicas)
    levels, pack = order.count, order.pack
    (grads, near, far, gain_sum, gain_got, gbt, gain, n2t, h1, acc, result) = refs[:11]
    parts = refs[11 : 11 + levels]
    sems = refs[11 + levels :]
    (load, s_load, near_out, near_in, far_out, far_in, store, gain_send, gain_recv) = sems[:9]
    ht_sem = sems[9]
    down_out, down_in, up_out, up_in = (
        sems[10 + kind * levels : 10 + (kind + 1) * levels] for kind in range(4)
    )
    partner, across = toggle(shard, 1), toggle(shard, 2)
    opposite = toggle(across, 1)
    tokens, width = gbt.shape
    length = own_length(lengths, assignment, shard * lax.axis_size("replica") + replica)
    flips = [at(partner, replica), at(across, replica)]
    stride = 1
    while stride < replicas:
        flips.append(at(shard, toggle(replica, stride)))
        stride *= 2

    def fetch(source, target, number):
        copy = pltpu.make_async_copy(source, target, load.at[number])
        copy.start()
        return copy

    cot_load = fetch(cot_hbm, gbt, 0)
    n2t_load = fetch(n2t_hbm, n2t, 1)
    h1_load = fetch(h1_hbm, h1, 2)
    gain_load = fetch(gain_hbm, gain, 4)

    greet(
        [at(partner, replica), at(across, replica)]
        + [at(shard, other) for level in range(levels) for other in order.group(level, 0)[1]]
    )

    chunks = UNITS // pack

    def view(owner, chunk, third, places):
        units, rows, columns = order.region(chunk, third, places)
        return grads.at[units, owner, rows, columns]

    def near_copy(unit, which):
        return remote(
            grads.at[unit, opposite if which == 0 else partner],
            near.at[unit, which],
            near_out.at[unit, which],
            near_in.at[unit, which],
            at(partner, replica),
        )

    def columns_of(third, width):
        return pl.ds(0, width) if third is None else pl.ds(third * (width // 3), width // 3)

    def far_copy(unit, third=None):
        columns = columns_of(third, COLS)
        item = order.item(unit, third)
        return remote(
            grads.at[unit, across, :, columns],
            far.at[unit, :, columns],
            far_out.at[item],
            far_in.at[item],
            at(across, replica),
        )

    def part(level, chunk, third, step):
        width = order.size(level + 1)[2]
        return parts[level].at[chunk, step, :, :, columns_of(third, width)]

    def down_copy(level, chunk, step, third=None):
        members = order.members[level]
        place, others = order.group(level, chunk)
        theirs = (place + step + 1) % members
        item = order.item(chunk, third)
        return remote(
            view(shard, chunk, third, order.places(chunk)[:level] + [theirs]),
            part(level, chunk, third, step),
            down_out[level].at[item, step],
            down_in[level].at[item, step],
            at(shard, others[step]),
        )

    def up_copy(level, chunk, step, third=None):
        piece = view(partner, chunk, third, order.places(chunk)[: level + 1])
        item = order.item(chunk, third)
        return remote(
            piece,
            piece,
            up_out[level].at[item, step],
            up_in[level].at[item, step],
            at(shard, order.group(level, chunk)[1][step]),
        )

    def store_copy(chunk, third=None):
        units = pl.ds(chunk * pack, pack)
        columns = columns_of(third, COLS)
        return pltpu.make_async_copy(
            grads.at[units, partner, :, columns],
            sums_out.at[units, :, columns],
            store.at[order.item(chunk, third)],
        )

    def over(level, act):
        for step in range(order.members[level] - 1):
            act(step)

    def give(unit):
        for which in range(2):
            near_copy(unit, which).start()

    def plus(*terms):
        total = terms[0].astype(F32)
        for term in terms[1:]:
            total = total + term.astype(F32)
        return total.astype(BF16)

    def take_near(unit):
        near_copy(unit, 0).wait_recv()
        grads[unit, across] = plus(grads[unit, across], near[unit, 0])
        if pack > 1:
            far_copy(unit).start()
        else:
            pl.when(unit < order.whole)(lambda: far_copy(unit).start())

            @pl.when(unit >= order.whole)
            def _():
                for third in range(3):
                    far_copy(unit, third).start()

        near_copy(unit, 1).wait_recv()
        grads[unit, shard] = plus(grads[unit, shard], near[unit, 1])

    def take_far(chunk, third=None):
        for piece in range(pack):
            unit = chunk * pack + piece
            if third is None or third == 0:
                near_copy(unit, 0).wait_send()
                near_copy(unit, 1).wait_send()
            far_copy(unit, third).wait_recv()
            columns = columns_of(third, COLS)
            grads[unit, shard, :, columns] = plus(
                grads[unit, shard, :, columns], far[unit, :, columns]
            )
        over(0, lambda step: down_copy(0, chunk, step, third).start())

    def take_down(level, chunk, third=None):
        over(level, lambda step: down_copy(level, chunk, step, third).wait_recv())
        places = order.places(chunk)[: level + 1]
        terms = [view(shard, chunk, third, places)[...]]
        terms += [part(level, chunk, third, step)[...] for step in range(order.members[level] - 1)]
        total = plus(*terms)
        if level + 1 < levels:
            view(shard, chunk, third, places)[...] = total
            over(level + 1, lambda step: down_copy(level + 1, chunk, step, third).start())
        else:
            view(partner, chunk, third, places)[...] = total
            over(level, lambda step: up_copy(level, chunk, step, third).start())

    def take_up(level, chunk, third=None):
        over(level, lambda step: up_copy(level, chunk, step, third).wait_recv())
        if level > 0:
            over(level - 1, lambda step: up_copy(level - 1, chunk, step, third).start())
        else:
            store_copy(chunk, third).start()

    stages = [take_far]
    stages += [functools.partial(take_down, level) for level in range(levels)]
    stages += [functools.partial(take_up, level) for level in reversed(range(levels))]

    def post(time):
        step = (time + 1) // pack - 1
        for lag, stage in enumerate(stages):
            good = (step >= lag) & (step < chunks + lag) & ((time + 1) % pack == 0)
            pl.when(good)(functools.partial(stage, step - lag))

    def remaining(first):
        arrival, found = 0.0, []
        for chunk, third in order.items:
            pace = 1.0 if third is None else 1.0 / 3
            arrival += pace
            wait = (0.0, 1.02, 2.02, 3.02, 5.02) if third is None else (0.0, 0.68, 1.36, 2.04, 2.72)
            for lag, stage in enumerate(stages):
                if chunk + lag >= first:
                    found.append((arrival + wait[lag], lag, len(found), stage, chunk, third))
        return [entry[3:] for entry in sorted(found, key=lambda entry: entry[:3])]

    def gain_copy(step):
        return remote(
            gain_sum.at[step], gain_got.at[step], gain_send.at[step], gain_recv.at[step], flips[step]
        )

    row = lax.broadcasted_iota(jnp.int32, (tokens, 1), 0)
    valid = jnp.where(row < length, 1.0, 0.0)

    def down_phase(ht):
        ht_loads = [
            pltpu.make_async_copy(ht_hbm.at[unit], ht.at[unit], ht_sem.at[unit])
            for unit in range(FBLOCKS)
        ]
        for copy in ht_loads:
            copy.start()
        cot_load.wait()
        gbt[...] = (gbt[...].astype(F32) * valid).astype(BF16)

        def down_grads(unit, carry):
            pltpu.make_async_copy(ht_hbm.at[unit], ht.at[unit], ht_sem.at[unit]).wait()
            product = dot(flat(ht[unit]), gbt[...]).astype(BF16)
            grads[unit] = product.reshape(SHARDS, ROWS, COLS)
            give(unit)
            pl.when(unit >= 1)(lambda: take_near(unit - 1))
            return carry

        lax.fori_loop(0, FBLOCKS, down_grads, 0)

    def feed_forward(down_w, gate_w, up_w, hid, grad_pair):
        def stream(block):
            slot = block % 2
            pairs = [
                (w_hbm.at[pl.ds(UNITS - FBLOCKS, FBLOCKS), block], down_w.at[slot]),
                (w_hbm.at[4 + 2 * block], gate_w.at[slot]),
                (w_hbm.at[5 + 2 * block], up_w.at[slot]),
                (hid_hbm.at[block], hid.at[slot]),
                (a_hbm.at[block], grad_pair.at[slot, 0]),
                (b_hbm.at[block], grad_pair.at[slot, 1]),
            ]
            return [
                pltpu.make_async_copy(source, target, s_load.at[slot, number])
                for number, (source, target) in enumerate(pairs)
            ]

        for copy in stream(0):
            copy.start()
        n2t_load.wait()
        acc[...] = jnp.zeros_like(acc)
        result[...] = jnp.zeros_like(result)

        def block_step(block, carry):
            slot = block % 2

            @pl.when(block + 1 < FBLOCKS)
            def _():
                for copy in stream(block + 1):
                    copy.start()

            for copy in stream(block):
                copy.wait()

            grad_hidden = dot_nt(gbt[...], flat(down_w[slot]))
            grad_pair[slot, 0] = (grad_hidden * grad_pair[slot, 0].astype(F32)).astype(BF16)
            grad_pair[slot, 1] = (grad_hidden * grad_pair[slot, 1].astype(F32)).astype(BF16)
            pl.when(block == 0)(lambda: take_near(FBLOCKS - 1))

            def kind_of(kind, inner):
                unit = FBLOCKS + 2 * block + kind
                product = dot(n2t[...], grad_pair[slot, kind]).astype(BF16)
                grads[unit] = product.reshape(SHARDS, ROWS, COLS)
                give(unit)
                return inner

            lax.fori_loop(0, 2, kind_of, 0)

            post(2 * block - block // 3)
            acc[...] += dot_nt(grad_pair[slot, 0], flat(gate_w[slot])) + dot_nt(
                grad_pair[slot, 1], flat(up_w[slot])
            )
            result[...] += dot(hid[slot], flat(down_w[slot]))
            take_near(FBLOCKS + 2 * block)
            take_near(FBLOCKS + 2 * block + 1)
            pl.when(block != 2)(lambda: post(2 * block + 1 - block // 3))
            return carry

        lax.fori_loop(0, FBLOCKS, block_step, 0)

    pl.run_scoped(down_phase, pltpu.VMEM((FBLOCKS, FBLOCKS, ROWS, tokens), BF16))
    pl.run_scoped(
        feed_forward,
        pltpu.VMEM((2, FBLOCKS, ROWS, COLS), BF16),
        pltpu.VMEM((2, SHARDS, ROWS, COLS), BF16),
        pltpu.VMEM((2, SHARDS, ROWS, COLS), BF16),
        pltpu.VMEM((2, tokens, COLS), BF16),
        pltpu.VMEM((2, 2, tokens, COLS), BF16),
    )

    def attention(attn_w, tables, qkv, lse, bias, grad_attended, grad_qkv, turned, x, out_low):
        at_load = fetch(at_hbm, turned.at[0], 5)
        w_load = fetch(w_hbm.at[pl.ds(0, 4)], attn_w, 8)
        qkv_load = fetch(qkv_hbm, qkv, 9)
        lse_load = fetch(lse_hbm.at[pl.ds(0, 16)], lse, 10)
        table_load = fetch(tables_hbm, tables, 11)
        nt_load = fetch(nt_hbm, turned.at[1], 6)
        x_load = fetch(x_hbm, x, 3)
        h1_load.wait()
        gain_load.wait()

        gain_grad = jnp.zeros((1, width), F32)
        for tile in range(tokens // TILE):
            rows = pl.ds(tile * TILE, TILE)
            good = jnp.where(
                lax.broadcasted_iota(jnp.int32, (TILE, 1), 0) + tile * TILE < length, 1.0, 0.0
            )
            out_low[rows] = ((h1[rows] + result[rows]) * good).astype(BF16)
            gain_piece, back = norm_back(acc[rows], h1[rows], gain[1:2])
            gain_grad = gain_grad + gain_piece
            grad_one = gbt[rows].astype(F32) + back
            result[rows] = grad_one
            gbt[rows] = grad_one.astype(BF16)
        gain_sum[0] = jnp.zeros_like(gain_sum[0])
        gain_sum[0, 1:2] = gain_grad
        output_store = pltpu.make_async_copy(out_low, output_out, load.at[12])
        output_store.start()
        at_load.wait()
        product = dot(turned[0], gbt[...]).astype(BF16)
        grads[UNITS - 4] = product.reshape(SHARDS, ROWS, COLS)
        give(UNITS - 4)
        w_load.wait()
        for tile in range(tokens // TILE):
            rows = pl.ds(tile * TILE, TILE)
            grad_attended[rows] = dot_nt(gbt[rows], flat(attn_w[3])).astype(BF16)
        take_near(UNITS - 4)
        post(7)

        key_row = lax.broadcasted_iota(jnp.int32, (tokens, tokens), 0)
        query_column = lax.broadcasted_iota(jnp.int32, (tokens, tokens), 1)
        seen = (key_row <= query_column) & ((query_column < length) | (key_row >= length))
        bias[...] = jnp.where(seen, 0.0, -jnp.inf).astype(BF16)
        qkv_load.wait()
        lse_load.wait()
        table_load.wait()
        inv_root = 1.0 / math.sqrt(HDIM)

        def attend_back(pair, carry):
            columns = span(pair * 128, 128, 128)
            grad_key = [jnp.zeros((TILE, 128), F32) for _ in range(tokens // TILE)]
            grad_value = [jnp.zeros((TILE, 128), F32) for _ in range(tokens // TILE)]
            for tile in range(tokens // TILE):
                rows = pl.ds(tile * TILE, TILE)
                query = qkv[0, rows, columns]
                grad_mixed = grad_attended[rows, columns]
                grad_query = jnp.zeros((TILE, 128), F32)
                for which in range(2):
                    mask = head_mask(which)
                    query_one = query * mask
                    mixed_one = grad_mixed * mask
                    log_row = lse[pl.ds(2 * pair + which, 1), rows]
                    probs, grad_probs = [], []
                    row_dot = jnp.zeros((1, TILE), F32)
                    for block in range(tile + 1):
                        keys = pl.ds(block * TILE, TILE)
                        scores = dot_nt(qkv[1, keys, columns], query_one) * inv_root
                        prob = jnp.exp(scores + bias[keys, rows].astype(F32) - log_row)
                        grad_value[block] += dot(prob.astype(BF16), mixed_one)
                        grad_prob = dot_nt(qkv[2, keys, columns], mixed_one)
                        row_dot = row_dot + jnp.sum(prob * grad_prob, axis=0, keepdims=True)
                        probs.append(prob)
                        grad_probs.append(grad_prob)
                    for block in range(tile + 1):
                        keys = pl.ds(block * TILE, TILE)
                        grad_scores = (probs[block] * (grad_probs[block] - row_dot)).astype(BF16)
                        grad_key[block] += dot(grad_scores, query_one)
                        grad_query += dot_tn(grad_scores, qkv[1, keys, columns] * mask)
                grad_query = grad_query * inv_root
                grad_query = grad_query * tables[0, rows] - half_swap(grad_query) * tables[1, rows]
                grad_qkv[0, rows, columns] = grad_query.astype(BF16)
            for block in range(tokens // TILE):
                keys = pl.ds(block * TILE, TILE)
                back = grad_key[block] * inv_root
                back = back * tables[0, keys] - half_swap(back) * tables[1, keys]
                grad_qkv[1, keys, columns] = back.astype(BF16)
                grad_qkv[2, keys, columns] = grad_value[block].astype(BF16)
            pl.when(pair % 2 == 1)(lambda: post(8 + pair // 2))
            return carry

        lax.fori_loop(0, HEADS // 2, attend_back, 0)
        nt_load.wait()

        def projection(which, carry):
            product = dot(turned[1], grad_qkv[which]).astype(BF16)
            grads[UNITS - 3 + which] = product.reshape(SHARDS, ROWS, COLS)
            give(UNITS - 3 + which)
            return carry

        lax.fori_loop(0, 3, projection, 0)
        acc[...] = jnp.zeros_like(acc)

        def input_back(which, carry):
            acc[...] += dot_nt(grad_qkv[which], flat(attn_w[which]))
            take_near(UNITS - 3 + which)
            return carry

        lax.fori_loop(0, 3, input_back, 0)
        x_load.wait()
        gain_grad = jnp.zeros((1, width), F32)
        for tile in range(tokens // TILE):
            rows = pl.ds(tile * TILE, TILE)
            gain_piece, back = norm_back(acc[rows], x[rows].astype(F32), gain[0:1])
            gain_grad = gain_grad + gain_piece
            result[rows] = result[rows] + back
        gain_sum[0, 0:1] = gain_grad
        grad_store = pltpu.make_async_copy(result, grad_out, load.at[13])
        grad_store.start()
        output_store.wait()
        grad_store.wait()

    pl.run_scoped(
        attention,
        pltpu.VMEM((4, SHARDS, ROWS, COLS), BF16),
        pltpu.VMEM((2, tokens, 128), F32),
        pltpu.VMEM((3, tokens, width), BF16),
        pltpu.VMEM((16, tokens), F32),
        pltpu.VMEM((tokens, tokens), BF16),
        pltpu.VMEM((tokens, width), BF16),
        pltpu.VMEM((3, tokens, width), BF16),
        pltpu.VMEM((2, width, tokens), BF16),
        pltpu.VMEM((tokens, width), BF16),
        pltpu.VMEM((tokens, width), BF16),
    )

    first = 11
    gain_copy(0).start()

    def gain_step(step):
        gain_copy(step).wait_recv()
        gain_sum[step + 1] = gain_sum[step] + gain_got[step]
        if step + 1 < len(flips):
            gain_copy(step + 1).start()

    if pack > 1:
        lax.fori_loop(first, pack * (chunks + len(stages) - 1), lambda time, _: (post(time), _)[1], 0)
        for step in range(len(flips)):
            gain_step(step)
    else:
        plan = remaining(first)
        for number, (stage, chunk, third) in enumerate(plan):
            stage(chunk, third)
            left = len(plan) - 1 - number
            if left % 2 == 1 and left // 2 < len(flips):
                gain_step(len(flips) - 1 - left // 2)
    gain_out[...] = gain_sum[len(flips)]

    def settle(chunk, third=None):
        for piece in range(pack):
            far_copy(chunk * pack + piece, third).wait_send()
        for level in range(levels):
            over(level, lambda step: down_copy(level, chunk, step, third).wait_send())
            over(level, lambda step: up_copy(level, chunk, step, third).wait_send())
        store_copy(chunk, third).wait()

    lax.fori_loop(0, order.whole, lambda chunk, _: (settle(chunk), _)[1], 0)
    for chunk, third in order.items[order.whole :]:
        settle(chunk, third)
    for step in range(len(flips)):
        gain_copy(step).wait_send()


def backward_pass(scalars, tokens, cotangent, saved):
    count, width = tokens.shape
    replicas = lax.axis_size("replica")
    order = Levels(0, replicas)
    chunks = UNITS // order.pack
    flips = 2 + replicas.bit_length() - 1
    gain = saved[-2]
    part_shapes = [
        (chunks, members - 1) + order.size(level + 1) for level, members in enumerate(order.members)
    ]
    items = max(len(order.items), UNITS)
    counts = [(items, members - 1) for members in order.members]
    anywhere = pl.BlockSpec(memory_space=pl.ANY)
    shape = jax.ShapeDtypeStruct
    return pl.pallas_call(
        functools.partial(backward_kernel, replicas),
        out_shape=(
            shape((UNITS, ROWS, COLS), BF16),
            shape(gain.shape, F32),
            shape((count, width), BF16),
            shape((count, width), F32),
        ),
        in_specs=[pl.BlockSpec(memory_space=pltpu.SMEM)] * 2 + [anywhere] * (2 + len(saved)),
        out_specs=[anywhere, pl.BlockSpec(memory_space=pltpu.VMEM), anywhere, anywhere],
        scratch_shapes=[
            pltpu.VMEM((UNITS, SHARDS, ROWS, COLS), BF16),
            pltpu.VMEM((UNITS, 2, ROWS, COLS), BF16),
            pltpu.VMEM((UNITS, ROWS, COLS), BF16),
            pltpu.VMEM((flips + 1,) + gain.shape, F32),
            pltpu.VMEM((flips,) + gain.shape, F32),
            pltpu.VMEM((count, width), BF16),
            pltpu.VMEM(gain.shape, F32),
            pltpu.VMEM((width, count), BF16),
            pltpu.VMEM((count, width), F32),
            pltpu.VMEM((count, width), F32),
            pltpu.VMEM((count, width), F32),
        ]
        + [pltpu.VMEM(part, BF16) for part in part_shapes]
        + [

            DMA((14,)), DMA((2, 6)), DMA((UNITS, 2)), DMA((UNITS, 2)), DMA((items,)), DMA((items,)),
            DMA((items,)), DMA((flips,)), DMA((flips,)), DMA((FBLOCKS,)),
        ]
        + [DMA(count_) for _ in range(4) for count_ in counts],
        compiler_params=pltpu.CompilerParams(
            collective_id=1, has_side_effects=True, vmem_limit_bytes=67043328
        ),
        name="backward_reduce",
    )(*scalars, tokens, cotangent, *saved)


def finish_kernel(
    sums, gain_sums, output_in, grad_in,
    down, gate, up, out, query, key, value, gain_one, gain_two, output, grad,
    low, wide, held_output, held_grad, in_sem, out_sem,
):
    targets = [down.at[pl.ds(piece * ROWS, ROWS)] for piece in range(FBLOCKS)]
    for block in range(FBLOCKS):
        columns = pl.ds(block * COLS, COLS)
        targets += [gate.at[:, columns], up.at[:, columns]]
    targets += [out, query, key, value]
    moves = [(output_in, held_output, output), (grad_in, held_grad, grad)]
    ins = [
        pltpu.make_async_copy(sums.at[unit], low.at[unit], in_sem.at[unit]) for unit in range(UNITS)
    ]
    ins += [
        pltpu.make_async_copy(source, held, in_sem.at[UNITS + number])
        for number, (source, held, _) in enumerate(moves)
    ]
    puts = [
        pltpu.make_async_copy(wide.at[unit], target, out_sem.at[unit])
        for unit, target in enumerate(targets)
    ]
    puts += [
        pltpu.make_async_copy(held, target, out_sem.at[UNITS + number])
        for number, (_, held, target) in enumerate(moves)
    ]
    for copy in ins[UNITS:] + ins[:UNITS]:
        copy.start()
    share = gain_sums.shape[1] // SHARDS
    shard = lax.axis_index("shard")
    turned = pltpu.roll(gain_sums[...], (SHARDS - shard) % SHARDS * share, 1)
    gain_one[...] = turned[0:1, :share]
    gain_two[...] = turned[1:2, :share]
    for number in range(UNITS, UNITS + len(moves)):
        ins[number].wait()
        puts[number].start()
    for unit in range(UNITS):
        ins[unit].wait()
        wide[unit] = low[unit].astype(F32)
        puts[unit].start()
    for copy in puts:
        copy.wait()


def finish(sums, gain_sums, output, input_grad):
    shape = jax.ShapeDtypeStruct
    small, broad = shape((ROWS, COLS), F32), shape((ROWS, FBLOCKS * COLS), F32)
    share = shape((1, gain_sums.shape[1] // SHARDS), F32)
    hbm, vmem = pl.BlockSpec(memory_space=pltpu.HBM), pl.BlockSpec(memory_space=pltpu.VMEM)
    return pl.pallas_call(
        finish_kernel,
        out_shape=(
            shape((FBLOCKS * ROWS, COLS), F32), broad, broad, small, small, small, small, share, share,
            shape(output.shape, output.dtype), shape(input_grad.shape, F32),
        ),
        in_specs=[hbm, vmem, hbm, hbm],
        out_specs=[hbm] * 7 + [vmem] * 2 + [hbm] * 2,
        scratch_shapes=[
            pltpu.VMEM((UNITS, ROWS, COLS), BF16),
            pltpu.VMEM((UNITS, ROWS, COLS), F32),
            pltpu.VMEM(output.shape, output.dtype),
            pltpu.VMEM(input_grad.shape, F32),
            DMA((UNITS + 2,)),
            DMA((UNITS + 2,)),
        ],
        compiler_params=pltpu.CompilerParams(vmem_limit_bytes=67043328),
        name="finish",
    )(sums, gain_sums, output, input_grad)


def per_device(
    tokens, cotangent, lengths, assignment, positions, attention_gain, query_weight, key_weight,
    value_weight, out_weight, feedforward_gain, gate_weight, up_weight, down_weight,
):
    shard = lax.axis_index("shard")
    lane = lax.broadcasted_iota(jnp.int32, (8, tokens.shape[1]), 1)
    row = lax.broadcasted_iota(jnp.int32, (8, tokens.shape[1]), 0)
    share = attention_gain.shape[0]
    spread = [
        jnp.broadcast_to(gain, (SHARDS, share)).reshape(1, -1).astype(F32)
        for gain in (attention_gain, feedforward_gain)
    ]
    gain_rows = jnp.where(
        (lane // share == shard) & (row < 2), jnp.where(row == 0, spread[0], spread[1]), 0.0
    )
    saved = forward_pass(
        [lengths, assignment, positions],
        tokens,
        gain_rows,
        [query_weight, key_weight, value_weight, out_weight, gate_weight, up_weight, down_weight],
    )
    sums, gain_sums, output, input_grad = backward_pass(
        [lengths, assignment], tokens, cotangent, saved
    )
    down, gate, up, out, query, key, value, gain_one, gain_two, output, input_grad = finish(
        sums, gain_sums, output, input_grad
    )
    return (
        output,
        input_grad,
        gain_one.reshape(-1),
        query,
        key,
        value,
        out,
        gain_two.reshape(-1),
        gate,
        up,
        down,
    )


def solution(mesh):
    return jax.shard_map(
        per_device,
        mesh=mesh,
        in_specs=(
            P(("shard", "replica"), None),
            P(("shard", "replica"), None),
            P(),
            P(),
            P(("shard", "replica")),
            P("shard"),
            P("shard", None),
            P("shard", None),
            P("shard", None),
            P("shard", None),
            P("shard"),
            P("shard", None),
            P("shard", None),
            P("shard", None),
        ),
        out_specs=(
            P(("shard", "replica"), None),
            P(("shard", "replica"), None),
            P("shard"),
            P("shard", None),
            P("shard", None),
            P("shard", None),
            P("shard", None),
            P("shard"),
            P("shard", None),
            P("shard", None),
            P("shard", None),
        ),
        check_vma=False,
    )
```
